32 devices in a mesh: dp: 8 (over z, x), rep: 4 (over y, core).
Axes of the slice: x: 2, y: 2, z: 4, core: 2. Of those that a mesh axis runs over, the one named last changes fastest.
Arguments:
- hot_ids: int32 [8192, 2], P(('dp', 'rep')), may hold values from 0 to 1023
- cold_owner: int32 [16384, 1], P(('dp', 'rep')), may hold values from 0 to 7; in each aligned block of 512 rows (0 to 511, 512 to 1023, ...) at most 128 rows name the same one
- cold_offset: int32 [16384], P(('dp', 'rep')), may hold values from 0 to 511
- labels: int32 [8192], P(('dp', 'rep')), may hold values 0 or 1
- top_weight: bfloat16 [512, 1024], replicated, may hold values from -0.25 to 0.25
- out_weight: float32 [1024], replicated, may hold values from -0.5 to 0.5
- cold_table: float32 [4096, 128], P('dp'), may hold values from -6 to 6
- cold_accum: float32 [4096, 128], P('dp'), may hold values from 0.0001 to 0.01
- hot_cache: float32 [1024, 128], replicated, may hold values from -6 to 6
- hot_accum: float32 [1024, 128], replicated, may hold values from 0.01 to 1
- pending: float32 [32768, 128], P(('dp', 'rep')), may hold values from -0.3 to 0.3
- refresh_blocks: int32 [3], replicated, may hold values from 0 to 7, as said below
- block_clock: int32 [8], replicated, may hold values from 0 to 8
Outputs:
- cold_table_new: float32 [4096, 128], P('dp')
- cold_accum_new: float32 [4096, 128], P('dp')
- hot_cache_new: float32 [1024, 128], replicated
- hot_accum_new: float32 [1024, 128], replicated
- pending_new: float32 [32768, 128], P(('dp', 'rep'))
- top_grad: float32 [512, 1024], P(('dp', 'rep'))
- out_grad: float32 [1024], replicated
The draws below stay inside these ranges and needn't reach their ends.
Inputs may be any that keep to these rules, and one draw needn't show every extreme that they name: `cold_owner`: within the lookups of one device (512 rows), no owner is named more than 128 times. `refresh_blocks`: the block numbers are distinct.
All inputs are finite; a program needn't handle non-finite values. No bound on the sum of `labels` on one device may be relied on, other than what follows from the above.
Results may differ from the reference program's by a relative error of at most 0.00165.
The reference program's roundings to bfloat16 on the way (of `hot_rows`, `cold_rows`, `inputs`, `hidden`, `dhidden` and `dinputs`) count: a program that leaves them out, or rounds other values in their place, can miss the bound.
Values may be sent and summed in bfloat16 or wider, within the bound.
A program may use at most 64 MiB of HBM per device.

```python
import math
import jax
import jax.numpy as jnp
import numpy as np
from jax import lax

E = 128
H = 1024
FH = 2
FC = 2
B_DEV = 256
OWN_ROWS = 512
BLOCK = 128
HBLK = 8
NREF = 3
HOT = 1024
CAP = 128
SAMPLES = 8192
N_DP = 8
N_REP = 4


def draw_refresh_blocks(key, part):
    shuffled = jax.random.permutation(jax.random.fold_in(key, 41), HBLK)
    return shuffled[:NREF].astype(jnp.int32)


def place_ends(drawn, own_key, smallest, high):
    dims = drawn.shape
    spot = [jax.random.randint(jax.random.fold_in(own_key, axis), (), 0, dims[axis]) for axis in range(len(dims))]
    drawn = drawn.at[tuple(spot)].set(smallest)
    longest = dims.index(max(dims))
    spot[longest] = (spot[longest] + 1) % dims[longest]
    return drawn.at[tuple(spot)].set(high)


def level_of(rng, shape, cuts, low, high):
    factor_of = 1.0
    for dim, parts in cuts:
        heights = jax.random.uniform(jax.random.fold_in(jax.random.fold_in(rng, 6), dim), (parts,), jnp.float32, low / len(cuts), high / len(cuts))
        factor_of = factor_of * jnp.repeat(jnp.exp(heights), shape[dim] // parts).reshape((-1,) + (1,) * (len(shape) - 1 - dim))
    return factor_of


def rank_bounds(number_of, skew):
    weights = [(1 << 20) // math.isqrt(standing ** skew) + 1 for standing in range(1, number_of + 1)]
    spread = 1 + sum(weights) // (1 << 30)
    return np.cumsum(np.array([max(1, weight // spread) for weight in weights]))


def ranked_ids(rng, shape, count, skew):
    table = rank_bounds(count, skew)
    pick = jax.random.randint(jax.random.fold_in(rng, 1), shape, 0, int(table[count - 1]))
    grade = jnp.searchsorted(jnp.asarray(table, jnp.int32), pick, side="right")
    return jax.random.permutation(jax.random.fold_in(rng, 2), count)[grade].astype(jnp.int32)


def shared_out(rng, own, number, rows, count, top, most, skew):
    ranking = jax.random.permutation(rng, count)
    crowded, usual = shares(count, rows * top, most, skew, True), shares(count, rows * top, most, skew, False)
    places = jnp.arange(count)

    def named(tallies, offset_by):
        used = int((tallies > 0).sum())
        fixed = max(1, used // 4)
        passed = fixed + (places - fixed + offset_by * (used - fixed)) % max(1, count - fixed)
        return jnp.zeros((count,), jnp.int32).at[ranking[jnp.where(places < fixed, places, passed)]].set(jnp.asarray(tallies, jnp.int32))

    tallies = jnp.where(number % 4 == 0, named(crowded, number // 4), named(usual, number - number // 4 - 1))
    mixed = jax.random.permutation(jax.random.fold_in(own, 3), count)
    giver, receiver = mixed[0:count // 2 * 2:2], mixed[1:count // 2 * 2:2]
    margin = jnp.minimum(tallies[giver] - 1, most - tallies[receiver]) // 2
    margin = jnp.where((giver == ranking[0]) | (receiver == ranking[0]) | (tallies[receiver] == 0), 0, jnp.maximum(margin, 0))
    passed = jax.random.randint(jax.random.fold_in(own, 4), (count // 2,), 0, 1 << 20) % (margin + 1)
    tallies = tallies.at[giver].add(-passed).at[receiver].add(passed)
    items = jnp.searchsorted(jnp.cumsum(tallies), jnp.arange(rows * top), side="right").astype(jnp.int32)
    listing = items.reshape(top, rows).T
    listing = listing[jax.random.permutation(jax.random.fold_in(own, 1), rows)]
    offset_by = jax.random.randint(jax.random.fold_in(own, 2), (rows, 1), 0, top)
    return jnp.take_along_axis(listing, (jnp.arange(top)[None, :] + offset_by) % top, axis=1)


def shares(count, total, reach, skew, full):
    loads = [(1 << 20) // math.isqrt(rank ** skew) + 1 for rank in range(1, count + 1)]
    largest = reach if full else min(reach, max(-(-total // count), total * loads[0] // sum(loads)))
    least = 1 if total - largest >= count - 1 else 0
    holding, surplus = [largest] + [least] * (count - 1), total - largest - least * (count - 1)
    while surplus > 0:
        free = [i for i in range(1, count) if holding[i] < largest] or [i for i in range(1, count) if holding[i] < reach]
        pool, remaining = sum([loads[i] for i in free]), surplus
        for i in free:
            extra = min(reach - holding[i], max(1, remaining * loads[i] // pool), surplus)
            holding[i] = holding[i] + extra
            surplus = surplus - extra
    return np.array(holding)


def normal_values(own_key, dims, scale, limit, cuts=(), kind=jnp.bfloat16):
    factor_of = level_of(own_key, dims, cuts, -0.22, 0.18) if cuts else 1.0
    array = jax.random.normal(own_key, dims, jnp.float32) * scale * factor_of
    return jnp.minimum(jnp.maximum(array, -limit), limit).astype(kind)


def setup_inputs(seed: int = 0) -> dict:
    key_of = jax.random.split(jax.random.key(seed), 14)
    hot_ids = place_ends(ranked_ids(key_of[0], (SAMPLES, FH), HOT, 2), jax.random.fold_in(key_of[0], 3), 0, HOT - 1).astype(jnp.int32)
    cold_owner_keys = jax.random.split(jax.random.fold_in(key_of[1], 1), (SAMPLES * FC) // (B_DEV * FC))
    cold_owner_turns = jax.random.permutation(jax.random.fold_in(key_of[1], 3), (SAMPLES * FC) // (B_DEV * FC))
    cold_owner = jax.vmap(lambda own, number: shared_out(jax.random.fold_in(key_of[1], 2), own, number, B_DEV * FC, N_DP, 1, CAP, 2))(cold_owner_keys, cold_owner_turns).reshape((SAMPLES * FC, 1))
    cold_offset = place_ends(jax.random.randint(key_of[2], (SAMPLES * FC,), 0, OWN_ROWS), jax.random.fold_in(key_of[2], 1), 0, OWN_ROWS - 1).astype(jnp.int32)
    labels = place_ends((jax.random.randint(key_of[3], (SAMPLES,), 0, 2) < 1).astype(jnp.int32), jax.random.fold_in(key_of[3], 1), 0, 1)
    top_weight = normal_values(key_of[4], ((FH + FC) * E, H), ((FH + FC) * E) ** -0.5, 0.25)
    out_weight = normal_values(key_of[5], (H,), (H // 8) ** -0.5, 0.5, (), jnp.float32)
    cold_table = normal_values(key_of[6], (N_DP * OWN_ROWS, E), 1.0, 6.0, ((0, 8),), jnp.float32)
    cold_accum = jnp.clip(jnp.exp(math.log(0.01) - 4.6051702 * jax.random.uniform(key_of[7], (N_DP * OWN_ROWS, E), jnp.float32) ** level_of(key_of[7], (N_DP * OWN_ROWS, E), ((0, 8),), -0.2, 0.2)), 0.0001, 0.01)
    hot_cache = normal_values(key_of[8], (HOT, E), 1.0, 6.0, (), jnp.float32)
    hot_accum = jnp.clip(jnp.exp(jax.random.uniform(key_of[9], (HOT, E), jnp.float32, math.log(0.01), math.log(1.0))), 0.01, 1.0)
    pending = normal_values(key_of[10], (N_DP * N_REP * HOT, E), 0.05, 0.3, ((0, 32),), jnp.float32)
    refresh_blocks = draw_refresh_blocks(jax.random.fold_in(key_of[13], 71), 0)
    block_clock = place_ends(jax.random.randint(key_of[12], (HBLK,), 0, 9), jax.random.fold_in(key_of[12], 1), 0, 8).astype(jnp.int32)
    return dict(hot_ids=hot_ids, cold_owner=cold_owner, cold_offset=cold_offset, labels=labels, top_weight=top_weight, out_weight=out_weight, cold_table=cold_table, cold_accum=cold_accum, hot_cache=hot_cache, hot_accum=hot_accum, pending=pending, refresh_blocks=refresh_blocks, block_clock=block_clock)


step_size = 0.5
epsilon = 1e-08

def adagrad(table_rows, accum_rows, gradient):
    accum_next = accum_rows + gradient * gradient
    return (table_rows - step_size * gradient / (jnp.sqrt(accum_next) + epsilon), accum_next)

def reference(hot_ids, cold_owner, cold_offset, labels, top_weight, out_weight, cold_table, cold_accum, hot_cache, hot_accum, pending, refresh_blocks, block_clock):
    devices = N_DP * N_REP
    samples = hot_ids.shape[0]
    width = hot_cache.shape[1]
    hot_rows = hot_cache[hot_ids].astype(jnp.bfloat16)
    global_rows = (cold_owner[:, 0] * OWN_ROWS + cold_offset).astype(jnp.int32)
    cold_rows = cold_table[global_rows].astype(jnp.bfloat16).reshape(samples, FC, width)
    inputs = jnp.concatenate([hot_rows, cold_rows], axis=1).reshape(samples, (FH + FC) * width)
    groups = N_DP
    inputs_grouped = inputs.reshape(groups, samples // groups, (FH + FC) * width)
    labels_grouped = labels.reshape(groups, samples // groups).astype(jnp.float32)

    def per_group(carry, pieces):
        block_inputs, block_labels = pieces
        preact = jnp.dot(block_inputs, top_weight, preferred_element_type=jnp.float32)
        hidden = jax.nn.silu(preact).astype(jnp.bfloat16)
        hidden_wide = hidden.astype(jnp.float32)
        logits = jnp.dot(hidden_wide, out_weight, precision=lax.Precision.HIGHEST)
        errors = jax.nn.sigmoid(logits) - block_labels
        gates = jax.nn.sigmoid(preact)
        slope = gates * (1.0 + preact * (1.0 - gates))
        dhidden = (errors[:, None] * out_weight[None, :] * slope).astype(jnp.bfloat16)
        weight_term = lax.dot_general(block_inputs, dhidden, (((0,), (0,)), ((), ())), preferred_element_type=jnp.float32)
        head_term = jnp.dot(errors, hidden_wide, precision=lax.Precision.HIGHEST)
        dinputs = lax.dot_general(dhidden, top_weight, (((1,), (1,)), ((), ())), preferred_element_type=jnp.float32).astype(jnp.bfloat16)
        return ((carry[0] + weight_term, carry[1] + head_term), dinputs)
    start = (jnp.zeros(top_weight.shape, jnp.float32), jnp.zeros(out_weight.shape, jnp.float32))
    totals, dinputs = lax.scan(per_group, start, (inputs_grouped, labels_grouped))
    top_grad, out_grad = totals
    dinputs = dinputs.reshape(samples, FH + FC, width)
    hot_dx = dinputs[:, :FH].reshape(samples * FH, width).astype(jnp.float32)
    cold_dx = dinputs[:, FH:].reshape(samples * FC, width).astype(jnp.float32)
    cold_grad = jnp.zeros(cold_table.shape, jnp.float32).at[global_rows].add(cold_dx)
    cold_table_new, cold_accum_new = adagrad(cold_table, cold_accum, cold_grad)
    device_of = (jnp.arange(samples) // (samples // devices)).astype(jnp.int32)
    hot_index = (device_of[:, None] * HOT + hot_ids).astype(jnp.int32).reshape(-1)
    hot_grad = jnp.zeros(pending.shape, jnp.float32).at[hot_index].add(hot_dx)
    carried = (pending + hot_grad).reshape(devices, HBLK, BLOCK, width)
    picked = lax.optimization_barrier(jnp.sum(carried[:, refresh_blocks], axis=0))
    divisors = 1.0 + block_clock[refresh_blocks].astype(jnp.float32)
    flush = picked / divisors[:, None, None]
    cache_blocks = hot_cache.reshape(HBLK, BLOCK, width)
    accum_blocks = hot_accum.reshape(HBLK, BLOCK, width)
    cache_part, accum_part = adagrad(cache_blocks[refresh_blocks], accum_blocks[refresh_blocks], flush)
    hot_cache_new = cache_blocks.at[refresh_blocks].set(cache_part).reshape(HOT, width)
    hot_accum_new = accum_blocks.at[refresh_blocks].set(accum_part).reshape(HOT, width)
    pending_new = carried.at[:, refresh_blocks].set(0.0).reshape(devices * HOT, width)
    return (cold_table_new, cold_accum_new, hot_cache_new, hot_accum_new, pending_new, top_grad, out_grad)
```

```python
import functools

import jax
import jax.numpy as jnp
from jax import lax
from jax.experimental import pallas as pl
from jax.experimental.pallas import tpu as pltpu
from jax.sharding import PartitionSpec as P

BLOCK = 128
MESH = pl.DeviceIdType.MESH


step_size = 0.5
epsilon = 1e-08


def adagrad(table_rows, accum_rows, gradient):
    accum_next = accum_rows + gradient * gradient
    return (table_rows - step_size * gradient / (jnp.sqrt(accum_next) + epsilon), accum_next)


def row_to_col(row, first, step, count):
    per = 128 // step
    shape = (per, 128)
    wanted = lax.broadcasted_iota(jnp.int32, shape, 1) == step * lax.broadcasted_iota(
        jnp.int32, shape, 0
    ) + first
    pieces = []
    for i in range(count // per):
        part = jnp.broadcast_to(row[:, i * 128 : (i + 1) * 128], shape)
        pieces.append(jnp.sum(jnp.where(wanted, part, 0.0), axis=1, keepdims=True))
    return jnp.concatenate(pieces, axis=0)


def col_to_row(col):
    shape = (128, 128)
    same = lax.broadcasted_iota(jnp.int32, shape, 0) == lax.broadcasted_iota(jnp.int32, shape, 1)
    pieces = []
    for i in range(col.shape[0] // 128):
        part = jnp.broadcast_to(col[i * 128 : (i + 1) * 128], shape)
        pieces.append(jnp.sum(jnp.where(same, part, 0.0), axis=0, keepdims=True))
    return jnp.concatenate(pieces, axis=1)


def one_hot(ids, shape, dim):
    match = lax.broadcasted_iota(jnp.int32, shape, dim) == jnp.broadcast_to(ids, shape)
    return jnp.where(match, 1.0, 0.0).astype(jnp.bfloat16)


def matmul(a, b, contract=(1, 0)):
    return lax.dot_general(
        a, b, (((contract[0],), (contract[1],)), ((), ())), preferred_element_type=jnp.float32
    )


def step_kernel(
    n, piece,
    hot_ids, owner, offset, labels, out_weight, blocks, weight, table, cache, pending,
    top_out, sums_out, cold_out, carried_out,
    weight_v, table_v, cache_v, pending_v, tables, requests, asked, look, placed_t, hot_t, own_hot,
    pre, gate, hidden, inputs_t, inputs_got, dh, dh_got, outgoing, incoming,
    top_a, top_b, got_a, got_b, sum_a, sum_b, fin_a, fin_b,
    cold, cold_got, cold_half, cold_last, cold_full, hot_sum, hot_got, hot_z, hot_all,
    loads, sends, recvs,
):
    me, rep = lax.axis_index("dp"), lax.axis_index("rep")
    x, z = lax.rem(me, 2), lax.div(me, 2)
    core, y = lax.rem(rep, 2), lax.div(rep, 2)
    depth = n // 2
    f32, bf16 = jnp.float32, jnp.bfloat16

    def flip(value, on):
        return 1 - value if on else value

    def near(mask):
        return (z * 2 + flip(x, mask & 4), flip(y, mask & 2) * 2 + flip(core, mask & 1))

    def along(k):
        return (lax.rem(z + k, depth) * 2 + x, rep)

    sibling = near(1)
    peers = [lax.rem(me + j, n) for j in range(1, n)]
    sources = [lax.rem(me + n - j, n) for j in range(1, n)]
    greeted = [(peer, rep) for peer in peers] + [near(m) for m in (1, 2, 3, 5, 6, 7)]
    barrier = pltpu.get_barrier_semaphore()
    for device in greeted:
        pl.semaphore_signal(barrier, inc=1, device_id=device, device_id_type=MESH)
    local = []
    for i, (src, dst) in enumerate(
        [(table, table_v), (cache, cache_v), (weight, weight_v), (pending, pending_v)]
    ):
        local.append(pltpu.make_async_copy(src, dst, loads.at[i]))
        local[-1].start()

    count = [0]
    started = []

    def send(src, dst, device):
        k = count[0]
        count[0] += 1
        copy = pltpu.make_async_remote_copy(src, dst, sends.at[k], recvs.at[k], device, MESH)
        copy.start()
        started.append(copy)
        return copy

    local[0].wait()
    tables[me] = table_v[...].astype(bf16)
    pl.semaphore_wait(barrier, len(greeted))
    spread = [send(tables.at[me, core], tables.at[me, core], (peer, rep)) for peer in peers]

    samples = hot_ids.shape[1]
    hot_feats = hot_ids.shape[0]
    lookups = owner.shape[1]
    feats = lookups // samples
    own_rows, width = tables.shape[1] * tables.shape[2], tables.shape[3]
    cap = requests.shape[2]
    hot_rows = cache_v.shape[0]
    columns = weight_v.shape[1]
    chunk = dh.shape[2]
    chunks = columns // chunk
    hot_in = hot_feats * width

    owner_row, offset_row = owner[...].astype(f32), offset[...].astype(f32)
    owner_col = jnp.concatenate(
        [row_to_col(owner_row, k, feats, samples) for k in range(feats)], axis=0
    )
    offset_col = jnp.concatenate(
        [row_to_col(offset_row, k, feats, samples) for k in range(feats)], axis=0
    )
    lanes = lax.broadcasted_iota(jnp.int32, (lookups, 128), 1)
    matches = jnp.where(lanes == owner_col.astype(jnp.int32), 1.0, 0.0)
    square = (lookups, lookups)
    before = lax.broadcasted_iota(jnp.int32, square, 1) < lax.broadcasted_iota(
        jnp.int32, square, 0
    )
    earlier = matmul(jnp.where(before, 1.0, 0.0).astype(bf16), matches.astype(bf16))
    target = owner_col * cap + jnp.sum(earlier * matches, axis=1, keepdims=True)
    target_int = target.astype(jnp.int32)
    for o in range(n):
        slots = lax.broadcasted_iota(jnp.int32, (lookups, cap), 1) + o * cap
        asks = jnp.where(slots == target_int, offset_col, 0.0)
        requests[o] = jnp.sum(asks, axis=0, keepdims=True).astype(jnp.int32)
    asking = [send(requests.at[peer], asked.at[me], (peer, rep)) for peer in peers]
    asked[me] = requests[me]

    global_col = (owner_col * own_rows + offset_col).astype(jnp.int32)
    for o in range(n):
        look[o] = one_hot(global_col - o * own_rows, (lookups, own_rows), 1)

    hot_col = jnp.concatenate(
        [row_to_col(hot_ids[k : k + 1].astype(f32), 0, 1, samples) for k in range(hot_feats)], axis=0
    )
    local[1].wait()
    hot_found = matmul(
        one_hot(hot_col.astype(jnp.int32), (hot_feats * samples, hot_rows), 1),
        cache_v[...].astype(bf16),
    )
    hot_x = [hot_found[k * samples : (k + 1) * samples] for k in range(hot_feats)]
    local[2].wait()
    hot_wide = jnp.concatenate(hot_x, axis=1).astype(bf16)
    for h in range(chunks):
        at = slice(h * chunk, (h + 1) * chunk)
        pre[:, at] = matmul(hot_wide, weight_v[:hot_in, at])

    forwards = []
    for j, source in enumerate(sources):
        spread[j].wait_recv()
        forwards.append(send(tables.at[source, core], tables.at[source, core], sibling))

    placed_t[...] = one_hot(
        col_to_row(target).astype(jnp.int32), (n * cap, lookups), 0
    )
    hot_t[...] = one_hot(
        jnp.concatenate([hot_ids[k : k + 1] for k in range(hot_feats)], axis=1),
        (hot_rows, hot_feats * samples), 0,
    )

    def looked(o):
        return matmul(look[o], tables[o].reshape(own_rows, width))

    cold_found = looked(me)
    for j, source in enumerate(sources):
        forwards[j].wait_recv()
        cold_found += looked(source)
    cold_x = [cold_found[k * samples : (k + 1) * samples] for k in range(feats)]
    inputs_t[...] = (
        jnp.concatenate([part.T for part in hot_x + cold_x], axis=0)
        .astype(bf16)
        .reshape(inputs_t.shape)
    )
    inputs_copy = send(inputs_t.at[:, 1 - core], inputs_got, sibling)

    cold_wide = jnp.concatenate(cold_x, axis=1).astype(bf16)
    logits = jnp.zeros((samples, 1), f32)
    for h in range(chunks):
        at = slice(h * chunk, (h + 1) * chunk)
        preact = pre[:, at] + matmul(cold_wide, weight_v[hot_in:, at])
        gates = jax.nn.sigmoid(preact)
        shown = (preact * gates).astype(bf16)
        hidden[:, at] = shown
        logits += jnp.sum(shown.astype(f32) * out_weight[:, at], axis=1, keepdims=True)
        gate[:, at] = out_weight[:, at] * (gates * (1.0 + preact * (1.0 - gates)))
    errors = jax.nn.sigmoid(logits) - row_to_col(labels[...].astype(f32), 0, 1, samples)
    dh_copies = []
    for h in range(chunks):
        at = slice(h * chunk, (h + 1) * chunk)
        dh[h] = (errors * gate[:, at]).astype(bf16)
        dh_copies.append(send(dh.at[h], dh_got.at[h], sibling))

    dinputs = matmul(dh[0], weight_v[:, :chunk], (1, 1))
    for h in range(1, chunks):
        dinputs += matmul(dh[h], weight_v[:, h * chunk : (h + 1) * chunk], (1, 1))
    dinputs = dinputs.astype(bf16)
    cold_dx = jnp.concatenate(
        [dinputs[:, hot_in + k * width : hot_in + (k + 1) * width] for k in range(feats)], axis=0
    )
    outgoing[...] = matmul(placed_t[...], cold_dx).astype(bf16).reshape(outgoing.shape)
    cold_copies = [send(outgoing.at[peer], incoming.at[me], (peer, rep)) for peer in peers]
    incoming[me] = outgoing[me]

    def top_part(h):
        mine = inputs_t[:, core].reshape(-1, samples)
        both = matmul(mine, dh[h])
        dh_copies[h].wait_recv()
        return both + matmul(inputs_got[...].reshape(-1, samples), dh_got[h])

    quads = [(flip(x, m & 4) * 2 + flip(y, m & 2), near(m)) for m in (2, 4, 6)]
    my_quad = x * 2 + y
    zs = [(lax.rem(z + k, depth), along(k)) for k in range(1, depth)]
    inputs_copy.wait_recv()
    half = columns // 2
    for h in range(chunks // 2, chunks):
        at = slice(h * chunk - half, (h + 1) * chunk - half)
        top_b[:, :, :, at] = top_part(h).reshape(top_b.shape[:3] + (chunk,))
    b_copies = [send(top_b.at[to], got_b.at[i], device) for i, (to, device) in enumerate(zs)]
    for h in range(chunks // 2):
        at = slice(h * chunk, (h + 1) * chunk)
        top_a[:, :, :, at] = top_part(h).reshape(top_a.shape[:3] + (chunk,))
    a_copies = [
        send(top_a.at[:, to], got_a.at[i], device) for i, (to, device) in enumerate(quads)
    ]

    hot_dx = jnp.concatenate(
        [dinputs[:, k * width : (k + 1) * width] for k in range(hot_feats)], axis=0
    )
    local[3].wait()
    carried_out[...] = pending_v[...] + matmul(hot_t[...], hot_dx)
    total_rows = hot_sum.shape[0]
    picks = blocks.shape[0]
    for k in range(picks):
        wanted = jnp.full((BLOCK, width), blocks[k])
        picked = carried_out[:BLOCK, :]
        for b in range(1, hot_rows // BLOCK):
            picked = jnp.where(wanted == b, carried_out[b * BLOCK : (b + 1) * BLOCK, :], picked)
        hot_sum[k * BLOCK : (k + 1) * BLOCK, :] = picked
    base = picks * BLOCK
    hot_sum[base:, :] = jnp.zeros((total_rows - base, width), f32)
    for h in range(chunks):
        head = jnp.sum(
            errors * hidden[:, h * chunk : (h + 1) * chunk].astype(f32), axis=0, keepdims=True
        )
        for i in range(chunk // width):
            row = base + h * (chunk // width) + i
            hot_sum[row : row + 1, :] = head[:, i * width : (i + 1) * width]

    def piece_of(ref, q):
        return ref.at[pl.ds(pl.multiple_of(q * piece, 8), piece)]

    def spot(m):
        return flip(x, m & 4) * 4 + flip(y, m & 2) * 2 + flip(core, m & 1)

    h_copies = [
        send(piece_of(hot_sum, spot(m)), hot_got.at[m - 1], near(m)) for m in range(1, 8)
    ]

    for o in range(n - 1):
        asking[o].wait_recv()
    for o in range(n):
        own_hot[:, o * cap : (o + 1) * cap] = one_hot(asked[o], (own_rows, cap), 0)

    for copy in h_copies:
        copy.wait_recv()
    mine = piece_of(hot_sum, spot(0))[...]
    for m in range(7):
        mine += hot_got[m]
    hot_z[z] = mine
    hz_copies = [send(hot_z.at[z], hot_z.at[z], device) for _, device in zs]

    for copy in cold_copies:
        copy.wait_recv()
    cold[...] = matmul(own_hot[...], incoming[...].reshape(n * cap, width)).reshape(cold.shape)
    cold_copy = send(cold.at[1 - core], cold_got, sibling)

    for copy in b_copies:
        copy.wait_recv()
    part = top_b[z]
    for i in range(depth - 1):
        part += got_b[i]
    sum_b[...] = part
    b_copies = [send(sum_b.at[to], fin_b.at[i], device) for i, (to, device) in enumerate(quads)]

    cold_copy.wait_recv()
    cold_half[...] = cold[core] + cold_got[...]
    cold_copy = send(cold_half, cold_last, near(2))

    for copy in a_copies:
        copy.wait_recv()
    part = top_a[:, my_quad]
    for i in range(3):
        part += got_a[i]
    sum_a[...] = part
    a_copies = [send(sum_a.at[to], fin_a.at[i], device) for i, (to, device) in enumerate(zs)]

    for copy in hz_copies:
        copy.wait_recv()
    final = hot_z[0]
    for k in range(1, depth):
        final += hot_z[k]
    piece_of(hot_all, spot(0))[...] = final
    hot_copies = [
        send(piece_of(hot_all, spot(0)), piece_of(hot_all, spot(0)), near(m)) for m in range(1, 8)
    ]

    cold_copy.wait_recv()
    cold_full[core] = cold_half[...] + cold_last[...]
    cold_copy = send(cold_full.at[core], cold_full.at[core], sibling)

    for copy in b_copies:
        copy.wait_recv()
    part = sum_b[my_quad]
    for i in range(3):
        part += fin_b[i]
    top_out[:, half:] = part
    for copy in a_copies:
        copy.wait_recv()
    part = sum_a[z]
    for i in range(depth - 1):
        part += fin_a[i]
    top_out[:, :half] = part
    for copy in hot_copies:
        copy.wait_recv()
    sums_out[...] = hot_all[...]
    cold_copy.wait_recv()
    cold_out[...] = cold_full[...].reshape(cold_out.shape)
    for copy in started:
        copy.wait_send()


def step(hot_ids, owner, offset, labels, out_weight, blocks, weight, table, cache, pending, n, cap):
    hot_feats, samples = hot_ids.shape
    lookups = owner.shape[1]
    features, columns = weight.shape
    own_rows, width = table.shape
    hot_rows = cache.shape[0]
    depth = n // 2
    rows = features // (4 * n)
    half, chunk = columns // 2, columns // 4
    sum_rows = blocks.shape[0] * BLOCK + columns // width
    piece = -(-sum_rows // 64) * 8
    f32 = lambda *shape: pltpu.VMEM(shape, jnp.float32)
    b16 = lambda *shape: pltpu.VMEM(shape, jnp.bfloat16)
    i32 = lambda *shape: pltpu.VMEM(shape, jnp.int32)
    copies = 4 * (n - 1) + 1 + 4 + 2 * (depth - 1 + 3) + 7 + depth - 1 + 7 + 3
    vmem = pl.BlockSpec(memory_space=pltpu.VMEM)
    hbm = pl.BlockSpec(memory_space=pl.ANY)
    out = lambda *shape: jax.ShapeDtypeStruct(shape, jnp.float32)
    return pl.pallas_call(
        functools.partial(step_kernel, n, piece),
        out_shape=(
            out(rows, columns), out(8 * piece, width), out(own_rows, width), out(hot_rows, width)
        ),
        in_specs=[vmem] * 5 + [pl.BlockSpec(memory_space=pltpu.SMEM)] + [hbm] * 4,
        out_specs=(vmem,) * 4,
        scratch_shapes=[
            b16(features, columns), f32(2, own_rows // 2, width), f32(hot_rows, width),
            f32(hot_rows, width), b16(n, 2, own_rows // 2, width), i32(n, 1, cap), i32(n, 1, cap),
            b16(n, lookups, own_rows), b16(n * cap, lookups), b16(hot_rows, hot_feats * samples),
            b16(own_rows, n * cap),
            f32(samples, columns), f32(samples, columns), b16(samples, columns),
            b16(4 * depth, 2, rows, samples), b16(4 * depth, rows, samples),
            b16(4, samples, chunk), b16(4, samples, chunk),
            b16(n, cap, width), b16(n, cap, width),
            f32(depth, 4, rows, half), f32(depth, 4, rows, half),
            f32(3, depth, rows, half), f32(depth - 1, 4, rows, half),
            f32(depth, rows, half), f32(4, rows, half),
            f32(depth - 1, rows, half), f32(3, rows, half),
            f32(2, own_rows // 2, width), f32(own_rows // 2, width), f32(own_rows // 2, width),
            f32(own_rows // 2, width), f32(2, own_rows // 2, width),
            f32(8 * piece, width), f32(7, piece, width), f32(depth, piece, width),
            f32(8 * piece, width),
            pltpu.SemaphoreType.DMA((4,)),
            pltpu.SemaphoreType.DMA((copies,)),
            pltpu.SemaphoreType.DMA((copies,)),
        ],
        compiler_params=pltpu.CompilerParams(collective_id=0, has_side_effects=True),
    )(
        hot_ids, owner, offset, labels, out_weight, blocks,
        weight, table.reshape(2, own_rows // 2, width), cache, pending,
    )


def update_kernel(
    blocks, clock, top, sums, cold, carried, table, accum, cache, hot_accum,
    table_out, accum_out, cache_out, hot_accum_out, pending_out, top_out, head_out,
):
    table_out[...], accum_out[...] = adagrad(table[...], accum[...], cold[...])
    cache_out[...] = cache[...]
    hot_accum_out[...] = hot_accum[...]
    pending_out[...] = carried[...]
    picks = blocks.shape[0]
    for k in range(picks):
        rows = pl.ds(pl.multiple_of(blocks[k] * BLOCK, BLOCK), BLOCK)
        divisor = 1.0 + clock[blocks[k]].astype(jnp.float32)
        flush = sums[k * BLOCK : (k + 1) * BLOCK, :] / divisor
        cache_next, accum_next = adagrad(cache[rows, :], hot_accum[rows, :], flush)
        cache_out[rows, :] = cache_next
        hot_accum_out[rows, :] = accum_next
        pending_out[rows, :] = jnp.zeros((BLOCK, cache.shape[1]), jnp.float32)
    top_out[...] = top[...]
    head_out[...] = sums[picks * BLOCK : picks * BLOCK + head_out.shape[0], :]


def update(blocks, clock, top, sums, cold, carried, table, accum, cache, hot_accum):
    head_rows = top.shape[1] // cache.shape[1]
    smem = pl.BlockSpec(memory_space=pltpu.SMEM)
    vmem = pl.BlockSpec(memory_space=pltpu.VMEM)
    like = lambda a: jax.ShapeDtypeStruct(a.shape, a.dtype)
    return pl.pallas_call(
        update_kernel,
        out_shape=(
            like(table), like(accum), like(cache), like(hot_accum), like(carried), like(top),
            jax.ShapeDtypeStruct((head_rows, cache.shape[1]), jnp.float32),
        ),
        in_specs=[smem] * 2 + [vmem] * 8,
        out_specs=(vmem,) * 7,
    )(blocks, clock, top, sums, cold, carried, table, accum, cache, hot_accum)


def suits(n, rep_n, top_weight, hot_ids, cold_offset, hot_cache, cold_table):
    features, columns = top_weight.shape
    samples, lookups, width = hot_ids.shape[0], cold_offset.shape[0], hot_cache.shape[1]
    return (
        rep_n == 4
        and n % 2 == 0
        and 4 <= n <= 16
        and features % (16 * 4 * n) == 0
        and columns % 1024 == 0
        and samples % 128 == 0
        and lookups == 2 * samples
        and width == 128
        and (2 * lookups // n) % 128 == 0
        and hot_cache.shape[0] % 128 == 0
        and cold_table.shape[0] % 256 == 0
    )


def direct(
    n, hot_ids, cold_owner, cold_offset, labels, top_weight, out_weight, cold_table, cold_accum,
    hot_cache, hot_accum, pending, refresh_blocks, block_clock,
):
    cap = 2 * cold_offset.shape[0] // n
    top, sums, cold, carried = step(
        hot_ids.T, cold_owner.reshape(1, -1), cold_offset.reshape(1, -1), labels.reshape(1, -1),
        out_weight.reshape(1, -1), refresh_blocks, top_weight, cold_table, hot_cache, pending, n, cap,
    )
    results = update(
        refresh_blocks, block_clock, top, sums, cold, carried, cold_table, cold_accum, hot_cache,
        hot_accum,
    )
    return results[:6] + (results[6].reshape(-1),)


def local(
    hot_ids,
    cold_owner,
    cold_offset,
    labels,
    top_weight,
    out_weight,
    cold_table,
    cold_accum,
    hot_cache,
    hot_accum,
    pending,
    refresh_blocks,
    block_clock,
):
    n, rep_n = lax.axis_size("dp"), lax.axis_size("rep")
    if suits(n, rep_n, top_weight, hot_ids, cold_offset, hot_cache, cold_table):
        return direct(
            n, hot_ids, cold_owner, cold_offset, labels, top_weight, out_weight, cold_table,
            cold_accum, hot_cache, hot_accum, pending, refresh_blocks, block_clock,
        )
    width = hot_cache.shape[1]
    samples = hot_ids.shape[0]
    hot_feats = hot_ids.shape[1]
    lookups = cold_offset.shape[0]
    cold_feats = lookups // samples
    owners_count = lax.axis_size("dp")
    capacity = max(2, 2 * lookups // owners_count)
    owners = cold_owner[:, 0]
    matches = (owners[:, None] == jnp.arange(owners_count, dtype=jnp.int32)[None, :]).astype(
        jnp.int32
    )
    before = jnp.arange(lookups)[:, None] > jnp.arange(lookups)[None, :]
    earlier = jnp.dot(
        before.astype(jnp.bfloat16),
        matches.astype(jnp.bfloat16),
        preferred_element_type=jnp.float32,
    ).astype(jnp.int32)
    positions = jnp.sum(earlier * matches, axis=1)
    targets = owners * capacity + positions
    places = jnp.arange(owners_count * capacity, dtype=jnp.int32)
    placed = targets[:, None] == places[None, :]
    requests = jnp.sum(jnp.where(placed, cold_offset[:, None], 0), axis=0)
    placed = placed.astype(jnp.bfloat16)
    requests = requests.reshape(owners_count, capacity)
    asked = lax.all_to_all(requests, "dp", split_axis=0, concat_axis=0, tiled=True)
    found = cold_table[asked].astype(jnp.bfloat16)
    returned = lax.all_to_all(found, "dp", split_axis=0, concat_axis=0, tiled=True)
    cold_rows = jnp.dot(
        placed,
        returned.reshape(owners_count * capacity, width),
        preferred_element_type=jnp.float32,
    ).astype(jnp.bfloat16)
    cold_rows = cold_rows.reshape(samples, cold_feats, width)
    hot_rows = hot_cache[hot_ids].astype(jnp.bfloat16)
    inputs = jnp.concatenate([hot_rows, cold_rows], axis=1).reshape(
        samples, (hot_feats + cold_feats) * width
    )
    preact = jnp.dot(inputs, top_weight, preferred_element_type=jnp.float32)
    hidden = jax.nn.silu(preact).astype(jnp.bfloat16)
    hidden_wide = hidden.astype(jnp.float32)
    logits = jnp.dot(hidden_wide, out_weight, precision=lax.Precision.HIGHEST)
    errors = jax.nn.sigmoid(logits) - labels.astype(jnp.float32)
    gates = jax.nn.sigmoid(preact)
    slope = gates * (1.0 + preact * (1.0 - gates))
    dhidden = (errors[:, None] * out_weight[None, :] * slope).astype(jnp.bfloat16)
    head_term = jnp.dot(errors, hidden_wide, precision=lax.Precision.HIGHEST)
    top_part = lax.dot_general(
        inputs, dhidden, (((0,), (0,)), ((), ())), preferred_element_type=jnp.float32
    )
    dinputs = lax.dot_general(
        dhidden, top_weight, (((1,), (1,)), ((), ())), preferred_element_type=jnp.float32
    ).astype(jnp.bfloat16)
    dinputs = dinputs.reshape(samples, hot_feats + cold_feats, width)
    cold_dx = dinputs[:, hot_feats:].reshape(lookups, width)
    outgoing = lax.dot_general(
        placed, cold_dx, (((0,), (0,)), ((), ())), preferred_element_type=jnp.float32
    ).astype(jnp.bfloat16)
    outgoing = outgoing.reshape(owners_count, capacity, width)
    own_rows = cold_table.shape[0]
    quarter = own_rows // lax.axis_size("rep")
    hot_count = hot_cache.shape[0]
    blocks_count = hot_count // BLOCK
    hot_dx = dinputs[:, :hot_feats].reshape(samples * hot_feats, width)
    hot_named = (
        jnp.arange(hot_count, dtype=jnp.int32)[:, None] == hot_ids.reshape(-1)[None, :]
    ).astype(jnp.bfloat16)
    hot_grad = jnp.dot(hot_named, hot_dx, preferred_element_type=jnp.float32)
    carried = (pending + hot_grad).reshape(blocks_count, BLOCK, width)
    picked = carried[refresh_blocks]
    divisors = 1.0 + block_clock.astype(jnp.float32)
    named = refresh_blocks[:, None] == jnp.arange(blocks_count, dtype=jnp.int32)[None, :]
    refreshed = jnp.any(named, axis=0)[:, None, None]
    cache_blocks = hot_cache.reshape(blocks_count, BLOCK, width)
    accum_blocks = hot_accum.reshape(blocks_count, BLOCK, width)
    incoming = lax.all_to_all(outgoing, "dp", split_axis=0, concat_axis=0, tiled=True)
    cold_grad = (
        jnp.zeros((own_rows, width), jnp.float32)
        .at[asked.reshape(-1)]
        .add(incoming.reshape(-1, width).astype(jnp.float32))
    )
    cold_share = lax.psum_scatter(cold_grad, "rep", scatter_dimension=0, tiled=True)
    offset_rows = lax.axis_index("rep") * quarter
    table_share = lax.dynamic_slice_in_dim(cold_table, offset_rows, quarter, 0)
    accum_share = lax.dynamic_slice_in_dim(cold_accum, offset_rows, quarter, 0)
    table_updated, accum_updated = adagrad(table_share, accum_share, cold_share)
    cold_table_new, cold_accum_new = (
        lax.all_gather(table_updated, "rep", axis=0, tiled=True),
        lax.all_gather(accum_updated, "rep", axis=0, tiled=True),
    )
    top_grad = lax.psum_scatter(top_part, ("dp", "rep"), scatter_dimension=0, tiled=True)
    picked_sum, out_grad = lax.psum((picked, head_term), ("dp", "rep"))
    block_sums = jnp.zeros((), jnp.float32)
    for k in range(refresh_blocks.shape[0]):
        block_sums = jnp.where(named[k][:, None, None], picked_sum[k][None], block_sums)
    flush = block_sums / divisors[:, None, None]
    cache_next, accum_next = adagrad(cache_blocks, accum_blocks, flush)
    hot_cache_new = jnp.where(refreshed, cache_next, cache_blocks).reshape(hot_count, width)
    hot_accum_new = jnp.where(refreshed, accum_next, accum_blocks).reshape(hot_count, width)
    pending_new = jnp.where(refreshed, 0.0, carried).reshape(hot_count, width)
    return (
        cold_table_new,
        cold_accum_new,
        hot_cache_new,
        hot_accum_new,
        pending_new,
        top_grad,
        out_grad,
    )


def solution(mesh):
    in_specs = (
        P(("dp", "rep"), None),
        P(("dp", "rep"), None),
        P(("dp", "rep")),
        P(("dp", "rep")),
        P(),
        P(),
        P("dp", None),
        P("dp", None),
        P(),
        P(),
        P(("dp", "rep"), None),
        P(),
        P(),
    )
    out_specs = (
        P("dp", None),
        P("dp", None),
        P(),
        P(),
        P(("dp", "rep"), None),
        P(("dp", "rep"), None),
        P(),
    )
    return jax.shard_map(local, mesh=mesh, in_specs=in_specs, out_specs=out_specs, check_vma=False)
```

```python
import functools

import jax
import jax.numpy as jnp
from jax import lax
from jax.experimental import pallas as pl
from jax.experimental.pallas import tpu as pltpu
from jax.sharding import PartitionSpec as P

BLOCK = 128
VMEM_LIMIT = 40 * 1024 * 1024
MESH = pl.DeviceIdType.MESH


step_size = 0.5
epsilon = 1e-08


def adagrad(table_rows, accum_rows, gradient):
    accum_next = accum_rows + gradient * gradient
    return (table_rows - step_size * gradient / (jnp.sqrt(accum_next) + epsilon), accum_next)


def row_to_col(row, first, step, count):
    per = 128 // step
    shape = (per, 128)
    wanted = lax.broadcasted_iota(jnp.int32, shape, 1) == step * lax.broadcasted_iota(
        jnp.int32, shape, 0
    ) + first
    pieces = []
    for i in range(count // per):
        part = jnp.broadcast_to(row[:, i * 128 : (i + 1) * 128], shape)
        pieces.append(jnp.sum(jnp.where(wanted, part, 0.0), axis=1, keepdims=True))
    return jnp.concatenate(pieces, axis=0)


def col_to_row(col):
    shape = (128, 128)
    same = lax.broadcasted_iota(jnp.int32, shape, 0) == lax.broadcasted_iota(jnp.int32, shape, 1)
    pieces = []
    for i in range(col.shape[0] // 128):
        part = jnp.broadcast_to(col[i * 128 : (i + 1) * 128], shape)
        pieces.append(jnp.sum(jnp.where(same, part, 0.0), axis=0, keepdims=True))
    return jnp.concatenate(pieces, axis=1)


def one_hot(ids, shape, dim):
    match = lax.broadcasted_iota(jnp.int32, shape, dim) == jnp.broadcast_to(ids, shape)
    return jnp.where(match, 1.0, 0.0).astype(jnp.bfloat16)


def matmul(a, b, contract=(1, 0)):
    return lax.dot_general(
        a, b, (((contract[0],), (contract[1],)), ((), ())), preferred_element_type=jnp.float32
    )


def step_kernel(
    n, piece,
    hot_ids_in, owner_in, offset_in, labels_in, out_weight_in, blocks_in, weight, table, cache,
    pending,
    top_out, sums_out, cold_out, carried_out,
    hot_ids, owner, offset, labels, out_weight, blocks,
    weight_v, table_v, table_all, cache_v, pending_v, tables, requests, asked, look, placed_t, hot_t, own_hot,
    pre, gate, hidden, inputs_t, inputs_got, dh, dh_got, outgoing, incoming,
    top, leave, got_1, part_1, got_2, part_2, got_3,
    cold, cold_got, cold_half, cold_last, cold_full, hot_sum, hot_got, hot_mid, hot_near, hot_z,
    hot_all,
    loads, sends, recvs,
):
    me, rep = lax.axis_index("dp"), lax.axis_index("rep")
    x, z = lax.rem(me, 2), lax.div(me, 2)
    core, y = lax.rem(rep, 2), lax.div(rep, 2)
    depth = n // 2
    f32, bf16 = jnp.float32, jnp.bfloat16

    def flip(value, on):
        return 1 - value if on else value

    def near(mask):
        return (z * 2 + flip(x, mask & 4), flip(y, mask & 2) * 2 + flip(core, mask & 1))

    def along(k):
        return lax.rem(z + k, depth) * 2 + x

    sibling, over_x, over_y = near(1), near(4), near(2)
    peers = [lax.rem(me + j, n) for j in range(1, n)]
    sources = [lax.rem(me + n - j, n) for j in range(1, n)]
    greeted = [(peer, rep) for peer in peers] + [sibling, over_y, near(6)]
    barrier = pltpu.get_barrier_semaphore()
    for device in greeted:
        pl.semaphore_signal(barrier, inc=1, device_id=device, device_id_type=MESH)
    local = []
    for src, dst in [
        (table.at[rep], table_v.at[rep]), (owner_in, owner), (offset_in, offset),
        (table, table_all), (hot_ids_in, hot_ids), (cache, cache_v),
        (weight, weight_v), (labels_in, labels), (out_weight_in, out_weight), (blocks_in, blocks),
        (pending, pending_v),
    ]:
        local.append(pltpu.make_async_copy(src, dst, loads.at[len(local)]))
        local[-1].start()

    count = [0]
    started = []

    def send(src, dst, device):
        k = count[0]
        count[0] += 1
        copy = pltpu.make_async_remote_copy(src, dst, sends.at[k], recvs.at[k], device, MESH)
        copy.start()
        started.append(copy)
        return copy

    def same(ref, device):
        return send(ref, ref, device)

    local[0].wait()
    tables[me, rep] = table_v[rep].astype(bf16)
    pl.semaphore_wait(barrier, len(greeted))
    mine = tables.at[me, rep]
    order = sorted(range(1, depth), key=lambda k: abs(2 * k - depth))
    z_table = {k: same(mine, (along(k), rep)) for k in order}
    x_table = same(mine, over_x)

    samples = hot_ids.shape[1]
    hot_feats = hot_ids.shape[0]
    lookups = owner.shape[1]
    feats = lookups // samples
    own_rows, width = tables.shape[1] * tables.shape[2], tables.shape[3]
    cap = requests.shape[2]
    hot_rows = cache_v.shape[0]
    columns = weight_v.shape[1]
    chunk = dh.shape[2]
    chunks = columns // chunk
    hot_in = hot_feats * width

    local[1].wait()
    local[2].wait()
    owner_row, offset_row = owner[...].astype(f32), offset[...].astype(f32)
    owner_col = jnp.concatenate(
        [row_to_col(owner_row, k, feats, samples) for k in range(feats)], axis=0
    )
    offset_col = jnp.concatenate(
        [row_to_col(offset_row, k, feats, samples) for k in range(feats)], axis=0
    )
    lanes = lax.broadcasted_iota(jnp.int32, (lookups, 128), 1)
    matches = jnp.where(lanes == owner_col.astype(jnp.int32), 1.0, 0.0)
    square = (lookups, lookups)
    before = lax.broadcasted_iota(jnp.int32, square, 1) < lax.broadcasted_iota(
        jnp.int32, square, 0
    )
    earlier = matmul(jnp.where(before, 1.0, 0.0).astype(bf16), matches.astype(bf16))
    target = owner_col * cap + jnp.sum(earlier * matches, axis=1, keepdims=True)
    target_int = target.astype(jnp.int32)
    for o in range(n):
        slots = lax.broadcasted_iota(jnp.int32, (lookups, cap), 1) + o * cap
        asks = jnp.where(slots == target_int, offset_col, 0.0)
        requests[o] = jnp.sum(asks, axis=0, keepdims=True).astype(jnp.int32)
    asking = [send(requests.at[peer], asked.at[me], (peer, rep)) for peer in peers]
    asked[me] = requests[me]

    global_col = (owner_col * own_rows + offset_col).astype(jnp.int32)
    for o in range(n):
        look[o] = one_hot(global_col - o * own_rows, (lookups, own_rows), 1)

    def relay(copy, source, *devices):
        copy.wait_recv()
        return [same(tables.at[source, rep], device) for device in devices]

    def looked(o):
        return matmul(look[o], tables[o].reshape(own_rows, width))

    order = order[::-1]
    x_source = z * 2 + 1 - x
    z_source = {k: lax.rem(z + depth - k, depth) * 2 + x for k in order}
    far_source = {k: lax.rem(z + depth - k, depth) * 2 + 1 - x for k in order}
    others = [x_source] + [z_source[k] for k in order] + [far_source[k] for k in order]
    by_y, by_core, y_core, by_x = {}, {}, {}, {}
    by_y[0], by_core[0] = relay(x_table, x_source, over_y, sibling)

    local[4].wait()
    hot_col = jnp.concatenate(
        [row_to_col(hot_ids[k : k + 1].astype(f32), 0, 1, samples) for k in range(hot_feats)], axis=0
    )
    local[5].wait()
    hot_found = matmul(
        one_hot(hot_col.astype(jnp.int32), (hot_feats * samples, hot_rows), 1),
        cache_v[...].astype(bf16),
    )
    hot_x = [hot_found[k * samples : (k + 1) * samples] for k in range(hot_feats)]

    for i, k in enumerate(order):
        by_x[k], by_y[1 + i], by_core[1 + i] = relay(
            z_table[k], z_source[k], over_x, over_y, sibling
        )

    local[6].wait()
    hot_wide = jnp.concatenate(hot_x, axis=1).astype(bf16)
    for h in range(chunks):
        at = slice(h * chunk, (h + 1) * chunk)
        pre[:, at] = matmul(hot_wide, weight_v[:hot_in, at])
    local[3].wait()
    for i in range(1, 4):
        tables[me, lax.rem(rep + i, 4)] = table_all[lax.rem(rep + i, 4)].astype(bf16)

    def relay_y(i):
        by_y[i].wait_recv()
        y_core[i] = same(tables.at[others[i], (1 - y) * 2 + core], sibling)

    relay_y(0)
    cold_found = looked(me)
    for i, k in enumerate(order):
        by_y[depth + i], by_core[depth + i] = relay(by_x[k], far_source[k], over_y, sibling)
        relay_y(1 + i)
    placed_t[...] = one_hot(
        col_to_row(target).astype(jnp.int32), (n * cap, lookups), 0
    )
    hot_t[...] = one_hot(
        jnp.concatenate([hot_ids[k : k + 1] for k in range(hot_feats)], axis=1),
        (hot_rows, hot_feats * samples), 0,
    )
    for i in range(depth, n - 1):
        relay_y(i)
        j = i - depth
        by_core[j].wait_recv()
        y_core[j].wait_recv()
        cold_found += looked(others[j])
    for j in range(depth - 1, n - 1):
        by_core[j].wait_recv()
        y_core[j].wait_recv()
        cold_found += looked(others[j])
    cold_x = [cold_found[k * samples : (k + 1) * samples] for k in range(feats)]
    inputs_t[...] = (
        jnp.concatenate([part.T for part in hot_x + cold_x], axis=0)
        .astype(bf16)
        .reshape(inputs_t.shape)
    )
    inputs_copy = send(inputs_t.at[:, 1 - core], inputs_got, sibling)

    local[7].wait()
    local[8].wait()
    cold_wide = jnp.concatenate(cold_x, axis=1).astype(bf16)
    logits = jnp.zeros((samples, 1), f32)
    for h in range(chunks):
        at = slice(h * chunk, (h + 1) * chunk)
        preact = pre[:, at] + matmul(cold_wide, weight_v[hot_in:, at])
        gates = jax.nn.sigmoid(preact)
        shown = (preact * gates).astype(bf16)
        hidden[:, at] = shown
        logits += jnp.sum(shown.astype(f32) * out_weight[:, at], axis=1, keepdims=True)
        gate[:, at] = out_weight[:, at] * (gates * (1.0 + preact * (1.0 - gates)))
    errors = jax.nn.sigmoid(logits) - row_to_col(labels[...].astype(f32), 0, 1, samples)
    dh_copies = []
    for h in range(chunks):
        at = slice(h * chunk, (h + 1) * chunk)
        dh[h] = (errors * gate[:, at]).astype(bf16)
        dh_copies.append(send(dh.at[h], dh_got.at[h], sibling))

    dinputs = matmul(dh[0], weight_v[:, :chunk], (1, 1))
    for h in range(1, chunks):
        dinputs += matmul(dh[h], weight_v[:, h * chunk : (h + 1) * chunk], (1, 1))
    dinputs = dinputs.astype(bf16)
    cold_dx = jnp.concatenate(
        [dinputs[:, hot_in + k * width : hot_in + (k + 1) * width] for k in range(feats)], axis=0
    )
    outgoing[...] = matmul(placed_t[...], cold_dx).astype(bf16).reshape(outgoing.shape)
    cold_copies = [send(outgoing.at[peer], incoming.at[me], (peer, rep)) for peer in peers]
    incoming[me] = outgoing[me]

    hot_dx = jnp.concatenate(
        [dinputs[:, k * width : (k + 1) * width] for k in range(hot_feats)], axis=0
    )
    local[9].wait()
    local[10].wait()
    carried_out[...] = pending_v[...] + matmul(hot_t[...], hot_dx)
    total_rows = hot_sum.shape[0]
    picks = blocks.shape[0]
    for k in range(picks):
        wanted = jnp.full((BLOCK, width), blocks[k])
        picked = carried_out[:BLOCK, :]
        for b in range(1, hot_rows // BLOCK):
            picked = jnp.where(wanted == b, carried_out[b * BLOCK : (b + 1) * BLOCK, :], picked)
        hot_sum[k * BLOCK : (k + 1) * BLOCK, :] = picked
    base = picks * BLOCK
    hot_sum[base:, :] = jnp.zeros((total_rows - base, width), f32)
    for h in range(chunks):
        head = jnp.sum(
            errors * hidden[:, h * chunk : (h + 1) * chunk].astype(f32), axis=0, keepdims=True
        )
        for i in range(chunk // width):
            row = base + h * (chunk // width) + i
            hot_sum[row : row + 1, :] = head[:, i * width : (i + 1) * width]

    def part_of(ref, q, rows):
        return ref.at[pl.ds(pl.multiple_of(q * rows, 8), rows)]

    hot_copy = send(part_of(hot_sum, 1 - core, 4 * piece), hot_got, sibling)
    my_quad = x * 2 + y
    quads = [(flip(x, m & 4) * 2 + flip(y, m & 2), near(m)) for m in (2, 4, 6)]

    inputs_copy.wait_recv()

    def first_step(h):
        both = matmul(inputs_t[:, core].reshape(-1, samples), dh[h])
        dh_copies[h].wait_recv()
        both += matmul(inputs_got[...].reshape(-1, samples), dh_got[h])
        top[h] = both.reshape(top.shape[1:])
        leaving = top[h, :, 1 - x] if h % 2 == 0 else top[h, :, :, 1 - y]
        leave[h] = leaving.astype(bf16)
        return send(leave.at[h], got_1.at[h], over_x if h % 2 == 0 else over_y)

    def second_step(h):
        first[h].wait_recv()
        kept = top[h, :, x] if h % 2 == 0 else top[h, :, :, y]
        part_1[h] = kept + got_1[h].astype(f32)
        if h % 2 == 0:
            return send(part_1.at[h, :, 1 - y], got_2.at[h], over_y)
        return send(part_1.at[h, :, 1 - x], got_2.at[h], over_x)

    def third_step(h):
        second[h].wait_recv()
        part_2[h] = part_1[h, :, y if h % 2 == 0 else x] + got_2[h]
        return [
            send(part_2.at[h, lax.rem(z + k, depth)], got_3.at[h, k - 1], (along(k), rep))
            for k in range(1, depth)
        ]

    first = [first_step(h) for h in range(chunks)]

    for o in range(n - 1):
        asking[o].wait_recv()
    for o in range(n):
        own_hot[:, o * cap : (o + 1) * cap] = one_hot(asked[o], (own_rows, cap), 0)

    hot_copy.wait_recv()
    hot_mid[...] = part_of(hot_sum, core, 4 * piece)[...] + hot_got[...]
    hot_copies = [
        send(part_of(hot_mid, q, piece), hot_near.at[i], device)
        for i, (q, device) in enumerate(quads)
    ]

    second = [second_step(h) for h in range(chunks)]

    for copy in hot_copies:
        copy.wait_recv()
    hot_z[z] = part_of(hot_mid, my_quad, piece)[...] + hot_near[0] + hot_near[1] + hot_near[2]
    hot_copies = [same(hot_z.at[z], (along(k), rep)) for k in range(1, depth)]

    for copy in cold_copies:
        copy.wait_recv()
    cold[...] = matmul(own_hot[...], incoming[...].reshape(n * cap, width)).reshape(cold.shape)
    cold_copy = send(cold.at[1 - core], cold_got, sibling)

    third = [third_step(h) for h in range(chunks)]

    cold_copy.wait_recv()
    cold_half[...] = cold[core] + cold_got[...]
    cold_copy = send(cold_half, cold_last, over_y)

    for copy in hot_copies:
        copy.wait_recv()
    final = hot_z[0]
    for k in range(1, depth):
        final += hot_z[k]
    ours = core * 4 + my_quad
    part_of(hot_all, ours, piece)[...] = final
    hot_copies = [same(part_of(hot_all, ours, piece), device) for _, device in quads]

    cold_copy.wait_recv()
    cold_full[core] = cold_half[...] + cold_last[...]
    cold_copy = same(cold_full.at[core], sibling)

    for copy in hot_copies:
        copy.wait_recv()
    hot_copy = same(part_of(hot_all, core, 4 * piece), sibling)

    for h in range(chunks):
        for copy in third[h]:
            copy.wait_recv()
        part = part_2[h, z]
        for k in range(depth - 1):
            part += got_3[h, k]
        top_out[:, h * chunk : (h + 1) * chunk] = part
    cold_copy.wait_recv()
    cold_out[...] = cold_full[...].reshape(cold_out.shape)
    hot_copy.wait_recv()
    sums_out[...] = hot_all[...]
    for copy in started:
        copy.wait_send()


def step(hot_ids, owner, offset, labels, out_weight, blocks, weight, table, cache, pending, n, cap):
    hot_feats, samples = hot_ids.shape
    lookups = owner.shape[1]
    features, columns = weight.shape
    own_rows, width = table.shape
    hot_rows = cache.shape[0]
    depth = n // 2
    rows = features // (4 * n)
    chunk = columns // 4
    sum_rows = blocks.shape[0] * BLOCK + columns // width
    piece = -(-sum_rows // 64) * 8
    f32 = lambda *shape: pltpu.VMEM(shape, jnp.float32)
    b16 = lambda *shape: pltpu.VMEM(shape, jnp.bfloat16)
    i32 = lambda *shape: pltpu.VMEM(shape, jnp.int32)
    copies = 6 * n + 8 * depth + 32
    vmem = pl.BlockSpec(memory_space=pltpu.VMEM)
    hbm = pl.BlockSpec(memory_space=pltpu.HBM)
    out = lambda *shape: jax.ShapeDtypeStruct(shape, jnp.float32)
    return pl.pallas_call(
        functools.partial(step_kernel, n, piece),
        out_shape=(
            out(rows, columns), out(8 * piece, width), out(own_rows, width), out(hot_rows, width)
        ),
        in_specs=[hbm] * 10,
        out_specs=(vmem,) * 4,
        scratch_shapes=[
            i32(hot_feats, samples), i32(1, lookups), i32(1, lookups), i32(1, samples),
            f32(1, columns), pltpu.SMEM(blocks.shape, jnp.int32),
            b16(features, columns), f32(4, own_rows // 4, width),
            f32(4, own_rows // 4, width), f32(hot_rows, width),
            f32(hot_rows, width), b16(n, 4, own_rows // 4, width), i32(n, 1, cap), i32(n, 1, cap),
            b16(n, lookups, own_rows), b16(n * cap, lookups), b16(hot_rows, hot_feats * samples),
            b16(own_rows, n * cap),
            f32(samples, columns), f32(samples, columns), b16(samples, columns),
            b16(4 * depth, 2, rows, samples), b16(4 * depth, rows, samples),
            b16(4, samples, chunk), b16(4, samples, chunk),
            b16(n, cap, width), b16(n, cap, width),
            f32(4, depth, 2, 2, rows, chunk), b16(4, depth, 2, rows, chunk),
            b16(4, depth, 2, rows, chunk),
            f32(4, depth, 2, rows, chunk), f32(4, depth, rows, chunk), f32(4, depth, rows, chunk),
            f32(4, depth - 1, rows, chunk),
            f32(2, own_rows // 2, width), f32(own_rows // 2, width), f32(own_rows // 2, width),
            f32(own_rows // 2, width), f32(2, own_rows // 2, width),
            f32(8 * piece, width), f32(4 * piece, width), f32(4 * piece, width),
            f32(3, piece, width), f32(depth, piece, width), f32(8 * piece, width),
            pltpu.SemaphoreType.DMA((11,)),
            pltpu.SemaphoreType.DMA((copies,)),
            pltpu.SemaphoreType.DMA((copies,)),
        ],
        compiler_params=pltpu.CompilerParams(
            collective_id=0, has_side_effects=True, vmem_limit_bytes=VMEM_LIMIT
        ),
    )(
        *[
            pltpu.with_memory_space_constraint(value, pltpu.HBM)
            for value in (
                hot_ids, owner, offset, labels, out_weight, blocks,
                weight, table.reshape(4, own_rows // 4, width), cache, pending,
            )
        ]
    )


def update_kernel(
    blocks, clock, top, sums, cold, carried, table, accum, cache, hot_accum,
    table_out, accum_out, cache_out, hot_accum_out, pending_out, top_out, head_out,
):
    table_out[...], accum_out[...] = adagrad(table[...], accum[...], cold[...])
    cache_out[...] = cache[...]
    hot_accum_out[...] = hot_accum[...]
    pending_out[...] = carried[...]
    picks = blocks.shape[0]
    for k in range(picks):
        rows = pl.ds(pl.multiple_of(blocks[k] * BLOCK, BLOCK), BLOCK)
        divisor = 1.0 + clock[blocks[k]].astype(jnp.float32)
        flush = sums[k * BLOCK : (k + 1) * BLOCK, :] / divisor
        cache_next, accum_next = adagrad(cache[rows, :], hot_accum[rows, :], flush)
        cache_out[rows, :] = cache_next
        hot_accum_out[rows, :] = accum_next
        pending_out[rows, :] = jnp.zeros((BLOCK, cache.shape[1]), jnp.float32)
    top_out[...] = top[...]
    head_out[...] = sums[picks * BLOCK : picks * BLOCK + head_out.shape[0], :]


def update(blocks, clock, top, sums, cold, carried, table, accum, cache, hot_accum):
    head_rows = top.shape[1] // cache.shape[1]
    smem = pl.BlockSpec(memory_space=pltpu.SMEM)
    vmem = pl.BlockSpec(memory_space=pltpu.VMEM)
    like = lambda a: jax.ShapeDtypeStruct(a.shape, a.dtype)
    return pl.pallas_call(
        update_kernel,
        out_shape=(
            like(table), like(accum), like(cache), like(hot_accum), like(carried), like(top),
            jax.ShapeDtypeStruct((head_rows, cache.shape[1]), jnp.float32),
        ),
        in_specs=[smem] * 2 + [vmem] * 8,
        out_specs=(vmem,) * 7,
        compiler_params=pltpu.CompilerParams(vmem_limit_bytes=VMEM_LIMIT // 2),
    )(blocks, clock, top, sums, cold, carried, table, accum, cache, hot_accum)


def suits(n, rep_n, top_weight, hot_ids, cold_offset, hot_cache, cold_table):
    features, columns = top_weight.shape
    samples, lookups, width = hot_ids.shape[0], cold_offset.shape[0], hot_cache.shape[1]
    return (
        rep_n == 4
        and n % 2 == 0
        and 4 <= n <= 16
        and features % (16 * 4 * n) == 0
        and columns % 1024 == 0
        and samples % 128 == 0
        and lookups == 2 * samples
        and width == 128
        and (2 * lookups // n) % 128 == 0
        and hot_cache.shape[0] % 128 == 0
        and cold_table.shape[0] % 256 == 0
    )


def direct(
    n, hot_ids, cold_owner, cold_offset, labels, top_weight, out_weight, cold_table, cold_accum,
    hot_cache, hot_accum, pending, refresh_blocks, block_clock,
):
    cap = 2 * cold_offset.shape[0] // n
    top, sums, cold, carried = step(
        hot_ids.T, cold_owner.reshape(1, -1), cold_offset.reshape(1, -1), labels.reshape(1, -1),
        out_weight.reshape(1, -1), refresh_blocks, top_weight, cold_table, hot_cache, pending, n, cap,
    )
    results = update(
        refresh_blocks, block_clock, top, sums, cold, carried, cold_table, cold_accum, hot_cache,
        hot_accum,
    )
    return results[:6] + (results[6].reshape(-1),)


def local(
    hot_ids,
    cold_owner,
    cold_offset,
    labels,
    top_weight,
    out_weight,
    cold_table,
    cold_accum,
    hot_cache,
    hot_accum,
    pending,
    refresh_blocks,
    block_clock,
):
    n, rep_n = lax.axis_size("dp"), lax.axis_size("rep")
    if suits(n, rep_n, top_weight, hot_ids, cold_offset, hot_cache, cold_table):
        return direct(
            n, hot_ids, cold_owner, cold_offset, labels, top_weight, out_weight, cold_table,
            cold_accum, hot_cache, hot_accum, pending, refresh_blocks, block_clock,
        )
    width = hot_cache.shape[1]
    samples = hot_ids.shape[0]
    hot_feats = hot_ids.shape[1]
    lookups = cold_offset.shape[0]
    cold_feats = lookups // samples
    owners_count = lax.axis_size("dp")
    capacity = max(2, 2 * lookups // owners_count)
    owners = cold_owner[:, 0]
    matches = (owners[:, None] == jnp.arange(owners_count, dtype=jnp.int32)[None, :]).astype(
        jnp.int32
    )
    before = jnp.arange(lookups)[:, None] > jnp.arange(lookups)[None, :]
    earlier = jnp.dot(
        before.astype(jnp.bfloat16),
        matches.astype(jnp.bfloat16),
        preferred_element_type=jnp.float32,
    ).astype(jnp.int32)
    positions = jnp.sum(earlier * matches, axis=1)
    targets = owners * capacity + positions
    places = jnp.arange(owners_count * capacity, dtype=jnp.int32)
    placed = targets[:, None] == places[None, :]
    requests = jnp.sum(jnp.where(placed, cold_offset[:, None], 0), axis=0)
    placed = placed.astype(jnp.bfloat16)
    requests = requests.reshape(owners_count, capacity)
    asked = lax.all_to_all(requests, "dp", split_axis=0, concat_axis=0, tiled=True)
    found = cold_table[asked].astype(jnp.bfloat16)
    returned = lax.all_to_all(found, "dp", split_axis=0, concat_axis=0, tiled=True)
    cold_rows = jnp.dot(
        placed,
        returned.reshape(owners_count * capacity, width),
        preferred_element_type=jnp.float32,
    ).astype(jnp.bfloat16)
    cold_rows = cold_rows.reshape(samples, cold_feats, width)
    hot_rows = hot_cache[hot_ids].astype(jnp.bfloat16)
    inputs = jnp.concatenate([hot_rows, cold_rows], axis=1).reshape(
        samples, (hot_feats + cold_feats) * width
    )
    preact = jnp.dot(inputs, top_weight, preferred_element_type=jnp.float32)
    hidden = jax.nn.silu(preact).astype(jnp.bfloat16)
    hidden_wide = hidden.astype(jnp.float32)
    logits = jnp.dot(hidden_wide, out_weight, precision=lax.Precision.HIGHEST)
    errors = jax.nn.sigmoid(logits) - labels.astype(jnp.float32)
    gates = jax.nn.sigmoid(preact)
    slope = gates * (1.0 + preact * (1.0 - gates))
    dhidden = (errors[:, None] * out_weight[None, :] * slope).astype(jnp.bfloat16)
    head_term = jnp.dot(errors, hidden_wide, precision=lax.Precision.HIGHEST)
    top_part = lax.dot_general(
        inputs, dhidden, (((0,), (0,)), ((), ())), preferred_element_type=jnp.float32
    )
    dinputs = lax.dot_general(
        dhidden, top_weight, (((1,), (1,)), ((), ())), preferred_element_type=jnp.float32
    ).astype(jnp.bfloat16)
    dinputs = dinputs.reshape(samples, hot_feats + cold_feats, width)
    cold_dx = dinputs[:, hot_feats:].reshape(lookups, width)
    outgoing = lax.dot_general(
        placed, cold_dx, (((0,), (0,)), ((), ())), preferred_element_type=jnp.float32
    ).astype(jnp.bfloat16)
    outgoing = outgoing.reshape(owners_count, capacity, width)
    own_rows = cold_table.shape[0]
    quarter = own_rows // lax.axis_size("rep")
    hot_count = hot_cache.shape[0]
    blocks_count = hot_count // BLOCK
    hot_dx = dinputs[:, :hot_feats].reshape(samples * hot_feats, width)
    hot_named = (
        jnp.arange(hot_count, dtype=jnp.int32)[:, None] == hot_ids.reshape(-1)[None, :]
    ).astype(jnp.bfloat16)
    hot_grad = jnp.dot(hot_named, hot_dx, preferred_element_type=jnp.float32)
    carried = (pending + hot_grad).reshape(blocks_count, BLOCK, width)
    picked = carried[refresh_blocks]
    divisors = 1.0 + block_clock.astype(jnp.float32)
    named = refresh_blocks[:, None] == jnp.arange(blocks_count, dtype=jnp.int32)[None, :]
    refreshed = jnp.any(named, axis=0)[:, None, None]
    cache_blocks = hot_cache.reshape(blocks_count, BLOCK, width)
    accum_blocks = hot_accum.reshape(blocks_count, BLOCK, width)
    incoming = lax.all_to_all(outgoing, "dp", split_axis=0, concat_axis=0, tiled=True)
    cold_grad = (
        jnp.zeros((own_rows, width), jnp.float32)
        .at[asked.reshape(-1)]
        .add(incoming.reshape(-1, width).astype(jnp.float32))
    )
    cold_share = lax.psum_scatter(cold_grad, "rep", scatter_dimension=0, tiled=True)
    offset_rows = lax.axis_index("rep") * quarter
    table_share = lax.dynamic_slice_in_dim(cold_table, offset_rows, quarter, 0)
    accum_share = lax.dynamic_slice_in_dim(cold_accum, offset_rows, quarter, 0)
    table_updated, accum_updated = adagrad(table_share, accum_share, cold_share)
    cold_table_new, cold_accum_new = (
        lax.all_gather(table_updated, "rep", axis=0, tiled=True),
        lax.all_gather(accum_updated, "rep", axis=0, tiled=True),
    )
    top_grad = lax.psum_scatter(top_part, ("dp", "rep"), scatter_dimension=0, tiled=True)
    picked_sum, out_grad = lax.psum((picked, head_term), ("dp", "rep"))
    block_sums = jnp.zeros((), jnp.float32)
    for k in range(refresh_blocks.shape[0]):
        block_sums = jnp.where(named[k][:, None, None], picked_sum[k][None], block_sums)
    flush = block_sums / divisors[:, None, None]
    cache_next, accum_next = adagrad(cache_blocks, accum_blocks, flush)
    hot_cache_new = jnp.where(refreshed, cache_next, cache_blocks).reshape(hot_count, width)
    hot_accum_new = jnp.where(refreshed, accum_next, accum_blocks).reshape(hot_count, width)
    pending_new = jnp.where(refreshed, 0.0, carried).reshape(hot_count, width)
    return (
        cold_table_new,
        cold_accum_new,
        hot_cache_new,
        hot_accum_new,
        pending_new,
        top_grad,
        out_grad,
    )


def solution(mesh):
    in_specs = (
        P(("dp", "rep"), None),
        P(("dp", "rep"), None),
        P(("dp", "rep")),
        P(("dp", "rep")),
        P(),
        P(),
        P("dp", None),
        P("dp", None),
        P(),
        P(),
        P(("dp", "rep"), None),
        P(),
        P(),
    )
    out_specs = (
        P("dp", None),
        P("dp", None),
        P(),
        P(),
        P(("dp", "rep"), None),
        P(("dp", "rep"), None),
        P(),
    )
    return jax.shard_map(local, mesh=mesh, in_specs=in_specs, out_specs=out_specs, check_vma=False)
```

```python
import functools

import jax
import jax.numpy as jnp
from jax import lax
from jax.experimental import pallas as pl
from jax.experimental.pallas import tpu as pltpu
from jax.sharding import PartitionSpec as P

BLOCK = 128
VMEM_LIMIT = 40 * 1024 * 1024
MESH = pl.DeviceIdType.MESH


step_size = 0.5
epsilon = 1e-08


def adagrad(table_rows, accum_rows, gradient):
    accum_next = accum_rows + gradient * gradient
    return (table_rows - step_size * gradient / (jnp.sqrt(accum_next) + epsilon), accum_next)


def row_to_col(row, first, step, count):
    per = 128 // step
    shape = (per, 128)
    wanted = lax.broadcasted_iota(jnp.int32, shape, 1) == step * lax.broadcasted_iota(
        jnp.int32, shape, 0
    ) + first
    pieces = []
    for i in range(count // per):
        part = jnp.broadcast_to(row[:, i * 128 : (i + 1) * 128], shape)
        pieces.append(jnp.sum(jnp.where(wanted, part, 0.0), axis=1, keepdims=True))
    return jnp.concatenate(pieces, axis=0)


def col_to_row(col):
    shape = (128, 128)
    same = lax.broadcasted_iota(jnp.int32, shape, 0) == lax.broadcasted_iota(jnp.int32, shape, 1)
    pieces = []
    for i in range(col.shape[0] // 128):
        part = jnp.broadcast_to(col[i * 128 : (i + 1) * 128], shape)
        pieces.append(jnp.sum(jnp.where(same, part, 0.0), axis=0, keepdims=True))
    return jnp.concatenate(pieces, axis=1)


def one_hot(ids, shape, dim):
    match = lax.broadcasted_iota(jnp.int32, shape, dim) == jnp.broadcast_to(ids, shape)
    return jnp.where(match, 1.0, 0.0).astype(jnp.bfloat16)


def matmul(a, b, contract=(1, 0)):
    return lax.dot_general(
        a, b, (((contract[0],), (contract[1],)), ((), ())), preferred_element_type=jnp.float32
    )


def step_kernel(
    n, piece,
    hot_ids_in, owner_in, offset_in, labels_in, out_weight_in, blocks_in, weight, table, cache,
    pending,
    top_out, sums_out, cold_out, carried_out,
    hot_ids, owner, offset, labels, out_weight, blocks,
    weight_v, table_v, table_all, cache_v, pending_v, tables, requests, asked, look, placed_t, hot_t, own_hot,
    pre, gate, hidden, inputs_t, inputs_got, dh, dh_got, outgoing, incoming,
    top, leave, got_1, part_1, got_2, part_2, got_3,
    cold, cold_got, cold_half, cold_last, cold_full, hot_sum, hot_got, hot_mid, hot_near, hot_z,
    hot_all,
    loads, sends, recvs,
):
    me, rep = lax.axis_index("dp"), lax.axis_index("rep")
    x, z = lax.rem(me, 2), lax.div(me, 2)
    core, y = lax.rem(rep, 2), lax.div(rep, 2)
    depth = n // 2
    f32, bf16 = jnp.float32, jnp.bfloat16

    def flip(value, on):
        return 1 - value if on else value

    def near(mask):
        return (z * 2 + flip(x, mask & 4), flip(y, mask & 2) * 2 + flip(core, mask & 1))

    def level(k):
        value = z
        for weight in (1, 2, 4):
            if k & weight:
                value = value + weight * (1 - 2 * lax.rem(lax.div(z, weight), 2))
        return value

    def along(k):
        return level(k) * 2 + x

    sibling, over_x, over_y = near(1), near(4), near(2)
    peers = [lax.rem(me + j, n) for j in range(1, n)]
    sources = [lax.rem(me + n - j, n) for j in range(1, n)]
    greeted = [(peer, rep) for peer in peers] + [sibling, over_y, near(6)]
    barrier = pltpu.get_barrier_semaphore()
    for device in greeted:
        pl.semaphore_signal(barrier, inc=1, device_id=device, device_id_type=MESH)
    local = []
    for src, dst in [
        (table.at[rep], table_v), (owner_in, owner), (offset_in, offset),
        (table, table_all), (hot_ids_in, hot_ids), (cache, cache_v),
        (weight, weight_v), (labels_in, labels), (out_weight_in, out_weight), (blocks_in, blocks),
        (pending, pending_v),
    ]:
        local.append(pltpu.make_async_copy(src, dst, loads.at[len(local)]))
    local[0].start()

    count = [0]
    started = []

    def send(src, dst, device):
        k = count[0]
        count[0] += 1
        copy = pltpu.make_async_remote_copy(src, dst, sends.at[k], recvs.at[k], device, MESH)
        copy.start()
        started.append(copy)
        return copy

    def same(ref, device):
        return send(ref, ref, device)

    local[0].wait()
    tables[me, rep] = table_v[...].astype(bf16)
    for copy in local[1:]:
        copy.start()
    pl.semaphore_wait(barrier, len(greeted))
    mine = tables.at[me, rep]
    order = list(range(1, depth))
    z_table = {k: same(mine, (along(k), rep)) for k in order[::-1]}
    x_table = same(mine, over_x)

    samples = hot_ids.shape[1]
    hot_feats = hot_ids.shape[0]
    lookups = owner.shape[1]
    feats = lookups // samples
    own_rows, width = tables.shape[1] * tables.shape[2], tables.shape[3]
    cap = requests.shape[2]
    hot_rows = cache_v.shape[0]
    columns = weight_v.shape[1]
    chunk = dh.shape[2]
    chunks = columns // chunk
    hot_in = hot_feats * width

    local[1].wait()
    local[2].wait()
    owner_row, offset_row = owner[...].astype(f32), offset[...].astype(f32)
    owner_col = jnp.concatenate(
        [row_to_col(owner_row, k, feats, samples) for k in range(feats)], axis=0
    )
    offset_col = jnp.concatenate(
        [row_to_col(offset_row, k, feats, samples) for k in range(feats)], axis=0
    )
    lanes = lax.broadcasted_iota(jnp.int32, (lookups, 128), 1)
    matches = jnp.where(lanes == owner_col.astype(jnp.int32), 1.0, 0.0)
    square = (lookups, lookups)
    before = lax.broadcasted_iota(jnp.int32, square, 1) < lax.broadcasted_iota(
        jnp.int32, square, 0
    )
    earlier = matmul(jnp.where(before, 1.0, 0.0).astype(bf16), matches.astype(bf16))
    target = owner_col * cap + jnp.sum(earlier * matches, axis=1, keepdims=True)
    target_int = target.astype(jnp.int32)
    for o in range(n):
        slots = lax.broadcasted_iota(jnp.int32, (lookups, cap), 1) + o * cap
        asks = jnp.where(slots == target_int, offset_col, 0.0)
        requests[o] = jnp.sum(asks, axis=0, keepdims=True).astype(jnp.int32)
    asking = [send(requests.at[peer], asked.at[me], (peer, rep)) for peer in peers]
    asked[me] = requests[me]

    global_col = (owner_col * own_rows + offset_col).astype(jnp.int32)
    for o in range(n):
        look[o] = one_hot(global_col - o * own_rows, (lookups, own_rows), 1)

    def relay(copy, source, *devices):
        copy.wait_recv()
        return [same(tables.at[source, rep], device) for device in devices]

    def looked(o):
        return matmul(look[o], tables[o].reshape(own_rows, width))

    x_source = z * 2 + 1 - x
    z_source = {k: along(k) for k in order}
    far_source = {k: level(k) * 2 + 1 - x for k in order}
    others = [x_source] + [z_source[k] for k in order] + [far_source[k] for k in order]
    by_y, by_core, y_core, by_x = {}, {}, {}, {}
    by_y[0], by_core[0] = relay(x_table, x_source, over_y, sibling)

    def relay_z(i):
        k = order[i]
        by_x[k], by_y[1 + i], by_core[1 + i] = relay(
            z_table[k], z_source[k], over_x, over_y, sibling
        )

    relay_z(0)

    local[4].wait()
    hot_col = jnp.concatenate(
        [row_to_col(hot_ids[k : k + 1].astype(f32), 0, 1, samples) for k in range(hot_feats)], axis=0
    )
    local[5].wait()
    hot_found = matmul(
        one_hot(hot_col.astype(jnp.int32), (hot_feats * samples, hot_rows), 1),
        cache_v[...].astype(bf16),
    )
    hot_x = [hot_found[k * samples : (k + 1) * samples] for k in range(hot_feats)]

    for i in range(1, depth - 1):
        relay_z(i)

    local[6].wait()
    hot_wide = jnp.concatenate(hot_x, axis=1).astype(bf16)
    for h in range(chunks):
        at = slice(h * chunk, (h + 1) * chunk)
        pre[:, at] = matmul(hot_wide, weight_v[:hot_in, at])
    local[3].wait()
    for i in range(1, 4):
        tables[me, lax.rem(rep + i, 4)] = table_all[lax.rem(rep + i, 4)].astype(bf16)

    def relay_y(i):
        by_y[i].wait_recv()
        y_core[i] = same(tables.at[others[i], (1 - y) * 2 + core], sibling)

    relay_y(0)
    for i, k in enumerate(order):
        by_y[depth + i], by_core[depth + i] = relay(by_x[k], far_source[k], over_y, sibling)
        relay_y(1 + i)
    placed_t[...] = one_hot(
        col_to_row(target).astype(jnp.int32), (n * cap, lookups), 0
    )
    hot_t[...] = one_hot(
        jnp.concatenate([hot_ids[k : k + 1] for k in range(hot_feats)], axis=1),
        (hot_rows, hot_feats * samples), 0,
    )
    cold_found = looked(me)

    def found(j):
        by_core[j].wait_recv()
        y_core[j].wait_recv()
        return looked(others[j])

    cold_found += found(0)
    for i in range(depth, n - 1):
        relay_y(i)
        cold_found += found(i - depth + 1)
    for j in range(depth, n - 1):
        cold_found += found(j)
    cold_x = [cold_found[k * samples : (k + 1) * samples] for k in range(feats)]
    inputs_t[...] = (
        jnp.concatenate([part.T for part in hot_x + cold_x], axis=0)
        .astype(bf16)
        .reshape(inputs_t.shape)
    )
    inputs_copy = send(inputs_t.at[:, 1 - core], inputs_got, sibling)

    local[7].wait()
    local[8].wait()
    cold_wide = jnp.concatenate(cold_x, axis=1).astype(bf16)
    logits = jnp.zeros((samples, 1), f32)
    for h in range(chunks):
        at = slice(h * chunk, (h + 1) * chunk)
        preact = pre[:, at] + matmul(cold_wide, weight_v[hot_in:, at])
        gates = jax.nn.sigmoid(preact)
        shown = (preact * gates).astype(bf16)
        hidden[:, at] = shown
        logits += jnp.sum(shown.astype(f32) * out_weight[:, at], axis=1, keepdims=True)
        gate[:, at] = out_weight[:, at] * (gates * (1.0 + preact * (1.0 - gates)))
    errors = jax.nn.sigmoid(logits) - row_to_col(labels[...].astype(f32), 0, 1, samples)
    dh_copies = []
    for h in range(chunks):
        at = slice(h * chunk, (h + 1) * chunk)
        dh[h] = (errors * gate[:, at]).astype(bf16)
        dh_copies.append(send(dh.at[h], dh_got.at[h], sibling))

    def dinputs(rows):
        total = matmul(dh[0], weight_v[rows, :chunk], (1, 1))
        for h in range(1, chunks):
            total += matmul(dh[h], weight_v[rows, h * chunk : (h + 1) * chunk], (1, 1))
        total = total.astype(bf16)
        return jnp.concatenate(
            [total[:, k : k + width] for k in range(0, total.shape[1], width)], axis=0
        )

    cold_dx = dinputs(slice(hot_in, weight_v.shape[0]))
    outgoing[...] = matmul(placed_t[...], cold_dx).astype(bf16).reshape(outgoing.shape)
    cold_copies = [send(outgoing.at[peer], incoming.at[me], (peer, rep)) for peer in peers]
    incoming[me] = outgoing[me]

    inputs_copy.wait_recv()

    def x_first(h):
        return h == chunks - 1

    def first_step(h):
        both = matmul(inputs_t[:, core].reshape(-1, samples), dh[h])
        dh_copies[h].wait_recv()
        both += matmul(inputs_got[...].reshape(-1, samples), dh_got[h])
        top[h] = both.reshape(top.shape[1:])
        leaving = top[h, :, 1 - x] if x_first(h) else top[h, :, :, 1 - y]
        leave[h] = leaving.astype(bf16)
        return send(leave.at[h], got_1.at[h], over_x if x_first(h) else over_y)

    def second_step(h):
        first[h].wait_recv()
        kept = top[h, :, x] if x_first(h) else top[h, :, :, y]
        part_1[h] = kept + got_1[h].astype(f32)
        if x_first(h):
            return send(part_1.at[h, :, 1 - y], got_2.at[h], over_y)
        return send(part_1.at[h, :, 1 - x], got_2.at[h], over_x)

    def third_step(h):
        second[h].wait_recv()
        part_2[h] = part_1[h, :, y if x_first(h) else x] + got_2[h]
        return [
            send(part_2.at[h, level(k)], got_3.at[h, k - 1], (along(k), rep))
            for k in range(1, depth)
        ]

    first = [first_step(h) for h in range(chunks // 2)]

    hot_dx = dinputs(slice(0, hot_in))
    local[9].wait()
    local[10].wait()
    carried_out[...] = pending_v[...] + matmul(hot_t[...], hot_dx)
    total_rows = hot_sum.shape[0]
    picks = blocks.shape[0]
    for k in range(picks):
        wanted = jnp.full((BLOCK, width), blocks[k])
        picked = carried_out[:BLOCK, :]
        for b in range(1, hot_rows // BLOCK):
            picked = jnp.where(wanted == b, carried_out[b * BLOCK : (b + 1) * BLOCK, :], picked)
        hot_sum[k * BLOCK : (k + 1) * BLOCK, :] = picked
    base = picks * BLOCK
    hot_sum[base:, :] = jnp.zeros((total_rows - base, width), f32)
    for h in range(chunks):
        head = jnp.sum(
            errors * hidden[:, h * chunk : (h + 1) * chunk].astype(f32), axis=0, keepdims=True
        )
        for i in range(chunk // width):
            row = base + h * (chunk // width) + i
            hot_sum[row : row + 1, :] = head[:, i * width : (i + 1) * width]

    def part_of(ref, q, rows):
        return ref.at[pl.ds(pl.multiple_of(q * rows, 8), rows)]

    hot_copy = send(part_of(hot_sum, 1 - core, 4 * piece), hot_got, sibling)
    my_quad = x * 2 + y
    quads = [(flip(x, m & 4) * 2 + flip(y, m & 2), near(m)) for m in (2, 4, 6)]

    first += [first_step(h) for h in range(chunks // 2, chunks)]


    hot_copy.wait_recv()
    hot_mid[...] = part_of(hot_sum, core, 4 * piece)[...] + hot_got[...]
    hot_copies = [
        send(part_of(hot_mid, q, piece), hot_near.at[i], device)
        for i, (q, device) in enumerate(quads)
    ]
    for o in range(n - 1):
        asking[o].wait_recv()
    for o in range(n):
        own_hot[:, o * cap : (o + 1) * cap] = one_hot(asked[o], (own_rows, cap), 0)

    second = [second_step(h) for h in range(chunks)]

    for copy in hot_copies:
        copy.wait_recv()
    hot_z[z] = part_of(hot_mid, my_quad, piece)[...] + hot_near[0] + hot_near[1] + hot_near[2]
    hot_copies = [same(hot_z.at[z], (along(k), rep)) for k in range(1, depth)]

    for copy in cold_copies:
        copy.wait_recv()
    cold[...] = matmul(own_hot[...], incoming[...].reshape(n * cap, width)).reshape(cold.shape)
    cold_copy = send(cold.at[1 - core], cold_got, sibling)

    cold_copy.wait_recv()
    cold_half[...] = cold[core] + cold_got[...]
    cold_copy = send(cold_half, cold_last, over_y)

    third = [third_step(h) for h in range(chunks)]

    for copy in hot_copies:
        copy.wait_recv()
    final = hot_z[0]
    for k in range(1, depth):
        final += hot_z[k]
    ours = core * 4 + my_quad
    part_of(hot_all, ours, piece)[...] = final
    hot_copies = [same(part_of(hot_all, ours, piece), device) for _, device in quads]

    cold_copy.wait_recv()
    cold_full[core] = cold_half[...] + cold_last[...]
    cold_copy = same(cold_full.at[core], sibling)

    for copy in hot_copies:
        copy.wait_recv()
    hot_copy = same(part_of(hot_all, core, 4 * piece), sibling)

    for h in range(chunks):
        for copy in third[h]:
            copy.wait_recv()
        part = part_2[h, z]
        for k in range(depth - 1):
            part += got_3[h, k]
        top_out[:, h * chunk : (h + 1) * chunk] = part
    cold_copy.wait_recv()
    cold_out[...] = cold_full[...].reshape(cold_out.shape)
    hot_copy.wait_recv()
    sums_out[...] = hot_all[...]
    for copy in started:
        copy.wait_send()


def step(hot_ids, owner, offset, labels, out_weight, blocks, weight, table, cache, pending, n, cap):
    hot_feats, samples = hot_ids.shape
    lookups = owner.shape[1]
    features, columns = weight.shape
    own_rows, width = table.shape
    hot_rows = cache.shape[0]
    depth = n // 2
    rows = features // (4 * n)
    chunk = columns // 4
    sum_rows = blocks.shape[0] * BLOCK + columns // width
    piece = -(-sum_rows // 64) * 8
    f32 = lambda *shape: pltpu.VMEM(shape, jnp.float32)
    b16 = lambda *shape: pltpu.VMEM(shape, jnp.bfloat16)
    i32 = lambda *shape: pltpu.VMEM(shape, jnp.int32)
    copies = 6 * n + 8 * depth + 32
    vmem = pl.BlockSpec(memory_space=pltpu.VMEM)
    hbm = pl.BlockSpec(memory_space=pltpu.HBM)
    out = lambda *shape: jax.ShapeDtypeStruct(shape, jnp.float32)
    return pl.pallas_call(
        functools.partial(step_kernel, n, piece),
        out_shape=(
            out(rows, columns), out(8 * piece, width), out(own_rows, width), out(hot_rows, width)
        ),
        in_specs=[hbm] * 10,
        out_specs=(vmem,) * 4,
        scratch_shapes=[
            i32(hot_feats, samples), i32(1, lookups), i32(1, lookups), i32(1, samples),
            f32(1, columns), pltpu.SMEM(blocks.shape, jnp.int32),
            b16(features, columns), f32(own_rows // 4, width),
            f32(4, own_rows // 4, width), f32(hot_rows, width),
            f32(hot_rows, width), b16(n, 4, own_rows // 4, width), i32(n, 1, cap), i32(n, 1, cap),
            b16(n, lookups, own_rows), b16(n * cap, lookups), b16(hot_rows, hot_feats * samples),
            b16(own_rows, n * cap),
            f32(samples, columns), f32(samples, columns), b16(samples, columns),
            b16(4 * depth, 2, rows, samples), b16(4 * depth, rows, samples),
            b16(4, samples, chunk), b16(4, samples, chunk),
            b16(n, cap, width), b16(n, cap, width),
            f32(4, depth, 2, 2, rows, chunk), b16(4, depth, 2, rows, chunk),
            b16(4, depth, 2, rows, chunk),
            f32(4, depth, 2, rows, chunk), f32(4, depth, rows, chunk), f32(4, depth, rows, chunk),
            f32(4, depth - 1, rows, chunk),
            f32(2, own_rows // 2, width), f32(own_rows // 2, width), f32(own_rows // 2, width),
            f32(own_rows // 2, width), f32(2, own_rows // 2, width),
            f32(8 * piece, width), f32(4 * piece, width), f32(4 * piece, width),
            f32(3, piece, width), f32(depth, piece, width), f32(8 * piece, width),
            pltpu.SemaphoreType.DMA((11,)),
            pltpu.SemaphoreType.DMA((copies,)),
            pltpu.SemaphoreType.DMA((copies,)),
        ],
        compiler_params=pltpu.CompilerParams(
            collective_id=0, has_side_effects=True, vmem_limit_bytes=VMEM_LIMIT
        ),
    )(
        *[
            pltpu.with_memory_space_constraint(value, pltpu.HBM)
            for value in (
                hot_ids, owner, offset, labels, out_weight, blocks,
                weight, table.reshape(4, own_rows // 4, width), cache, pending,
            )
        ]
    )


def update_kernel(
    blocks_in, clock_in, top, sums, cold, carried, table, accum, cache, hot_accum,
    table_out, accum_out, cache_out, hot_accum_out, pending_out, top_out, head_out,
    blocks, clock, table_next, accum_next, cache_next, hot_accum_next, pending_next, sems,
):
    scalars = [
        pltpu.make_async_copy(blocks_in, blocks, sems.at[0]),
        pltpu.make_async_copy(clock_in, clock, sems.at[1]),
    ]
    for copy in scalars:
        copy.start()
    writes = []

    def write(src, dst):
        writes.append(pltpu.make_async_copy(src, dst, sems.at[2 + len(writes)]))
        writes[-1].start()

    picks = blocks.shape[0]
    write(top, top_out)
    write(sums.at[picks * BLOCK : picks * BLOCK + head_out.shape[0]], head_out)
    table_next[...], accum_next[...] = adagrad(table[...], accum[...], cold[...])
    write(table_next, table_out)
    write(accum_next, accum_out)
    pending_next[...] = carried[...]
    cache_next[...] = cache[...]
    hot_accum_next[...] = hot_accum[...]
    for copy in scalars:
        copy.wait()
    rows = [pl.ds(pl.multiple_of(blocks[k] * BLOCK, BLOCK), BLOCK) for k in range(picks)]
    for k in range(picks):
        pending_next[rows[k], :] = jnp.zeros((BLOCK, cache.shape[1]), jnp.float32)
    write(pending_next, pending_out)
    for k in range(picks):
        divisor = 1.0 + clock[blocks[k]].astype(jnp.float32)
        flush = sums[k * BLOCK : (k + 1) * BLOCK, :] / divisor
        cache_next[rows[k], :], hot_accum_next[rows[k], :] = adagrad(
            cache[rows[k], :], hot_accum[rows[k], :], flush
        )
    write(cache_next, cache_out)
    write(hot_accum_next, hot_accum_out)
    for copy in writes:
        copy.wait()


def update(blocks, clock, top, sums, cold, carried, table, accum, cache, hot_accum):
    head_rows = top.shape[1] // cache.shape[1]
    hbm = pl.BlockSpec(memory_space=pltpu.HBM)
    vmem = pl.BlockSpec(memory_space=pltpu.VMEM)
    like = lambda a: jax.ShapeDtypeStruct(a.shape, a.dtype)
    scratch = lambda a: pltpu.VMEM(a.shape, a.dtype)
    return pl.pallas_call(
        update_kernel,
        out_shape=(
            like(table), like(accum), like(cache), like(hot_accum), like(carried), like(top),
            jax.ShapeDtypeStruct((head_rows, cache.shape[1]), jnp.float32),
        ),
        in_specs=[hbm] * 2 + [vmem] * 8,
        out_specs=(hbm,) * 7,
        scratch_shapes=[
            pltpu.SMEM(blocks.shape, jnp.int32), pltpu.SMEM(clock.shape, jnp.int32),
            scratch(table), scratch(accum), scratch(cache), scratch(hot_accum), scratch(carried),
            pltpu.SemaphoreType.DMA((9,)),
        ],
        compiler_params=pltpu.CompilerParams(vmem_limit_bytes=VMEM_LIMIT // 2),
    )(
        pltpu.with_memory_space_constraint(blocks, pltpu.HBM),
        pltpu.with_memory_space_constraint(clock, pltpu.HBM),
        top, sums, cold, carried, table, accum, cache, hot_accum,
    )


def suits(n, rep_n, top_weight, hot_ids, cold_offset, hot_cache, cold_table):
    features, columns = top_weight.shape
    samples, lookups, width = hot_ids.shape[0], cold_offset.shape[0], hot_cache.shape[1]
    return (
        rep_n == 4
        and n % 2 == 0
        and n in (4, 8, 16)
        and features % (16 * 4 * n) == 0
        and columns % 1024 == 0
        and samples % 128 == 0
        and lookups == 2 * samples
        and width == 128
        and (2 * lookups // n) % 128 == 0
        and hot_cache.shape[0] % 128 == 0
        and cold_table.shape[0] % 256 == 0
    )


def direct(
    n, hot_ids, cold_owner, cold_offset, labels, top_weight, out_weight, cold_table, cold_accum,
    hot_cache, hot_accum, pending, refresh_blocks, block_clock,
):
    cap = 2 * cold_offset.shape[0] // n
    top, sums, cold, carried = step(
        hot_ids.T, cold_owner.reshape(1, -1), cold_offset.reshape(1, -1), labels.reshape(1, -1),
        out_weight.reshape(1, -1), refresh_blocks, top_weight, cold_table, hot_cache, pending, n, cap,
    )
    results = update(
        refresh_blocks, block_clock, top, sums, cold, carried, cold_table, cold_accum, hot_cache,
        hot_accum,
    )
    return results[:6] + (results[6].reshape(-1),)


def local(
    hot_ids,
    cold_owner,
    cold_offset,
    labels,
    top_weight,
    out_weight,
    cold_table,
    cold_accum,
    hot_cache,
    hot_accum,
    pending,
    refresh_blocks,
    block_clock,
):
    n, rep_n = lax.axis_size("dp"), lax.axis_size("rep")
    if suits(n, rep_n, top_weight, hot_ids, cold_offset, hot_cache, cold_table):
        return direct(
            n, hot_ids, cold_owner, cold_offset, labels, top_weight, out_weight, cold_table,
            cold_accum, hot_cache, hot_accum, pending, refresh_blocks, block_clock,
        )
    width = hot_cache.shape[1]
    samples = hot_ids.shape[0]
    hot_feats = hot_ids.shape[1]
    lookups = cold_offset.shape[0]
    cold_feats = lookups // samples
    owners_count = lax.axis_size("dp")
    capacity = max(2, 2 * lookups // owners_count)
    owners = cold_owner[:, 0]
    matches = (owners[:, None] == jnp.arange(owners_count, dtype=jnp.int32)[None, :]).astype(
        jnp.int32
    )
    before = jnp.arange(lookups)[:, None] > jnp.arange(lookups)[None, :]
    earlier = jnp.dot(
        before.astype(jnp.bfloat16),
        matches.astype(jnp.bfloat16),
        preferred_element_type=jnp.float32,
    ).astype(jnp.int32)
    positions = jnp.sum(earlier * matches, axis=1)
    targets = owners * capacity + positions
    places = jnp.arange(owners_count * capacity, dtype=jnp.int32)
    placed = targets[:, None] == places[None, :]
    requests = jnp.sum(jnp.where(placed, cold_offset[:, None], 0), axis=0)
    placed = placed.astype(jnp.bfloat16)
    requests = requests.reshape(owners_count, capacity)
    asked = lax.all_to_all(requests, "dp", split_axis=0, concat_axis=0, tiled=True)
    found = cold_table[asked].astype(jnp.bfloat16)
    returned = lax.all_to_all(found, "dp", split_axis=0, concat_axis=0, tiled=True)
    cold_rows = jnp.dot(
        placed,
        returned.reshape(owners_count * capacity, width),
        preferred_element_type=jnp.float32,
    ).astype(jnp.bfloat16)
    cold_rows = cold_rows.reshape(samples, cold_feats, width)
    hot_rows = hot_cache[hot_ids].astype(jnp.bfloat16)
    inputs = jnp.concatenate([hot_rows, cold_rows], axis=1).reshape(
        samples, (hot_feats + cold_feats) * width
    )
    preact = jnp.dot(inputs, top_weight, preferred_element_type=jnp.float32)
    hidden = jax.nn.silu(preact).astype(jnp.bfloat16)
    hidden_wide = hidden.astype(jnp.float32)
    logits = jnp.dot(hidden_wide, out_weight, precision=lax.Precision.HIGHEST)
    errors = jax.nn.sigmoid(logits) - labels.astype(jnp.float32)
    gates = jax.nn.sigmoid(preact)
    slope = gates * (1.0 + preact * (1.0 - gates))
    dhidden = (errors[:, None] * out_weight[None, :] * slope).astype(jnp.bfloat16)
    head_term = jnp.dot(errors, hidden_wide, precision=lax.Precision.HIGHEST)
    top_part = lax.dot_general(
        inputs, dhidden, (((0,), (0,)), ((), ())), preferred_element_type=jnp.float32
    )
    dinputs = lax.dot_general(
        dhidden, top_weight, (((1,), (1,)), ((), ())), preferred_element_type=jnp.float32
    ).astype(jnp.bfloat16)
    dinputs = dinputs.reshape(samples, hot_feats + cold_feats, width)
    cold_dx = dinputs[:, hot_feats:].reshape(lookups, width)
    outgoing = lax.dot_general(
        placed, cold_dx, (((0,), (0,)), ((), ())), preferred_element_type=jnp.float32
    ).astype(jnp.bfloat16)
    outgoing = outgoing.reshape(owners_count, capacity, width)
    own_rows = cold_table.shape[0]
    quarter = own_rows // lax.axis_size("rep")
    hot_count = hot_cache.shape[0]
    blocks_count = hot_count // BLOCK
    hot_dx = dinputs[:, :hot_feats].reshape(samples * hot_feats, width)
    hot_named = (
        jnp.arange(hot_count, dtype=jnp.int32)[:, None] == hot_ids.reshape(-1)[None, :]
    ).astype(jnp.bfloat16)
    hot_grad = jnp.dot(hot_named, hot_dx, preferred_element_type=jnp.float32)
    carried = (pending + hot_grad).reshape(blocks_count, BLOCK, width)
    picked = carried[refresh_blocks]
    divisors = 1.0 + block_clock.astype(jnp.float32)
    named = refresh_blocks[:, None] == jnp.arange(blocks_count, dtype=jnp.int32)[None, :]
    refreshed = jnp.any(named, axis=0)[:, None, None]
    cache_blocks = hot_cache.reshape(blocks_count, BLOCK, width)
    accum_blocks = hot_accum.reshape(blocks_count, BLOCK, width)
    incoming = lax.all_to_all(outgoing, "dp", split_axis=0, concat_axis=0, tiled=True)
    cold_grad = (
        jnp.zeros((own_rows, width), jnp.float32)
        .at[asked.reshape(-1)]
        .add(incoming.reshape(-1, width).astype(jnp.float32))
    )
    cold_share = lax.psum_scatter(cold_grad, "rep", scatter_dimension=0, tiled=True)
    offset_rows = lax.axis_index("rep") * quarter
    table_share = lax.dynamic_slice_in_dim(cold_table, offset_rows, quarter, 0)
    accum_share = lax.dynamic_slice_in_dim(cold_accum, offset_rows, quarter, 0)
    table_updated, accum_updated = adagrad(table_share, accum_share, cold_share)
    cold_table_new, cold_accum_new = (
        lax.all_gather(table_updated, "rep", axis=0, tiled=True),
        lax.all_gather(accum_updated, "rep", axis=0, tiled=True),
    )
    top_grad = lax.psum_scatter(top_part, ("dp", "rep"), scatter_dimension=0, tiled=True)
    picked_sum, out_grad = lax.psum((picked, head_term), ("dp", "rep"))
    block_sums = jnp.zeros((), jnp.float32)
    for k in range(refresh_blocks.shape[0]):
        block_sums = jnp.where(named[k][:, None, None], picked_sum[k][None], block_sums)
    flush = block_sums / divisors[:, None, None]
    cache_next, accum_next = adagrad(cache_blocks, accum_blocks, flush)
    hot_cache_new = jnp.where(refreshed, cache_next, cache_blocks).reshape(hot_count, width)
    hot_accum_new = jnp.where(refreshed, accum_next, accum_blocks).reshape(hot_count, width)
    pending_new = jnp.where(refreshed, 0.0, carried).reshape(hot_count, width)
    return (
        cold_table_new,
        cold_accum_new,
        hot_cache_new,
        hot_accum_new,
        pending_new,
        top_grad,
        out_grad,
    )


def solution(mesh):
    in_specs = (
        P(("dp", "rep"), None),
        P(("dp", "rep"), None),
        P(("dp", "rep")),
        P(("dp", "rep")),
        P(),
        P(),
        P("dp", None),
        P("dp", None),
        P(),
        P(),
        P(("dp", "rep"), None),
        P(),
        P(),
    )
    out_specs = (
        P("dp", None),
        P("dp", None),
        P(),
        P(),
        P(("dp", "rep"), None),
        P(("dp", "rep"), None),
        P(),
    )
    return jax.shard_map(local, mesh=mesh, in_specs=in_specs, out_specs=out_specs, check_vma=False)
```

```python
import functools

import jax
import jax.numpy as jnp
from jax import lax
from jax.experimental import pallas as pl
from jax.experimental.pallas import tpu as pltpu
from jax.sharding import PartitionSpec as P

BLOCK = 128
VMEM_LIMIT = 40 * 1024 * 1024
MESH = pl.DeviceIdType.MESH


step_size = 0.5
epsilon = 1e-08


def adagrad(table_rows, accum_rows, gradient):
    accum_next = accum_rows + gradient * gradient
    return (table_rows - step_size * gradient / (jnp.sqrt(accum_next) + epsilon), accum_next)


def row_to_col(row, first, step, count):
    per = 128 // step
    shape = (per, 128)
    wanted = lax.broadcasted_iota(jnp.int32, shape, 1) == step * lax.broadcasted_iota(
        jnp.int32, shape, 0
    ) + first
    pieces = []
    for i in range(count // per):
        part = jnp.broadcast_to(row[:, i * 128 : (i + 1) * 128], shape)
        pieces.append(jnp.sum(jnp.where(wanted, part, 0.0), axis=1, keepdims=True))
    return jnp.concatenate(pieces, axis=0)


def col_to_row(col):
    shape = (128, 128)
    same = lax.broadcasted_iota(jnp.int32, shape, 0) == lax.broadcasted_iota(jnp.int32, shape, 1)
    pieces = []
    for i in range(col.shape[0] // 128):
        part = jnp.broadcast_to(col[i * 128 : (i + 1) * 128], shape)
        pieces.append(jnp.sum(jnp.where(same, part, 0.0), axis=0, keepdims=True))
    return jnp.concatenate(pieces, axis=1)


def one_hot(ids, shape, dim):
    match = lax.broadcasted_iota(jnp.int32, shape, dim) == jnp.broadcast_to(ids, shape)
    return jnp.where(match, 1.0, 0.0).astype(jnp.bfloat16)


def matmul(a, b, contract=(1, 0)):
    return lax.dot_general(
        a, b, (((contract[0],), (contract[1],)), ((), ())), preferred_element_type=jnp.float32
    )


def step_kernel(
    n, piece,
    hot_ids_in, owner_in, offset_in, labels_in, out_weight_in, blocks_in, weight, table, cache,
    pending,
    top_out, sums_out, cold_out, carried_out,
    hot_ids, owner, offset, labels, out_weight, blocks,
    weight_v, table_v, table_all, cache_v, pending_v, tables, requests, asked, look, placed_t, hot_t, own_hot,
    pre, gate, hidden, inputs_t, inputs_got, dh, dh_got, outgoing, incoming,
    top, leave, got_1, part_1, got_2, part_2, got_3, leave_z, got_z, part_z, got_zx, part_zx, got_zy,
    cold, cold_got, cold_half, cold_last, cold_full, hot_sum, hot_got, hot_mid, hot_near, hot_z,
    hot_all,
    loads, sends, recvs,
):
    me, rep = lax.axis_index("dp"), lax.axis_index("rep")
    x, z = lax.rem(me, 2), lax.div(me, 2)
    core, y = lax.rem(rep, 2), lax.div(rep, 2)
    depth = n // 2
    f32, bf16 = jnp.float32, jnp.bfloat16

    def flip(value, on):
        return 1 - value if on else value

    def near(mask):
        return (z * 2 + flip(x, mask & 4), flip(y, mask & 2) * 2 + flip(core, mask & 1))

    def level(k):
        value = z
        for weight in (1, 2, 4):
            if k & weight:
                value = value + weight * (1 - 2 * lax.rem(lax.div(z, weight), 2))
        return value

    def along(k):
        return level(k) * 2 + x

    sibling, over_x, over_y = near(1), near(4), near(2)
    peers = [lax.rem(me + j, n) for j in range(1, n)]
    sources = [lax.rem(me + n - j, n) for j in range(1, n)]
    greeted = [(peer, rep) for peer in peers] + [sibling, over_y, near(6)]
    barrier = pltpu.get_barrier_semaphore()
    for device in greeted:
        pl.semaphore_signal(barrier, inc=1, device_id=device, device_id_type=MESH)
    local = []
    for src, dst in [
        (table.at[rep], table_v), (owner_in, owner), (offset_in, offset),
        (table, table_all), (hot_ids_in, hot_ids), (cache, cache_v),
        (weight, weight_v), (labels_in, labels), (out_weight_in, out_weight), (blocks_in, blocks),
        (pending, pending_v),
    ]:
        local.append(pltpu.make_async_copy(src, dst, loads.at[len(local)]))
    for copy in local[:3]:
        copy.start()

    count = [0]
    started = []

    def send(src, dst, device):
        k = count[0]
        count[0] += 1
        copy = pltpu.make_async_remote_copy(src, dst, sends.at[k], recvs.at[k], device, MESH)
        copy.start()
        started.append(copy)
        return copy

    def same(ref, device):
        return send(ref, ref, device)

    local[0].wait()
    tables[me, rep] = table_v[...].astype(bf16)
    for copy in local[3:]:
        copy.start()
    pl.semaphore_wait(barrier, len(greeted))
    mine = tables.at[me, rep]
    order = list(range(1, depth))
    z_table = {k: same(mine, (along(k), rep)) for k in order[::-1]}
    x_table = same(mine, over_x)

    samples = hot_ids.shape[1]
    hot_feats = hot_ids.shape[0]
    lookups = owner.shape[1]
    feats = lookups // samples
    own_rows, width = tables.shape[1] * tables.shape[2], tables.shape[3]
    cap = requests.shape[2]
    hot_rows = cache_v.shape[0]
    columns = weight_v.shape[1]
    chunk = dh.shape[2]
    chunks = columns // chunk
    hot_in = hot_feats * width

    local[1].wait()
    local[2].wait()
    owner_row, offset_row = owner[...].astype(f32), offset[...].astype(f32)
    owner_col = jnp.concatenate(
        [row_to_col(owner_row, k, feats, samples) for k in range(feats)], axis=0
    )
    offset_col = jnp.concatenate(
        [row_to_col(offset_row, k, feats, samples) for k in range(feats)], axis=0
    )
    lanes = lax.broadcasted_iota(jnp.int32, (lookups, 128), 1)
    matches = jnp.where(lanes == owner_col.astype(jnp.int32), 1.0, 0.0)
    square = (lookups, lookups)
    before = lax.broadcasted_iota(jnp.int32, square, 1) < lax.broadcasted_iota(
        jnp.int32, square, 0
    )
    earlier = matmul(jnp.where(before, 1.0, 0.0).astype(bf16), matches.astype(bf16))
    target = owner_col * cap + jnp.sum(earlier * matches, axis=1, keepdims=True)
    target_int = target.astype(jnp.int32)
    for o in range(n):
        slots = lax.broadcasted_iota(jnp.int32, (lookups, cap), 1) + o * cap
        asks = jnp.where(slots == target_int, offset_col, 0.0)
        requests[o] = jnp.sum(asks, axis=0, keepdims=True).astype(jnp.int32)
    asking = [send(requests.at[peer], asked.at[me], (peer, rep)) for peer in peers]
    asked[me] = requests[me]

    def relay(copy, source, *devices):
        copy.wait_recv()
        return [same(tables.at[source, rep], device) for device in devices]

    def looked(o):
        return matmul(look[o], tables[o].reshape(own_rows, width))

    x_source = z * 2 + 1 - x
    z_source = {k: along(k) for k in order}
    far_source = {k: level(k) * 2 + 1 - x for k in order}
    others = [x_source] + [z_source[k] for k in order] + [far_source[k] for k in order]
    by_y, by_core, y_core, by_x = {}, {}, {}, {}
    by_y[0], by_core[0] = relay(x_table, x_source, over_y, sibling)

    def relay_z(i):
        k = order[i]
        by_x[k], by_y[1 + i], by_core[1 + i] = relay(
            z_table[k], z_source[k], over_x, over_y, sibling
        )

    relay_z(0)

    local[4].wait()
    hot_col = jnp.concatenate(
        [row_to_col(hot_ids[k : k + 1].astype(f32), 0, 1, samples) for k in range(hot_feats)], axis=0
    )
    local[5].wait()
    hot_found = matmul(
        one_hot(hot_col.astype(jnp.int32), (hot_feats * samples, hot_rows), 1),
        cache_v[...].astype(bf16),
    )
    hot_x = [hot_found[k * samples : (k + 1) * samples] for k in range(hot_feats)]

    for i in range(1, depth - 1):
        relay_z(i)

    global_col = (owner_col * own_rows + offset_col).astype(jnp.int32)
    for o in range(n):
        look[o] = one_hot(global_col - o * own_rows, (lookups, own_rows), 1)

    local[6].wait()
    hot_wide = jnp.concatenate(hot_x, axis=1).astype(bf16)
    for h in range(chunks):
        at = slice(h * chunk, (h + 1) * chunk)
        pre[:, at] = matmul(hot_wide, weight_v[:hot_in, at])
    local[3].wait()
    for i in range(1, 4):
        tables[me, lax.rem(rep + i, 4)] = table_all[lax.rem(rep + i, 4)].astype(bf16)

    def relay_y(i):
        by_y[i].wait_recv()
        y_core[i] = same(tables.at[others[i], (1 - y) * 2 + core], sibling)

    relay_y(0)
    for i, k in enumerate(order):
        by_y[depth + i], by_core[depth + i] = relay(by_x[k], far_source[k], over_y, sibling)
        relay_y(1 + i)
    placed_t[...] = one_hot(
        col_to_row(target).astype(jnp.int32), (n * cap, lookups), 0
    )
    hot_t[...] = one_hot(
        jnp.concatenate([hot_ids[k : k + 1] for k in range(hot_feats)], axis=1),
        (hot_rows, hot_feats * samples), 0,
    )
    cold_found = looked(me)

    def found(j):
        by_core[j].wait_recv()
        y_core[j].wait_recv()
        return looked(others[j])

    cold_found += found(0)
    for i in range(depth, n - 1):
        relay_y(i)
        cold_found += found(i - depth + 1)
    for j in range(depth, n - 1):
        cold_found += found(j)
    cold_x = [cold_found[k * samples : (k + 1) * samples] for k in range(feats)]
    inputs_t[...] = (
        jnp.concatenate([part.T for part in hot_x + cold_x], axis=0)
        .astype(bf16)
        .reshape(inputs_t.shape)
    )
    inputs_copy = send(inputs_t.at[:, 1 - core], inputs_got, sibling)

    local[7].wait()
    local[8].wait()
    cold_wide = jnp.concatenate(cold_x, axis=1).astype(bf16)
    logits = jnp.zeros((samples, 1), f32)
    for h in range(chunks):
        at = slice(h * chunk, (h + 1) * chunk)
        preact = pre[:, at] + matmul(cold_wide, weight_v[hot_in:, at])
        gates = jax.nn.sigmoid(preact)
        shown = (preact * gates).astype(bf16)
        hidden[:, at] = shown
        logits += jnp.sum(shown.astype(f32) * out_weight[:, at], axis=1, keepdims=True)
        gate[:, at] = out_weight[:, at] * (gates * (1.0 + preact * (1.0 - gates)))
    errors = jax.nn.sigmoid(logits) - row_to_col(labels[...].astype(f32), 0, 1, samples)
    dh_copies = []
    for h in range(chunks):
        at = slice(h * chunk, (h + 1) * chunk)
        dh[h] = (errors * gate[:, at]).astype(bf16)
        dh_copies.append(send(dh.at[h], dh_got.at[h], sibling))

    def dinputs(rows):
        total = matmul(dh[0], weight_v[rows, :chunk], (1, 1))
        for h in range(1, chunks):
            total += matmul(dh[h], weight_v[rows, h * chunk : (h + 1) * chunk], (1, 1))
        total = total.astype(bf16)
        return jnp.concatenate(
            [total[:, k : k + width] for k in range(0, total.shape[1], width)], axis=0
        )

    cold_dx = dinputs(slice(hot_in, weight_v.shape[0]))
    outgoing[...] = matmul(placed_t[...], cold_dx).astype(bf16).reshape(outgoing.shape)
    cold_copies = [send(outgoing.at[peer], incoming.at[me], (peer, rep)) for peer in peers]
    incoming[me] = outgoing[me]

    inputs_copy.wait_recv()

    kinds = ["y", "y", "x", "z"]

    def first_step(h):
        both = matmul(inputs_t[:, core].reshape(-1, samples), dh[h])
        dh_copies[h].wait_recv()
        both += matmul(inputs_got[...].reshape(-1, samples), dh_got[h])
        top[h] = both.reshape(top.shape[1:])
        if kinds[h] == "z":
            copies = []
            for k in range(1, depth):
                leave_z[k - 1] = top[h, level(k)].astype(bf16)
                copies.append(send(leave_z.at[k - 1], got_z.at[k - 1], (along(k), rep)))
            return copies
        leaving = top[h, :, 1 - x] if kinds[h] == "x" else top[h, :, :, 1 - y]
        leave[h] = leaving.astype(bf16)
        return [send(leave.at[h], got_1.at[h], over_x if kinds[h] == "x" else over_y)]

    def second_step(h):
        for copy in first[h]:
            copy.wait_recv()
        if kinds[h] == "z":
            part = top[h, z]
            for k in range(depth - 1):
                part += got_z[k].astype(f32)
            part_z[...] = part
            return send(part_z.at[1 - x], got_zx, over_x)
        kept = top[h, :, x] if kinds[h] == "x" else top[h, :, :, y]
        part_1[h] = kept + got_1[h].astype(f32)
        if kinds[h] == "x":
            return send(part_1.at[h, :, 1 - y], got_2.at[h], over_y)
        return send(part_1.at[h, :, 1 - x], got_2.at[h], over_x)

    def third_step(h):
        second[h].wait_recv()
        if kinds[h] == "z":
            part_zx[...] = part_z[x] + got_zx[...]
            return [send(part_zx.at[1 - y], got_zy, over_y)]
        part_2[h] = part_1[h, :, y if kinds[h] == "x" else x] + got_2[h]
        return [
            send(part_2.at[h, level(k)], got_3.at[h, k - 1], (along(k), rep))
            for k in range(1, depth)
        ]

    def last_step(h):
        for copy in third[h]:
            copy.wait_recv()
        if kinds[h] == "z":
            part = part_zx[y] + got_zy[...]
        else:
            part = part_2[h, z]
            for k in range(depth - 1):
                part += got_3[h, k]
        top_out[:, h * chunk : (h + 1) * chunk] = part

    first = [first_step(h) for h in range(chunks // 2)]

    hot_dx = dinputs(slice(0, hot_in))
    local[9].wait()
    local[10].wait()
    carried_out[...] = pending_v[...] + matmul(hot_t[...], hot_dx)
    total_rows = hot_sum.shape[0]
    picks = blocks.shape[0]
    for k in range(picks):
        wanted = jnp.full((BLOCK, width), blocks[k])
        picked = carried_out[:BLOCK, :]
        for b in range(1, hot_rows // BLOCK):
            picked = jnp.where(wanted == b, carried_out[b * BLOCK : (b + 1) * BLOCK, :], picked)
        hot_sum[k * BLOCK : (k + 1) * BLOCK, :] = picked
    base = picks * BLOCK
    hot_sum[base:, :] = jnp.zeros((total_rows - base, width), f32)
    for h in range(chunks):
        head = jnp.sum(
            errors * hidden[:, h * chunk : (h + 1) * chunk].astype(f32), axis=0, keepdims=True
        )
        for i in range(chunk // width):
            row = base + h * (chunk // width) + i
            hot_sum[row : row + 1, :] = head[:, i * width : (i + 1) * width]

    def part_of(ref, q, rows):
        return ref.at[pl.ds(pl.multiple_of(q * rows, 8), rows)]

    hot_copy = send(part_of(hot_sum, 1 - core, 4 * piece), hot_got, sibling)
    my_quad = x * 2 + y
    quads = [(flip(x, m & 4) * 2 + flip(y, m & 2), near(m)) for m in (2, 4, 6)]

    first += [first_step(h) for h in range(chunks // 2, chunks)]


    hot_copy.wait_recv()
    hot_mid[...] = part_of(hot_sum, core, 4 * piece)[...] + hot_got[...]
    hot_copies = [
        send(part_of(hot_mid, q, piece), hot_near.at[i], device)
        for i, (q, device) in enumerate(quads)
    ]
    for o in range(n - 1):
        asking[o].wait_recv()
    for o in range(n):
        own_hot[:, o * cap : (o + 1) * cap] = one_hot(asked[o], (own_rows, cap), 0)

    second = {h: second_step(h) for h in (0, 1, 2)}

    for copy in hot_copies:
        copy.wait_recv()
    hot_z[z] = part_of(hot_mid, my_quad, piece)[...] + hot_near[0] + hot_near[1] + hot_near[2]
    hot_copies = [same(hot_z.at[z], (along(k), rep)) for k in range(1, depth)]

    for copy in cold_copies:
        copy.wait_recv()
    cold[...] = matmul(own_hot[...], incoming[...].reshape(n * cap, width)).reshape(cold.shape)
    cold_copy = send(cold.at[1 - core], cold_got, sibling)

    second[3] = second_step(3)

    cold_copy.wait_recv()
    cold_half[...] = cold[core] + cold_got[...]
    cold_copy = send(cold_half, cold_last, over_y)

    third = {h: third_step(h) for h in (2, 0, 1)}

    for copy in hot_copies:
        copy.wait_recv()
    final = hot_z[0]
    for k in range(1, depth):
        final += hot_z[k]
    ours = core * 4 + my_quad
    part_of(hot_all, ours, piece)[...] = final
    hot_copies = [same(part_of(hot_all, ours, piece), device) for _, device in quads]

    third[3] = third_step(3)

    cold_copy.wait_recv()
    cold_full[core] = cold_half[...] + cold_last[...]
    cold_copy = same(cold_full.at[core], sibling)

    for copy in hot_copies:
        copy.wait_recv()
    hot_copy = same(part_of(hot_all, core, 4 * piece), sibling)

    for h in (3, 2, 0, 1):
        last_step(h)
    cold_copy.wait_recv()
    cold_out[...] = cold_full[...].reshape(cold_out.shape)
    hot_copy.wait_recv()
    sums_out[...] = hot_all[...]
    for copy in started:
        copy.wait_send()


def step(hot_ids, owner, offset, labels, out_weight, blocks, weight, table, cache, pending, n, cap):
    hot_feats, samples = hot_ids.shape
    lookups = owner.shape[1]
    features, columns = weight.shape
    own_rows, width = table.shape
    hot_rows = cache.shape[0]
    depth = n // 2
    rows = features // (4 * n)
    chunk = columns // 4
    sum_rows = blocks.shape[0] * BLOCK + columns // width
    piece = -(-sum_rows // 64) * 8
    f32 = lambda *shape: pltpu.VMEM(shape, jnp.float32)
    b16 = lambda *shape: pltpu.VMEM(shape, jnp.bfloat16)
    i32 = lambda *shape: pltpu.VMEM(shape, jnp.int32)
    copies = 6 * n + 8 * depth + 32
    vmem = pl.BlockSpec(memory_space=pltpu.VMEM)
    hbm = pl.BlockSpec(memory_space=pltpu.HBM)
    out = lambda *shape: jax.ShapeDtypeStruct(shape, jnp.float32)
    return pl.pallas_call(
        functools.partial(step_kernel, n, piece),
        out_shape=(
            out(rows, columns), out(8 * piece, width), out(own_rows, width), out(hot_rows, width)
        ),
        in_specs=[hbm] * 10,
        out_specs=(vmem,) * 4,
        scratch_shapes=[
            i32(hot_feats, samples), i32(1, lookups), i32(1, lookups), i32(1, samples),
            f32(1, columns), pltpu.SMEM(blocks.shape, jnp.int32),
            b16(features, columns), f32(own_rows // 4, width),
            f32(4, own_rows // 4, width), f32(hot_rows, width),
            f32(hot_rows, width), b16(n, 4, own_rows // 4, width), i32(n, 1, cap), i32(n, 1, cap),
            b16(n, lookups, own_rows), b16(n * cap, lookups), b16(hot_rows, hot_feats * samples),
            b16(own_rows, n * cap),
            f32(samples, columns), f32(samples, columns), b16(samples, columns),
            b16(4 * depth, 2, rows, samples), b16(4 * depth, rows, samples),
            b16(4, samples, chunk), b16(4, samples, chunk),
            b16(n, cap, width), b16(n, cap, width),
            f32(4, depth, 2, 2, rows, chunk), b16(4, depth, 2, rows, chunk),
            b16(4, depth, 2, rows, chunk),
            f32(4, depth, 2, rows, chunk), f32(4, depth, rows, chunk), f32(4, depth, rows, chunk),
            f32(4, depth - 1, rows, chunk), b16(depth - 1, 2, 2, rows, chunk),
            b16(depth - 1, 2, 2, rows, chunk), f32(2, 2, rows, chunk), f32(2, rows, chunk),
            f32(2, rows, chunk), f32(rows, chunk),
            f32(2, own_rows // 2, width), f32(own_rows // 2, width), f32(own_rows // 2, width),
            f32(own_rows // 2, width), f32(2, own_rows // 2, width),
            f32(8 * piece, width), f32(4 * piece, width), f32(4 * piece, width),
            f32(3, piece, width), f32(depth, piece, width), f32(8 * piece, width),
            pltpu.SemaphoreType.DMA((11,)),
            pltpu.SemaphoreType.DMA((copies,)),
            pltpu.SemaphoreType.DMA((copies,)),
        ],
        compiler_params=pltpu.CompilerParams(
            collective_id=0, has_side_effects=True, vmem_limit_bytes=VMEM_LIMIT
        ),
    )(
        *[
            pltpu.with_memory_space_constraint(value, pltpu.HBM)
            for value in (
                hot_ids, owner, offset, labels, out_weight, blocks,
                weight, table.reshape(4, own_rows // 4, width), cache, pending,
            )
        ]
    )


def update_kernel(
    blocks_in, clock_in, top, sums, cold, carried, table, accum, cache, hot_accum,
    table_out, accum_out, cache_out, hot_accum_out, pending_out, top_out, head_out,
    blocks, clock, table_next, accum_next, cache_next, hot_accum_next, pending_next, sems,
):
    scalars = [
        pltpu.make_async_copy(blocks_in, blocks, sems.at[0]),
        pltpu.make_async_copy(clock_in, clock, sems.at[1]),
    ]
    for copy in scalars:
        copy.start()
    writes = []

    def write(src, dst):
        writes.append(pltpu.make_async_copy(src, dst, sems.at[2 + len(writes)]))
        writes[-1].start()

    picks = blocks.shape[0]
    write(top, top_out)
    write(sums.at[picks * BLOCK : picks * BLOCK + head_out.shape[0]], head_out)
    table_next[...], accum_next[...] = adagrad(table[...], accum[...], cold[...])
    write(table_next, table_out)
    write(accum_next, accum_out)
    pending_next[...] = carried[...]
    cache_next[...] = cache[...]
    hot_accum_next[...] = hot_accum[...]
    for copy in scalars:
        copy.wait()
    rows = [pl.ds(pl.multiple_of(blocks[k] * BLOCK, BLOCK), BLOCK) for k in range(picks)]
    for k in range(picks):
        pending_next[rows[k], :] = jnp.zeros((BLOCK, cache.shape[1]), jnp.float32)
    write(pending_next, pending_out)
    for k in range(picks):
        divisor = 1.0 + clock[blocks[k]].astype(jnp.float32)
        flush = sums[k * BLOCK : (k + 1) * BLOCK, :] / divisor
        cache_next[rows[k], :], hot_accum_next[rows[k], :] = adagrad(
            cache[rows[k], :], hot_accum[rows[k], :], flush
        )
    write(cache_next, cache_out)
    write(hot_accum_next, hot_accum_out)
    for copy in writes:
        copy.wait()


def update(blocks, clock, top, sums, cold, carried, table, accum, cache, hot_accum):
    head_rows = top.shape[1] // cache.shape[1]
    hbm = pl.BlockSpec(memory_space=pltpu.HBM)
    vmem = pl.BlockSpec(memory_space=pltpu.VMEM)
    like = lambda a: jax.ShapeDtypeStruct(a.shape, a.dtype)
    scratch = lambda a: pltpu.VMEM(a.shape, a.dtype)
    return pl.pallas_call(
        update_kernel,
        out_shape=(
            like(table), like(accum), like(cache), like(hot_accum), like(carried), like(top),
            jax.ShapeDtypeStruct((head_rows, cache.shape[1]), jnp.float32),
        ),
        in_specs=[hbm] * 2 + [vmem] * 8,
        out_specs=(hbm,) * 7,
        scratch_shapes=[
            pltpu.SMEM(blocks.shape, jnp.int32), pltpu.SMEM(clock.shape, jnp.int32),
            scratch(table), scratch(accum), scratch(cache), scratch(hot_accum), scratch(carried),
            pltpu.SemaphoreType.DMA((9,)),
        ],
        compiler_params=pltpu.CompilerParams(vmem_limit_bytes=VMEM_LIMIT // 2),
    )(
        pltpu.with_memory_space_constraint(blocks, pltpu.HBM),
        pltpu.with_memory_space_constraint(clock, pltpu.HBM),
        top, sums, cold, carried, table, accum, cache, hot_accum,
    )


def suits(n, rep_n, top_weight, hot_ids, cold_offset, hot_cache, cold_table):
    features, columns = top_weight.shape
    samples, lookups, width = hot_ids.shape[0], cold_offset.shape[0], hot_cache.shape[1]
    return (
        rep_n == 4
        and n % 2 == 0
        and n in (4, 8, 16)
        and features % (16 * 4 * n) == 0
        and columns % 1024 == 0
        and samples % 128 == 0
        and lookups == 2 * samples
        and width == 128
        and (2 * lookups // n) % 128 == 0
        and hot_cache.shape[0] % 128 == 0
        and cold_table.shape[0] % 256 == 0
    )


def direct(
    n, hot_ids, cold_owner, cold_offset, labels, top_weight, out_weight, cold_table, cold_accum,
    hot_cache, hot_accum, pending, refresh_blocks, block_clock,
):
    cap = 2 * cold_offset.shape[0] // n
    top, sums, cold, carried = step(
        hot_ids.T, cold_owner.reshape(1, -1), cold_offset.reshape(1, -1), labels.reshape(1, -1),
        out_weight.reshape(1, -1), refresh_blocks, top_weight, cold_table, hot_cache, pending, n, cap,
    )
    results = update(
        refresh_blocks, block_clock, top, sums, cold, carried, cold_table, cold_accum, hot_cache,
        hot_accum,
    )
    return results[:6] + (results[6].reshape(-1),)


def local(
    hot_ids,
    cold_owner,
    cold_offset,
    labels,
    top_weight,
    out_weight,
    cold_table,
    cold_accum,
    hot_cache,
    hot_accum,
    pending,
    refresh_blocks,
    block_clock,
):
    n, rep_n = lax.axis_size("dp"), lax.axis_size("rep")
    if suits(n, rep_n, top_weight, hot_ids, cold_offset, hot_cache, cold_table):
        return direct(
            n, hot_ids, cold_owner, cold_offset, labels, top_weight, out_weight, cold_table,
            cold_accum, hot_cache, hot_accum, pending, refresh_blocks, block_clock,
        )
    width = hot_cache.shape[1]
    samples = hot_ids.shape[0]
    hot_feats = hot_ids.shape[1]
    lookups = cold_offset.shape[0]
    cold_feats = lookups // samples
    owners_count = lax.axis_size("dp")
    capacity = max(2, 2 * lookups // owners_count)
    owners = cold_owner[:, 0]
    matches = (owners[:, None] == jnp.arange(owners_count, dtype=jnp.int32)[None, :]).astype(
        jnp.int32
    )
    before = jnp.arange(lookups)[:, None] > jnp.arange(lookups)[None, :]
    earlier = jnp.dot(
        before.astype(jnp.bfloat16),
        matches.astype(jnp.bfloat16),
        preferred_element_type=jnp.float32,
    ).astype(jnp.int32)
    positions = jnp.sum(earlier * matches, axis=1)
    targets = owners * capacity + positions
    places = jnp.arange(owners_count * capacity, dtype=jnp.int32)
    placed = targets[:, None] == places[None, :]
    requests = jnp.sum(jnp.where(placed, cold_offset[:, None], 0), axis=0)
    placed = placed.astype(jnp.bfloat16)
    requests = requests.reshape(owners_count, capacity)
    asked = lax.all_to_all(requests, "dp", split_axis=0, concat_axis=0, tiled=True)
    found = cold_table[asked].astype(jnp.bfloat16)
    returned = lax.all_to_all(found, "dp", split_axis=0, concat_axis=0, tiled=True)
    cold_rows = jnp.dot(
        placed,
        returned.reshape(owners_count * capacity, width),
        preferred_element_type=jnp.float32,
    ).astype(jnp.bfloat16)
    cold_rows = cold_rows.reshape(samples, cold_feats, width)
    hot_rows = hot_cache[hot_ids].astype(jnp.bfloat16)
    inputs = jnp.concatenate([hot_rows, cold_rows], axis=1).reshape(
        samples, (hot_feats + cold_feats) * width
    )
    preact = jnp.dot(inputs, top_weight, preferred_element_type=jnp.float32)
    hidden = jax.nn.silu(preact).astype(jnp.bfloat16)
    hidden_wide = hidden.astype(jnp.float32)
    logits = jnp.dot(hidden_wide, out_weight, precision=lax.Precision.HIGHEST)
    errors = jax.nn.sigmoid(logits) - labels.astype(jnp.float32)
    gates = jax.nn.sigmoid(preact)
    slope = gates * (1.0 + preact * (1.0 - gates))
    dhidden = (errors[:, None] * out_weight[None, :] * slope).astype(jnp.bfloat16)
    head_term = jnp.dot(errors, hidden_wide, precision=lax.Precision.HIGHEST)
    top_part = lax.dot_general(
        inputs, dhidden, (((0,), (0,)), ((), ())), preferred_element_type=jnp.float32
    )
    dinputs = lax.dot_general(
        dhidden, top_weight, (((1,), (1,)), ((), ())), preferred_element_type=jnp.float32
    ).astype(jnp.bfloat16)
    dinputs = dinputs.reshape(samples, hot_feats + cold_feats, width)
    cold_dx = dinputs[:, hot_feats:].reshape(lookups, width)
    outgoing = lax.dot_general(
        placed, cold_dx, (((0,), (0,)), ((), ())), preferred_element_type=jnp.float32
    ).astype(jnp.bfloat16)
    outgoing = outgoing.reshape(owners_count, capacity, width)
    own_rows = cold_table.shape[0]
    quarter = own_rows // lax.axis_size("rep")
    hot_count = hot_cache.shape[0]
    blocks_count = hot_count // BLOCK
    hot_dx = dinputs[:, :hot_feats].reshape(samples * hot_feats, width)
    hot_named = (
        jnp.arange(hot_count, dtype=jnp.int32)[:, None] == hot_ids.reshape(-1)[None, :]
    ).astype(jnp.bfloat16)
    hot_grad = jnp.dot(hot_named, hot_dx, preferred_element_type=jnp.float32)
    carried = (pending + hot_grad).reshape(blocks_count, BLOCK, width)
    picked = carried[refresh_blocks]
    divisors = 1.0 + block_clock.astype(jnp.float32)
    named = refresh_blocks[:, None] == jnp.arange(blocks_count, dtype=jnp.int32)[None, :]
    refreshed = jnp.any(named, axis=0)[:, None, None]
    cache_blocks = hot_cache.reshape(blocks_count, BLOCK, width)
    accum_blocks = hot_accum.reshape(blocks_count, BLOCK, width)
    incoming = lax.all_to_all(outgoing, "dp", split_axis=0, concat_axis=0, tiled=True)
    cold_grad = (
        jnp.zeros((own_rows, width), jnp.float32)
        .at[asked.reshape(-1)]
        .add(incoming.reshape(-1, width).astype(jnp.float32))
    )
    cold_share = lax.psum_scatter(cold_grad, "rep", scatter_dimension=0, tiled=True)
    offset_rows = lax.axis_index("rep") * quarter
    table_share = lax.dynamic_slice_in_dim(cold_table, offset_rows, quarter, 0)
    accum_share = lax.dynamic_slice_in_dim(cold_accum, offset_rows, quarter, 0)
    table_updated, accum_updated = adagrad(table_share, accum_share, cold_share)
    cold_table_new, cold_accum_new = (
        lax.all_gather(table_updated, "rep", axis=0, tiled=True),
        lax.all_gather(accum_updated, "rep", axis=0, tiled=True),
    )
    top_grad = lax.psum_scatter(top_part, ("dp", "rep"), scatter_dimension=0, tiled=True)
    picked_sum, out_grad = lax.psum((picked, head_term), ("dp", "rep"))
    block_sums = jnp.zeros((), jnp.float32)
    for k in range(refresh_blocks.shape[0]):
        block_sums = jnp.where(named[k][:, None, None], picked_sum[k][None], block_sums)
    flush = block_sums / divisors[:, None, None]
    cache_next, accum_next = adagrad(cache_blocks, accum_blocks, flush)
    hot_cache_new = jnp.where(refreshed, cache_next, cache_blocks).reshape(hot_count, width)
    hot_accum_new = jnp.where(refreshed, accum_next, accum_blocks).reshape(hot_count, width)
    pending_new = jnp.where(refreshed, 0.0, carried).reshape(hot_count, width)
    return (
        cold_table_new,
        cold_accum_new,
        hot_cache_new,
        hot_accum_new,
        pending_new,
        top_grad,
        out_grad,
    )


def solution(mesh):
    in_specs = (
        P(("dp", "rep"), None),
        P(("dp", "rep"), None),
        P(("dp", "rep")),
        P(("dp", "rep")),
        P(),
        P(),
        P("dp", None),
        P("dp", None),
        P(),
        P(),
        P(("dp", "rep"), None),
        P(),
        P(),
    )
    out_specs = (
        P("dp", None),
        P("dp", None),
        P(),
        P(),
        P(("dp", "rep"), None),
        P(("dp", "rep"), None),
        P(),
    )
    return jax.shard_map(local, mesh=mesh, in_specs=in_specs, out_specs=out_specs, check_vma=False)
```

```python
import functools

import jax
import jax.numpy as jnp
from jax import lax
from jax.experimental import pallas as pl
from jax.experimental.pallas import tpu as pltpu
from jax.sharding import PartitionSpec as P

BLOCK = 128
VMEM_LIMIT = 40 * 1024 * 1024
MESH = pl.DeviceIdType.MESH


step_size = 0.5
epsilon = 1e-08


def adagrad(table_rows, accum_rows, gradient):
    accum_next = accum_rows + gradient * gradient
    return (table_rows - step_size * gradient / (jnp.sqrt(accum_next) + epsilon), accum_next)


def row_to_col(row, first, step, count):
    per = 128 // step
    shape = (per, 128)
    wanted = lax.broadcasted_iota(jnp.int32, shape, 1) == step * lax.broadcasted_iota(
        jnp.int32, shape, 0
    ) + first
    pieces = []
    for i in range(count // per):
        part = jnp.broadcast_to(row[:, i * 128 : (i + 1) * 128], shape)
        pieces.append(jnp.sum(jnp.where(wanted, part, 0.0), axis=1, keepdims=True))
    return jnp.concatenate(pieces, axis=0)


def col_to_row(col):
    shape = (128, 128)
    same = lax.broadcasted_iota(jnp.int32, shape, 0) == lax.broadcasted_iota(jnp.int32, shape, 1)
    pieces = []
    for i in range(col.shape[0] // 128):
        part = jnp.broadcast_to(col[i * 128 : (i + 1) * 128], shape)
        pieces.append(jnp.sum(jnp.where(same, part, 0.0), axis=0, keepdims=True))
    return jnp.concatenate(pieces, axis=1)


def one_hot(ids, shape, dim):
    match = lax.broadcasted_iota(jnp.int32, shape, dim) == jnp.broadcast_to(ids, shape)
    return jnp.where(match, 1.0, 0.0).astype(jnp.bfloat16)


def matmul(a, b, contract=(1, 0)):
    return lax.dot_general(
        a, b, (((contract[0],), (contract[1],)), ((), ())), preferred_element_type=jnp.float32
    )


def step_kernel(
    n, piece,
    hot_ids_in, owner_in, offset_in, labels_in, out_weight_in, blocks_in, weight, table, cache,
    pending,
    top_out, sums_out, cold_out, carried_out,
    hot_ids, owner, offset, labels, out_weight, blocks,
    weight_v, table_v, table_all, cache_v, pending_v, tables, requests, asked, look, placed_t, hot_t, own_hot,
    pre, gate, hidden, inputs_t, inputs_got, dh, dh_got, outgoing, incoming,
    top, leave, got_1, part_1, got_2, part_2, got_3, leave_z, got_z, part_z, got_zx, part_zx, got_zy,
    cold, cold_got, cold_half, cold_last, cold_full, hot_sum, hot_got, hot_mid, hot_near, hot_z,
    hot_all,
    loads, sends, recvs,
):
    me, rep = lax.axis_index("dp"), lax.axis_index("rep")
    x, z = lax.rem(me, 2), lax.div(me, 2)
    core, y = lax.rem(rep, 2), lax.div(rep, 2)
    depth = n // 2
    f32, bf16 = jnp.float32, jnp.bfloat16

    def flip(value, on):
        return 1 - value if on else value

    def near(mask):
        return (z * 2 + flip(x, mask & 4), flip(y, mask & 2) * 2 + flip(core, mask & 1))

    def level(k):
        value = z
        for weight in (1, 2, 4):
            if k & weight:
                value = value + weight * (1 - 2 * lax.rem(lax.div(z, weight), 2))
        return value

    def along(k):
        return level(k) * 2 + x

    sibling, over_x, over_y, over_xy = near(1), near(4), near(2), near(6)
    peers = [lax.rem(me + j, n) for j in range(1, n)]
    sources = [lax.rem(me + n - j, n) for j in range(1, n)]
    greeted = [(peer, rep) for peer in peers] + [sibling, over_y, over_xy]
    barrier = pltpu.get_barrier_semaphore()
    for device in greeted:
        pl.semaphore_signal(barrier, inc=1, device_id=device, device_id_type=MESH)
    local = []
    for src, dst in [
        (table.at[rep], table_v), (owner_in, owner), (offset_in, offset),
        (table, table_all), (hot_ids_in, hot_ids), (cache, cache_v),
        (weight, weight_v), (labels_in, labels), (out_weight_in, out_weight), (blocks_in, blocks),
        (pending, pending_v),
    ]:
        local.append(pltpu.make_async_copy(src, dst, loads.at[len(local)]))
    for copy in local[:3]:
        copy.start()

    count = [0]
    started = []

    def send(src, dst, device):
        k = count[0]
        count[0] += 1
        copy = pltpu.make_async_remote_copy(src, dst, sends.at[k], recvs.at[k], device, MESH)
        copy.start()
        started.append(copy)
        return copy

    def same(ref, device):
        return send(ref, ref, device)

    local[0].wait()
    tables[me, rep] = table_v[...].astype(bf16)
    for copy in local[3:]:
        copy.start()
    pl.semaphore_wait(barrier, len(greeted))
    mine = tables.at[me, rep]
    order = list(range(1, depth))
    z_table = {k: same(mine, (along(k), rep)) for k in order[::-1]}
    x_table = same(mine, over_x)
    xy_table = same(mine, over_xy)

    samples = hot_ids.shape[1]
    hot_feats = hot_ids.shape[0]
    lookups = owner.shape[1]
    feats = lookups // samples
    own_rows, width = tables.shape[1] * tables.shape[2], tables.shape[3]
    cap = requests.shape[2]
    hot_rows = cache_v.shape[0]
    columns = weight_v.shape[1]
    chunk = dh.shape[2]
    chunks = columns // chunk
    hot_in = hot_feats * width

    local[1].wait()
    local[2].wait()
    owner_row, offset_row = owner[...].astype(f32), offset[...].astype(f32)
    owner_col = jnp.concatenate(
        [row_to_col(owner_row, k, feats, samples) for k in range(feats)], axis=0
    )
    offset_col = jnp.concatenate(
        [row_to_col(offset_row, k, feats, samples) for k in range(feats)], axis=0
    )
    lanes = lax.broadcasted_iota(jnp.int32, (lookups, 128), 1)
    matches = jnp.where(lanes == owner_col.astype(jnp.int32), 1.0, 0.0)
    square = (lookups, lookups)
    before = lax.broadcasted_iota(jnp.int32, square, 1) < lax.broadcasted_iota(
        jnp.int32, square, 0
    )
    earlier = matmul(jnp.where(before, 1.0, 0.0).astype(bf16), matches.astype(bf16))
    target = owner_col * cap + jnp.sum(earlier * matches, axis=1, keepdims=True)
    target_int = target.astype(jnp.int32)
    for o in range(n):
        slots = lax.broadcasted_iota(jnp.int32, (lookups, cap), 1) + o * cap
        asks = jnp.where(slots == target_int, offset_col, 0.0)
        requests[o] = jnp.sum(asks, axis=0, keepdims=True).astype(jnp.int32)
    asking = [send(requests.at[peer], asked.at[me], (peer, rep)) for peer in peers]
    asked[me] = requests[me]

    def relay(copy, source, *devices):
        copy.wait_recv()
        return [same(tables.at[source, rep], device) for device in devices]

    def looked(o):
        return matmul(look[o], tables[o].reshape(own_rows, width))

    x_source = z * 2 + 1 - x
    z_source = {k: along(k) for k in order}
    far_source = {k: level(k) * 2 + 1 - x for k in order}
    others = [x_source] + [z_source[k] for k in order] + [far_source[k] for k in order]
    by_y, by_core, y_core, by_x = {}, {}, {}, {}
    (by_core[0],) = relay(x_table, x_source, sibling)
    by_y[0] = xy_table

    def relay_z(i):
        k = order[i]
        by_x[k], by_y[depth + i], by_y[1 + i], by_core[1 + i] = relay(
            z_table[k], z_source[k], over_x, over_xy, over_y, sibling
        )

    relay_z(0)

    local[4].wait()
    hot_col = jnp.concatenate(
        [row_to_col(hot_ids[k : k + 1].astype(f32), 0, 1, samples) for k in range(hot_feats)], axis=0
    )
    local[5].wait()
    hot_found = matmul(
        one_hot(hot_col.astype(jnp.int32), (hot_feats * samples, hot_rows), 1),
        cache_v[...].astype(bf16),
    )
    hot_x = [hot_found[k * samples : (k + 1) * samples] for k in range(hot_feats)]

    for i in range(1, depth - 1):
        relay_z(i)

    global_col = (owner_col * own_rows + offset_col).astype(jnp.int32)
    for o in range(n):
        look[o] = one_hot(global_col - o * own_rows, (lookups, own_rows), 1)

    local[6].wait()
    hot_wide = jnp.concatenate(hot_x, axis=1).astype(bf16)
    for h in range(chunks):
        at = slice(h * chunk, (h + 1) * chunk)
        pre[:, at] = matmul(hot_wide, weight_v[:hot_in, at])
    local[3].wait()
    for i in range(1, 4):
        tables[me, lax.rem(rep + i, 4)] = table_all[lax.rem(rep + i, 4)].astype(bf16)

    def relay_y(i):
        by_y[i].wait_recv()
        y_core[i] = same(tables.at[others[i], (1 - y) * 2 + core], sibling)

    def found(j):
        by_core[j].wait_recv()
        y_core[j].wait_recv()
        return looked(others[j])

    def relay_far(i):
        k = order[i]
        (by_core[depth + i],) = relay(by_x[k], far_source[k], sibling)
        relay_y(1 + i)
        relay_y(depth + i)

    relay_y(0)
    relay_far(0)
    placed_t[...] = one_hot(
        col_to_row(target).astype(jnp.int32), (n * cap, lookups), 0
    )
    hot_t[...] = one_hot(
        jnp.concatenate([hot_ids[k : k + 1] for k in range(hot_feats)], axis=1),
        (hot_rows, hot_feats * samples), 0,
    )
    cold_found = looked(me) + found(0)
    for i in range(1, depth - 1):
        relay_far(i)
        if i < depth - 2:
            cold_found += found(i)
    for j in range(max(1, depth - 2), n - 1):
        cold_found += found(j)
    cold_x = [cold_found[k * samples : (k + 1) * samples] for k in range(feats)]
    inputs_t[...] = (
        jnp.concatenate([part.T for part in hot_x + cold_x], axis=0)
        .astype(bf16)
        .reshape(inputs_t.shape)
    )
    inputs_copy = send(inputs_t.at[:, 1 - core], inputs_got, sibling)

    local[7].wait()
    local[8].wait()
    cold_wide = jnp.concatenate(cold_x, axis=1).astype(bf16)
    logits = jnp.zeros((samples, 1), f32)
    for h in range(chunks):
        at = slice(h * chunk, (h + 1) * chunk)
        preact = pre[:, at] + matmul(cold_wide, weight_v[hot_in:, at])
        gates = jax.nn.sigmoid(preact)
        shown = (preact * gates).astype(bf16)
        hidden[:, at] = shown
        logits += jnp.sum(shown.astype(f32) * out_weight[:, at], axis=1, keepdims=True)
        gate[:, at] = out_weight[:, at] * (gates * (1.0 + preact * (1.0 - gates)))
    errors = jax.nn.sigmoid(logits) - row_to_col(labels[...].astype(f32), 0, 1, samples)
    dh_copies = []
    for h in range(chunks):
        at = slice(h * chunk, (h + 1) * chunk)
        dh[h] = (errors * gate[:, at]).astype(bf16)
        dh_copies.append(send(dh.at[h], dh_got.at[h], sibling))

    def dinputs(rows):
        total = matmul(dh[0], weight_v[rows, :chunk], (1, 1))
        for h in range(1, chunks):
            total += matmul(dh[h], weight_v[rows, h * chunk : (h + 1) * chunk], (1, 1))
        total = total.astype(bf16)
        return jnp.concatenate(
            [total[:, k : k + width] for k in range(0, total.shape[1], width)], axis=0
        )

    cold_dx = dinputs(slice(hot_in, weight_v.shape[0]))
    outgoing[...] = matmul(placed_t[...], cold_dx).astype(bf16).reshape(outgoing.shape)
    cold_copies = [send(outgoing.at[peer], incoming.at[me], (peer, rep)) for peer in peers]
    incoming[me] = outgoing[me]

    inputs_copy.wait_recv()

    kinds = ["y", "y", "x", "z"]

    def first_step(h):
        both = matmul(inputs_t[:, core].reshape(-1, samples), dh[h])
        dh_copies[h].wait_recv()
        both += matmul(inputs_got[...].reshape(-1, samples), dh_got[h])
        top[h] = both.reshape(top.shape[1:])
        if kinds[h] == "z":
            copies = []
            for k in range(1, depth):
                leave_z[k - 1] = top[h, level(k)].astype(bf16)
                copies.append(send(leave_z.at[k - 1], got_z.at[k - 1], (along(k), rep)))
            return copies
        leaving = top[h, :, 1 - x] if kinds[h] == "x" else top[h, :, :, 1 - y]
        leave[h] = leaving.astype(bf16)
        return [send(leave.at[h], got_1.at[h], over_x if kinds[h] == "x" else over_y)]

    def second_step(h):
        for copy in first[h]:
            copy.wait_recv()
        if kinds[h] == "z":
            part = top[h, z]
            for k in range(depth - 1):
                part += got_z[k].astype(f32)
            part_z[...] = part
            return send(part_z.at[1 - x], got_zx, over_x)
        kept = top[h, :, x] if kinds[h] == "x" else top[h, :, :, y]
        part_1[h] = kept + got_1[h].astype(f32)
        if kinds[h] == "x":
            return send(part_1.at[h, :, 1 - y], got_2.at[h], over_y)
        return send(part_1.at[h, :, 1 - x], got_2.at[h], over_x)

    def third_step(h):
        second[h].wait_recv()
        if kinds[h] == "z":
            part_zx[...] = part_z[x] + got_zx[...]
            return [send(part_zx.at[1 - y], got_zy, over_y)]
        part_2[h] = part_1[h, :, y if kinds[h] == "x" else x] + got_2[h]
        return [
            send(part_2.at[h, level(k)], got_3.at[h, k - 1], (along(k), rep))
            for k in range(1, depth)
        ]

    def last_step(h):
        for copy in third[h]:
            copy.wait_recv()
        if kinds[h] == "z":
            part = part_zx[y] + got_zy[...]
        else:
            part = part_2[h, z]
            for k in range(depth - 1):
                part += got_3[h, k]
        top_out[:, h * chunk : (h + 1) * chunk] = part

    first = [first_step(h) for h in range(chunks // 2)]

    hot_dx = dinputs(slice(0, hot_in))
    local[9].wait()
    local[10].wait()
    carried_out[...] = pending_v[...] + matmul(hot_t[...], hot_dx)
    total_rows = hot_sum.shape[0]
    picks = blocks.shape[0]
    for k in range(picks):
        wanted = jnp.full((BLOCK, width), blocks[k])
        picked = carried_out[:BLOCK, :]
        for b in range(1, hot_rows // BLOCK):
            picked = jnp.where(wanted == b, carried_out[b * BLOCK : (b + 1) * BLOCK, :], picked)
        hot_sum[k * BLOCK : (k + 1) * BLOCK, :] = picked
    base = picks * BLOCK
    hot_sum[base:, :] = jnp.zeros((total_rows - base, width), f32)
    for h in range(chunks):
        head = jnp.sum(
            errors * hidden[:, h * chunk : (h + 1) * chunk].astype(f32), axis=0, keepdims=True
        )
        for i in range(chunk // width):
            row = base + h * (chunk // width) + i
            hot_sum[row : row + 1, :] = head[:, i * width : (i + 1) * width]

    def part_of(ref, q, rows):
        return ref.at[pl.ds(pl.multiple_of(q * rows, 8), rows)]

    hot_copy = send(part_of(hot_sum, 1 - core, 4 * piece), hot_got, sibling)
    my_quad = x * 2 + y
    quads = [(flip(x, m & 4) * 2 + flip(y, m & 2), near(m)) for m in (2, 4, 6)]

    first += [first_step(h) for h in range(chunks // 2, chunks)]


    for o in range(n - 1):
        asking[o].wait_recv()
    for o in range(n):
        own_hot[:, :, o * cap : (o + 1) * cap] = one_hot(asked[o], (own_rows, cap), 0).reshape(
            2, own_rows // 2, cap
        )

    hot_copy.wait_recv()
    hot_mid[...] = part_of(hot_sum, core, 4 * piece)[...] + hot_got[...]
    hot_copies = [
        send(part_of(hot_mid, q, piece), hot_near.at[i], device)
        for i, (q, device) in enumerate(quads)
    ]
    second = {h: second_step(h) for h in (0, 1, 2)}

    for copy in hot_copies:
        copy.wait_recv()
    hot_z[z] = part_of(hot_mid, my_quad, piece)[...] + hot_near[0] + hot_near[1] + hot_near[2]
    hot_copies = [same(hot_z.at[z], (along(k), rep)) for k in range(1, depth)]

    for copy in cold_copies:
        copy.wait_recv()
    arrived = incoming[...].reshape(n * cap, width)
    cold[1 - core] = matmul(own_hot[1 - core], arrived)
    cold_copy = send(cold.at[1 - core], cold_got, sibling)
    cold[core] = matmul(own_hot[core], arrived)

    second[3] = second_step(3)

    cold_copy.wait_recv()
    cold_half[...] = cold[core] + cold_got[...]
    cold_copy = send(cold_half, cold_last, over_y)

    third = {h: third_step(h) for h in (2, 0, 1)}

    for copy in hot_copies:
        copy.wait_recv()
    final = hot_z[0]
    for k in range(1, depth):
        final += hot_z[k]
    ours = core * 4 + my_quad
    part_of(hot_all, ours, piece)[...] = final
    hot_copies = [same(part_of(hot_all, ours, piece), device) for _, device in quads]

    third[3] = third_step(3)

    cold_copy.wait_recv()
    cold_full[core] = cold_half[...] + cold_last[...]
    cold_copy = same(cold_full.at[core], sibling)

    for copy in hot_copies:
        copy.wait_recv()
    hot_copy = same(part_of(hot_all, core, 4 * piece), sibling)

    for h in (3, 2, 0, 1):
        last_step(h)
    cold_copy.wait_recv()
    cold_out[...] = cold_full[...].reshape(cold_out.shape)
    hot_copy.wait_recv()
    sums_out[...] = hot_all[...]
    for copy in started:
        copy.wait_send()


def step(hot_ids, owner, offset, labels, out_weight, blocks, weight, table, cache, pending, n, cap):
    hot_feats, samples = hot_ids.shape
    lookups = owner.shape[1]
    features, columns = weight.shape
    own_rows, width = table.shape
    hot_rows = cache.shape[0]
    depth = n // 2
    rows = features // (4 * n)
    chunk = columns // 4
    sum_rows = blocks.shape[0] * BLOCK + columns // width
    piece = -(-sum_rows // 64) * 8
    f32 = lambda *shape: pltpu.VMEM(shape, jnp.float32)
    b16 = lambda *shape: pltpu.VMEM(shape, jnp.bfloat16)
    i32 = lambda *shape: pltpu.VMEM(shape, jnp.int32)
    copies = 6 * n + 8 * depth + 32
    vmem = pl.BlockSpec(memory_space=pltpu.VMEM)
    hbm = pl.BlockSpec(memory_space=pltpu.HBM)
    out = lambda *shape: jax.ShapeDtypeStruct(shape, jnp.float32)
    return pl.pallas_call(
        functools.partial(step_kernel, n, piece),
        out_shape=(
            out(rows, columns), out(8 * piece, width), out(own_rows, width), out(hot_rows, width)
        ),
        in_specs=[hbm] * 10,
        out_specs=(vmem,) * 4,
        scratch_shapes=[
            i32(hot_feats, samples), i32(1, lookups), i32(1, lookups), i32(1, samples),
            f32(1, columns), pltpu.SMEM(blocks.shape, jnp.int32),
            b16(features, columns), f32(own_rows // 4, width),
            f32(4, own_rows // 4, width), f32(hot_rows, width),
            f32(hot_rows, width), b16(n, 4, own_rows // 4, width), i32(n, 1, cap), i32(n, 1, cap),
            b16(n, lookups, own_rows), b16(n * cap, lookups), b16(hot_rows, hot_feats * samples),
            b16(2, own_rows // 2, n * cap),
            f32(samples, columns), f32(samples, columns), b16(samples, columns),
            b16(4 * depth, 2, rows, samples), b16(4 * depth, rows, samples),
            b16(4, samples, chunk), b16(4, samples, chunk),
            b16(n, cap, width), b16(n, cap, width),
            f32(4, depth, 2, 2, rows, chunk), b16(4, depth, 2, rows, chunk),
            b16(4, depth, 2, rows, chunk),
            f32(4, depth, 2, rows, chunk), f32(4, depth, rows, chunk), f32(4, depth, rows, chunk),
            f32(4, depth - 1, rows, chunk), b16(depth - 1, 2, 2, rows, chunk),
            b16(depth - 1, 2, 2, rows, chunk), f32(2, 2, rows, chunk), f32(2, rows, chunk),
            f32(2, rows, chunk), f32(rows, chunk),
            f32(2, own_rows // 2, width), f32(own_rows // 2, width), f32(own_rows // 2, width),
            f32(own_rows // 2, width), f32(2, own_rows // 2, width),
            f32(8 * piece, width), f32(4 * piece, width), f32(4 * piece, width),
            f32(3, piece, width), f32(depth, piece, width), f32(8 * piece, width),
            pltpu.SemaphoreType.DMA((11,)),
            pltpu.SemaphoreType.DMA((copies,)),
            pltpu.SemaphoreType.DMA((copies,)),
        ],
        compiler_params=pltpu.CompilerParams(
            collective_id=0, has_side_effects=True, vmem_limit_bytes=VMEM_LIMIT
        ),
    )(
        *[
            pltpu.with_memory_space_constraint(value, pltpu.HBM)
            for value in (
                hot_ids, owner, offset, labels, out_weight, blocks,
                weight, table.reshape(4, own_rows // 4, width), cache, pending,
            )
        ]
    )


def update_kernel(
    blocks_in, clock_in, top, sums, cold, carried, table, accum, cache, hot_accum,
    table_out, accum_out, cache_out, hot_accum_out, pending_out, top_out, head_out,
    blocks, clock, table_next, accum_next, cache_next, hot_accum_next, pending_next, sems,
):
    scalars = [
        pltpu.make_async_copy(blocks_in, blocks, sems.at[0]),
        pltpu.make_async_copy(clock_in, clock, sems.at[1]),
    ]
    for copy in scalars:
        copy.start()
    writes = []

    def write(src, dst):
        writes.append(pltpu.make_async_copy(src, dst, sems.at[2 + len(writes)]))
        writes[-1].start()

    picks = blocks.shape[0]
    write(top, top_out)
    write(sums.at[picks * BLOCK : picks * BLOCK + head_out.shape[0]], head_out)
    table_next[...], accum_next[...] = adagrad(table[...], accum[...], cold[...])
    write(table_next, table_out)
    write(accum_next, accum_out)
    pending_next[...] = carried[...]
    cache_next[...] = cache[...]
    hot_accum_next[...] = hot_accum[...]
    for copy in scalars:
        copy.wait()
    rows = [pl.ds(pl.multiple_of(blocks[k] * BLOCK, BLOCK), BLOCK) for k in range(picks)]
    for k in range(picks):
        pending_next[rows[k], :] = jnp.zeros((BLOCK, cache.shape[1]), jnp.float32)
    write(pending_next, pending_out)
    for k in range(picks):
        divisor = 1.0 + clock[blocks[k]].astype(jnp.float32)
        flush = sums[k * BLOCK : (k + 1) * BLOCK, :] / divisor
        cache_next[rows[k], :], hot_accum_next[rows[k], :] = adagrad(
            cache[rows[k], :], hot_accum[rows[k], :], flush
        )
    write(cache_next, cache_out)
    write(hot_accum_next, hot_accum_out)
    for copy in writes:
        copy.wait()


def update(blocks, clock, top, sums, cold, carried, table, accum, cache, hot_accum):
    head_rows = top.shape[1] // cache.shape[1]
    hbm = pl.BlockSpec(memory_space=pltpu.HBM)
    vmem = pl.BlockSpec(memory_space=pltpu.VMEM)
    like = lambda a: jax.ShapeDtypeStruct(a.shape, a.dtype)
    scratch = lambda a: pltpu.VMEM(a.shape, a.dtype)
    return pl.pallas_call(
        update_kernel,
        out_shape=(
            like(table), like(accum), like(cache), like(hot_accum), like(carried), like(top),
            jax.ShapeDtypeStruct((head_rows, cache.shape[1]), jnp.float32),
        ),
        in_specs=[hbm] * 2 + [vmem] * 8,
        out_specs=(hbm,) * 7,
        scratch_shapes=[
            pltpu.SMEM(blocks.shape, jnp.int32), pltpu.SMEM(clock.shape, jnp.int32),
            scratch(table), scratch(accum), scratch(cache), scratch(hot_accum), scratch(carried),
            pltpu.SemaphoreType.DMA((9,)),
        ],
        compiler_params=pltpu.CompilerParams(vmem_limit_bytes=VMEM_LIMIT // 2),
    )(
        pltpu.with_memory_space_constraint(blocks, pltpu.HBM),
        pltpu.with_memory_space_constraint(clock, pltpu.HBM),
        top, sums, cold, carried, table, accum, cache, hot_accum,
    )


def suits(n, rep_n, top_weight, hot_ids, cold_offset, hot_cache, cold_table):
    features, columns = top_weight.shape
    samples, lookups, width = hot_ids.shape[0], cold_offset.shape[0], hot_cache.shape[1]
    return (
        rep_n == 4
        and n % 2 == 0
        and n in (4, 8, 16)
        and features % (16 * 4 * n) == 0
        and columns % 1024 == 0
        and samples % 128 == 0
        and lookups == 2 * samples
        and width == 128
        and (2 * lookups // n) % 128 == 0
        and hot_cache.shape[0] % 128 == 0
        and cold_table.shape[0] % 256 == 0
    )


def direct(
    n, hot_ids, cold_owner, cold_offset, labels, top_weight, out_weight, cold_table, cold_accum,
    hot_cache, hot_accum, pending, refresh_blocks, block_clock,
):
    cap = 2 * cold_offset.shape[0] // n
    top, sums, cold, carried = step(
        hot_ids.T, cold_owner.reshape(1, -1), cold_offset.reshape(1, -1), labels.reshape(1, -1),
        out_weight.reshape(1, -1), refresh_blocks, top_weight, cold_table, hot_cache, pending, n, cap,
    )
    results = update(
        refresh_blocks, block_clock, top, sums, cold, carried, cold_table, cold_accum, hot_cache,
        hot_accum,
    )
    return results[:6] + (results[6].reshape(-1),)


def local(
    hot_ids,
    cold_owner,
    cold_offset,
    labels,
    top_weight,
    out_weight,
    cold_table,
    cold_accum,
    hot_cache,
    hot_accum,
    pending,
    refresh_blocks,
    block_clock,
):
    n, rep_n = lax.axis_size("dp"), lax.axis_size("rep")
    if suits(n, rep_n, top_weight, hot_ids, cold_offset, hot_cache, cold_table):
        return direct(
            n, hot_ids, cold_owner, cold_offset, labels, top_weight, out_weight, cold_table,
            cold_accum, hot_cache, hot_accum, pending, refresh_blocks, block_clock,
        )
    width = hot_cache.shape[1]
    samples = hot_ids.shape[0]
    hot_feats = hot_ids.shape[1]
    lookups = cold_offset.shape[0]
    cold_feats = lookups // samples
    owners_count = lax.axis_size("dp")
    capacity = max(2, 2 * lookups // owners_count)
    owners = cold_owner[:, 0]
    matches = (owners[:, None] == jnp.arange(owners_count, dtype=jnp.int32)[None, :]).astype(
        jnp.int32
    )
    before = jnp.arange(lookups)[:, None] > jnp.arange(lookups)[None, :]
    earlier = jnp.dot(
        before.astype(jnp.bfloat16),
        matches.astype(jnp.bfloat16),
        preferred_element_type=jnp.float32,
    ).astype(jnp.int32)
    positions = jnp.sum(earlier * matches, axis=1)
    targets = owners * capacity + positions
    places = jnp.arange(owners_count * capacity, dtype=jnp.int32)
    placed = targets[:, None] == places[None, :]
    requests = jnp.sum(jnp.where(placed, cold_offset[:, None], 0), axis=0)
    placed = placed.astype(jnp.bfloat16)
    requests = requests.reshape(owners_count, capacity)
    asked = lax.all_to_all(requests, "dp", split_axis=0, concat_axis=0, tiled=True)
    found = cold_table[asked].astype(jnp.bfloat16)
    returned = lax.all_to_all(found, "dp", split_axis=0, concat_axis=0, tiled=True)
    cold_rows = jnp.dot(
        placed,
        returned.reshape(owners_count * capacity, width),
        preferred_element_type=jnp.float32,
    ).astype(jnp.bfloat16)
    cold_rows = cold_rows.reshape(samples, cold_feats, width)
    hot_rows = hot_cache[hot_ids].astype(jnp.bfloat16)
    inputs = jnp.concatenate([hot_rows, cold_rows], axis=1).reshape(
        samples, (hot_feats + cold_feats) * width
    )
    preact = jnp.dot(inputs, top_weight, preferred_element_type=jnp.float32)
    hidden = jax.nn.silu(preact).astype(jnp.bfloat16)
    hidden_wide = hidden.astype(jnp.float32)
    logits = jnp.dot(hidden_wide, out_weight, precision=lax.Precision.HIGHEST)
    errors = jax.nn.sigmoid(logits) - labels.astype(jnp.float32)
    gates = jax.nn.sigmoid(preact)
    slope = gates * (1.0 + preact * (1.0 - gates))
    dhidden = (errors[:, None] * out_weight[None, :] * slope).astype(jnp.bfloat16)
    head_term = jnp.dot(errors, hidden_wide, precision=lax.Precision.HIGHEST)
    top_part = lax.dot_general(
        inputs, dhidden, (((0,), (0,)), ((), ())), preferred_element_type=jnp.float32
    )
    dinputs = lax.dot_general(
        dhidden, top_weight, (((1,), (1,)), ((), ())), preferred_element_type=jnp.float32
    ).astype(jnp.bfloat16)
    dinputs = dinputs.reshape(samples, hot_feats + cold_feats, width)
    cold_dx = dinputs[:, hot_feats:].reshape(lookups, width)
    outgoing = lax.dot_general(
        placed, cold_dx, (((0,), (0,)), ((), ())), preferred_element_type=jnp.float32
    ).astype(jnp.bfloat16)
    outgoing = outgoing.reshape(owners_count, capacity, width)
    own_rows = cold_table.shape[0]
    quarter = own_rows // lax.axis_size("rep")
    hot_count = hot_cache.shape[0]
    blocks_count = hot_count // BLOCK
    hot_dx = dinputs[:, :hot_feats].reshape(samples * hot_feats, width)
    hot_named = (
        jnp.arange(hot_count, dtype=jnp.int32)[:, None] == hot_ids.reshape(-1)[None, :]
    ).astype(jnp.bfloat16)
    hot_grad = jnp.dot(hot_named, hot_dx, preferred_element_type=jnp.float32)
    carried = (pending + hot_grad).reshape(blocks_count, BLOCK, width)
    picked = carried[refresh_blocks]
    divisors = 1.0 + block_clock.astype(jnp.float32)
    named = refresh_blocks[:, None] == jnp.arange(blocks_count, dtype=jnp.int32)[None, :]
    refreshed = jnp.any(named, axis=0)[:, None, None]
    cache_blocks = hot_cache.reshape(blocks_count, BLOCK, width)
    accum_blocks = hot_accum.reshape(blocks_count, BLOCK, width)
    incoming = lax.all_to_all(outgoing, "dp", split_axis=0, concat_axis=0, tiled=True)
    cold_grad = (
        jnp.zeros((own_rows, width), jnp.float32)
        .at[asked.reshape(-1)]
        .add(incoming.reshape(-1, width).astype(jnp.float32))
    )
    cold_share = lax.psum_scatter(cold_grad, "rep", scatter_dimension=0, tiled=True)
    offset_rows = lax.axis_index("rep") * quarter
    table_share = lax.dynamic_slice_in_dim(cold_table, offset_rows, quarter, 0)
    accum_share = lax.dynamic_slice_in_dim(cold_accum, offset_rows, quarter, 0)
    table_updated, accum_updated = adagrad(table_share, accum_share, cold_share)
    cold_table_new, cold_accum_new = (
        lax.all_gather(table_updated, "rep", axis=0, tiled=True),
        lax.all_gather(accum_updated, "rep", axis=0, tiled=True),
    )
    top_grad = lax.psum_scatter(top_part, ("dp", "rep"), scatter_dimension=0, tiled=True)
    picked_sum, out_grad = lax.psum((picked, head_term), ("dp", "rep"))
    block_sums = jnp.zeros((), jnp.float32)
    for k in range(refresh_blocks.shape[0]):
        block_sums = jnp.where(named[k][:, None, None], picked_sum[k][None], block_sums)
    flush = block_sums / divisors[:, None, None]
    cache_next, accum_next = adagrad(cache_blocks, accum_blocks, flush)
    hot_cache_new = jnp.where(refreshed, cache_next, cache_blocks).reshape(hot_count, width)
    hot_accum_new = jnp.where(refreshed, accum_next, accum_blocks).reshape(hot_count, width)
    pending_new = jnp.where(refreshed, 0.0, carried).reshape(hot_count, width)
    return (
        cold_table_new,
        cold_accum_new,
        hot_cache_new,
        hot_accum_new,
        pending_new,
        top_grad,
        out_grad,
    )


def solution(mesh):
    in_specs = (
        P(("dp", "rep"), None),
        P(("dp", "rep"), None),
        P(("dp", "rep")),
        P(("dp", "rep")),
        P(),
        P(),
        P("dp", None),
        P("dp", None),
        P(),
        P(),
        P(("dp", "rep"), None),
        P(),
        P(),
    )
    out_specs = (
        P("dp", None),
        P("dp", None),
        P(),
        P(),
        P(("dp", "rep"), None),
        P(("dp", "rep"), None),
        P(),
    )
    return jax.shard_map(local, mesh=mesh, in_specs=in_specs, out_specs=out_specs, check_vma=False)
```

```python
import functools

import jax
import jax.numpy as jnp
from jax import lax
from jax.experimental import pallas as pl
from jax.experimental.pallas import tpu as pltpu
from jax.sharding import PartitionSpec as P

BLOCK = 128
VMEM_LIMIT = 40 * 1024 * 1024
MESH = pl.DeviceIdType.MESH


step_size = 0.5
epsilon = 1e-08


def adagrad(table_rows, accum_rows, gradient):
    accum_next = accum_rows + gradient * gradient
    return (table_rows - step_size * gradient / (jnp.sqrt(accum_next) + epsilon), accum_next)


def row_to_col(row, first, step, count):
    per = 128 // step
    shape = (per, 128)
    wanted = lax.broadcasted_iota(jnp.int32, shape, 1) == step * lax.broadcasted_iota(
        jnp.int32, shape, 0
    ) + first
    pieces = []
    for i in range(count // per):
        part = jnp.broadcast_to(row[:, i * 128 : (i + 1) * 128], shape)
        pieces.append(jnp.sum(jnp.where(wanted, part, 0.0), axis=1, keepdims=True))
    return jnp.concatenate(pieces, axis=0)


def col_to_row(col):
    shape = (128, 128)
    same = lax.broadcasted_iota(jnp.int32, shape, 0) == lax.broadcasted_iota(jnp.int32, shape, 1)
    pieces = []
    for i in range(col.shape[0] // 128):
        part = jnp.broadcast_to(col[i * 128 : (i + 1) * 128], shape)
        pieces.append(jnp.sum(jnp.where(same, part, 0.0), axis=0, keepdims=True))
    return jnp.concatenate(pieces, axis=1)


def one_hot(ids, shape, dim):
    match = lax.broadcasted_iota(jnp.int32, shape, dim) == jnp.broadcast_to(ids, shape)
    return jnp.where(match, 1.0, 0.0).astype(jnp.bfloat16)


def matmul(a, b, contract=(1, 0)):
    return lax.dot_general(
        a, b, (((contract[0],), (contract[1],)), ((), ())), preferred_element_type=jnp.float32
    )


def step_kernel(
    n, piece,
    hot_ids_in, owner_in, offset_in, labels_in, out_weight_in, blocks_in, weight, table, cache,
    pending,
    top_out, sums_out, cold_out, carried_out,
    hot_ids, owner, offset, labels, out_weight, blocks,
    weight_v, table_v, table_all, cache_v, pending_v, tables, requests, asked, look, placed_t, hot_t, own_hot,
    pre, gate, hidden, inputs_t, inputs_got, dh, dh_got, outgoing, incoming,
    top, leave, got_1, part_1, got_2, part_2, got_3, leave_z, got_z, part_z, got_zx, part_zx, got_zy,
    cold, cold_got, cold_half, cold_last, cold_full, hot_sum, hot_got, hot_mid, hot_near, hot_z,
    hot_all,
    loads, sends, recvs,
):
    me, rep = lax.axis_index("dp"), lax.axis_index("rep")
    x, z = lax.rem(me, 2), lax.div(me, 2)
    core, y = lax.rem(rep, 2), lax.div(rep, 2)
    depth = n // 2
    f32, bf16 = jnp.float32, jnp.bfloat16

    def flip(value, on):
        return 1 - value if on else value

    def near(mask):
        return (z * 2 + flip(x, mask & 4), flip(y, mask & 2) * 2 + flip(core, mask & 1))

    def level(k):
        value = z
        for weight in (1, 2, 4):
            if k & weight:
                value = value + weight * (1 - 2 * lax.rem(lax.div(z, weight), 2))
        return value

    def along(k):
        return level(k) * 2 + x

    sibling, over_x, over_y, over_xy = near(1), near(4), near(2), near(6)
    peers = [lax.rem(me + j, n) for j in range(1, n)]
    sources = [lax.rem(me + n - j, n) for j in range(1, n)]
    greeted = [(peer, rep) for peer in peers] + [sibling, over_y, over_xy]
    barrier = pltpu.get_barrier_semaphore()
    for device in greeted:
        pl.semaphore_signal(barrier, inc=1, device_id=device, device_id_type=MESH)
    local = []
    for src, dst in [
        (table.at[rep], table_v), (owner_in, owner), (offset_in, offset),
        (table, table_all), (hot_ids_in, hot_ids), (cache, cache_v),
        (weight, weight_v), (labels_in, labels), (out_weight_in, out_weight), (blocks_in, blocks),
        (pending, pending_v),
    ]:
        local.append(pltpu.make_async_copy(src, dst, loads.at[len(local)]))
    for copy in local[:3]:
        copy.start()

    count = [0]
    started = []

    def send(src, dst, device):
        k = count[0]
        count[0] += 1
        copy = pltpu.make_async_remote_copy(src, dst, sends.at[k], recvs.at[k], device, MESH)
        copy.start()
        started.append(copy)
        return copy

    def same(ref, device):
        return send(ref, ref, device)

    local[0].wait()
    tables[me, rep] = table_v[...].astype(bf16)
    for copy in local[3:]:
        copy.start()
    pl.semaphore_wait(barrier, len(greeted))
    mine = tables.at[me, rep]
    order = list(range(1, depth))
    z_table = {k: same(mine, (along(k), rep)) for k in order[::-1]}
    x_table = same(mine, over_x)
    xy_table = same(mine, over_xy)

    samples = hot_ids.shape[1]
    hot_feats = hot_ids.shape[0]
    lookups = owner.shape[1]
    feats = lookups // samples
    own_rows, width = tables.shape[1] * tables.shape[2], tables.shape[3]
    cap = requests.shape[2]
    hot_rows = cache_v.shape[0]
    columns = weight_v.shape[1]
    chunk = dh.shape[2]
    chunks = columns // chunk
    hot_in = hot_feats * width

    local[1].wait()
    local[2].wait()
    owner_row, offset_row = owner[...].astype(f32), offset[...].astype(f32)
    owner_col = jnp.concatenate(
        [row_to_col(owner_row, k, feats, samples) for k in range(feats)], axis=0
    )
    offset_col = jnp.concatenate(
        [row_to_col(offset_row, k, feats, samples) for k in range(feats)], axis=0
    )
    lanes = lax.broadcasted_iota(jnp.int32, (lookups, 128), 1)
    matches = jnp.where(lanes == owner_col.astype(jnp.int32), 1.0, 0.0)
    square = (lookups, lookups)
    before = lax.broadcasted_iota(jnp.int32, square, 1) < lax.broadcasted_iota(
        jnp.int32, square, 0
    )
    earlier = matmul(jnp.where(before, 1.0, 0.0).astype(bf16), matches.astype(bf16))
    target = owner_col * cap + jnp.sum(earlier * matches, axis=1, keepdims=True)
    target_int = target.astype(jnp.int32)
    for o in range(n):
        slots = lax.broadcasted_iota(jnp.int32, (lookups, cap), 1) + o * cap
        asks = jnp.where(slots == target_int, offset_col, 0.0)
        requests[o] = jnp.sum(asks, axis=0, keepdims=True).astype(jnp.int32)
    asking = [send(requests.at[peer], asked.at[me], (peer, rep)) for peer in peers]
    asked[me] = requests[me]

    def relay(copy, source, *devices):
        copy.wait_recv()
        return [same(tables.at[source, rep], device) for device in devices]

    def looked(o):
        return matmul(look[o], tables[o].reshape(own_rows, width))

    x_source = z * 2 + 1 - x
    z_source = {k: along(k) for k in order}
    far_source = {k: level(k) * 2 + 1 - x for k in order}
    others = [x_source] + [z_source[k] for k in order] + [far_source[k] for k in order]
    by_y, by_core, y_core, by_x = {}, {}, {}, {}
    (by_core[0],) = relay(x_table, x_source, sibling)
    by_y[0] = xy_table

    def relay_z(i):
        k = order[i]
        by_x[k], by_y[depth + i], by_y[1 + i], by_core[1 + i] = relay(
            z_table[k], z_source[k], over_x, over_xy, over_y, sibling
        )

    relay_z(0)

    local[4].wait()
    hot_col = jnp.concatenate(
        [row_to_col(hot_ids[k : k + 1].astype(f32), 0, 1, samples) for k in range(hot_feats)], axis=0
    )
    local[5].wait()
    hot_found = matmul(
        one_hot(hot_col.astype(jnp.int32), (hot_feats * samples, hot_rows), 1),
        cache_v[...].astype(bf16),
    )
    hot_x = [hot_found[k * samples : (k + 1) * samples] for k in range(hot_feats)]

    for i in range(1, depth - 1):
        relay_z(i)

    global_col = (owner_col * own_rows + offset_col).astype(jnp.int32)
    for o in range(n):
        look[o] = one_hot(global_col - o * own_rows, (lookups, own_rows), 1)

    local[6].wait()
    hot_wide = jnp.concatenate(hot_x, axis=1).astype(bf16)
    for h in range(chunks):
        at = slice(h * chunk, (h + 1) * chunk)
        pre[:, at] = matmul(hot_wide, weight_v[:hot_in, at])
    local[3].wait()
    for i in range(1, 4):
        tables[me, lax.rem(rep + i, 4)] = table_all[lax.rem(rep + i, 4)].astype(bf16)

    def relay_y(i):
        by_y[i].wait_recv()
        y_core[i] = same(tables.at[others[i], (1 - y) * 2 + core], sibling)

    def found(j):
        by_core[j].wait_recv()
        y_core[j].wait_recv()
        return looked(others[j])

    def relay_far(i):
        k = order[i]
        (by_core[depth + i],) = relay(by_x[k], far_source[k], sibling)
        relay_y(1 + i)
        relay_y(depth + i)

    placed_t[...] = one_hot(
        col_to_row(target).astype(jnp.int32), (n * cap, lookups), 0
    )
    hot_t[...] = one_hot(
        jnp.concatenate([hot_ids[k : k + 1] for k in range(hot_feats)], axis=1),
        (hot_rows, hot_feats * samples), 0,
    )
    cold_found = looked(me)
    relay_y(0)
    relay_far(0)
    cold_found += found(0)
    for i in range(1, depth - 1):
        relay_far(i)
        if i < depth - 2:
            cold_found += found(i)
    for j in range(max(1, depth - 2), n - 1):
        cold_found += found(j)
    cold_x = [cold_found[k * samples : (k + 1) * samples] for k in range(feats)]
    inputs_t[...] = (
        jnp.concatenate([part.T for part in hot_x + cold_x], axis=0)
        .astype(bf16)
        .reshape(inputs_t.shape)
    )
    inputs_copy = send(inputs_t.at[:, 1 - core], inputs_got, sibling)

    local[7].wait()
    local[8].wait()
    cold_wide = jnp.concatenate(cold_x, axis=1).astype(bf16)
    logits = jnp.zeros((samples, 1), f32)
    for h in range(chunks):
        at = slice(h * chunk, (h + 1) * chunk)
        preact = pre[:, at] + matmul(cold_wide, weight_v[hot_in:, at])
        gates = jax.nn.sigmoid(preact)
        shown = (preact * gates).astype(bf16)
        hidden[:, at] = shown
        logits += jnp.sum(shown.astype(f32) * out_weight[:, at], axis=1, keepdims=True)
        gate[:, at] = out_weight[:, at] * (gates * (1.0 + preact * (1.0 - gates)))
    errors = jax.nn.sigmoid(logits) - row_to_col(labels[...].astype(f32), 0, 1, samples)
    dh_copies = []
    for h in range(chunks):
        at = slice(h * chunk, (h + 1) * chunk)
        dh[h] = (errors * gate[:, at]).astype(bf16)
        dh_copies.append(send(dh.at[h], dh_got.at[h], sibling))

    def dinputs(rows):
        total = matmul(dh[0], weight_v[rows, :chunk], (1, 1))
        for h in range(1, chunks):
            total += matmul(dh[h], weight_v[rows, h * chunk : (h + 1) * chunk], (1, 1))
        total = total.astype(bf16)
        return jnp.concatenate(
            [total[:, k : k + width] for k in range(0, total.shape[1], width)], axis=0
        )

    cold_dx = dinputs(slice(hot_in, weight_v.shape[0]))
    outgoing[...] = matmul(placed_t[...], cold_dx).astype(bf16).reshape(outgoing.shape)
    cold_copies = [send(outgoing.at[peer], incoming.at[me], (peer, rep)) for peer in peers]
    incoming[me] = outgoing[me]

    hot_dx = dinputs(slice(0, hot_in))
    local[9].wait()
    local[10].wait()
    carried_out[...] = pending_v[...] + matmul(hot_t[...], hot_dx)
    total_rows = hot_sum.shape[0]
    picks = blocks.shape[0]
    for k in range(picks):
        wanted = jnp.full((BLOCK, width), blocks[k])
        picked = carried_out[:BLOCK, :]
        for b in range(1, hot_rows // BLOCK):
            picked = jnp.where(wanted == b, carried_out[b * BLOCK : (b + 1) * BLOCK, :], picked)
        hot_sum[k * BLOCK : (k + 1) * BLOCK, :] = picked
    base = picks * BLOCK
    hot_sum[base:, :] = jnp.zeros((total_rows - base, width), f32)
    for h in range(chunks):
        head = jnp.sum(
            errors * hidden[:, h * chunk : (h + 1) * chunk].astype(f32), axis=0, keepdims=True
        )
        for i in range(chunk // width):
            row = base + h * (chunk // width) + i
            hot_sum[row : row + 1, :] = head[:, i * width : (i + 1) * width]

    def part_of(ref, q, rows):
        return ref.at[pl.ds(pl.multiple_of(q * rows, 8), rows)]

    hot_copy = send(part_of(hot_sum, 1 - core, 4 * piece), hot_got, sibling)
    my_quad = x * 2 + y
    quads = [(flip(x, m & 4) * 2 + flip(y, m & 2), near(m)) for m in (2, 4, 6)]

    inputs_copy.wait_recv()

    kinds = ["y", "y", "x", "z"]

    def first_step(h):
        both = matmul(inputs_t[:, core].reshape(-1, samples), dh[h])
        dh_copies[h].wait_recv()
        both += matmul(inputs_got[...].reshape(-1, samples), dh_got[h])
        top[h] = both.reshape(top.shape[1:])
        if kinds[h] == "z":
            copies = []
            for k in range(1, depth):
                leave_z[k - 1] = top[h, level(k)].astype(bf16)
                copies.append(send(leave_z.at[k - 1], got_z.at[k - 1], (along(k), rep)))
            return copies
        leaving = top[h, :, 1 - x] if kinds[h] == "x" else top[h, :, :, 1 - y]
        leave[h] = leaving.astype(bf16)
        return [send(leave.at[h], got_1.at[h], over_x if kinds[h] == "x" else over_y)]

    def second_step(h):
        for copy in first[h]:
            copy.wait_recv()
        if kinds[h] == "z":
            part = top[h, z]
            for k in range(depth - 1):
                part += got_z[k].astype(f32)
            part_z[...] = part
            return send(part_z.at[1 - x], got_zx, over_x)
        kept = top[h, :, x] if kinds[h] == "x" else top[h, :, :, y]
        part_1[h] = kept + got_1[h].astype(f32)
        if kinds[h] == "x":
            return send(part_1.at[h, :, 1 - y], got_2.at[h], over_y)
        return send(part_1.at[h, :, 1 - x], got_2.at[h], over_x)

    def third_step(h):
        second[h].wait_recv()
        if kinds[h] == "z":
            part_zx[...] = part_z[x] + got_zx[...]
            return [send(part_zx.at[1 - y], got_zy, over_y)]
        part_2[h] = part_1[h, :, y if kinds[h] == "x" else x] + got_2[h]
        return [
            send(part_2.at[h, level(k)], got_3.at[h, k - 1], (along(k), rep))
            for k in range(1, depth)
        ]

    def last_step(h):
        for copy in third[h]:
            copy.wait_recv()
        if kinds[h] == "z":
            part = part_zx[y] + got_zy[...]
        else:
            part = part_2[h, z]
            for k in range(depth - 1):
                part += got_3[h, k]
        top_out[:, h * chunk : (h + 1) * chunk] = part

    first = [first_step(h) for h in range(chunks // 2)]

    hot_copy.wait_recv()
    hot_mid[...] = part_of(hot_sum, core, 4 * piece)[...] + hot_got[...]
    hot_copies = [
        send(part_of(hot_mid, q, piece), hot_near.at[i], device)
        for i, (q, device) in enumerate(quads)
    ]
    first += [first_step(h) for h in range(chunks // 2, chunks)]


    for o in range(n - 1):
        asking[o].wait_recv()
    for o in range(n):
        own_hot[:, :, o * cap : (o + 1) * cap] = one_hot(asked[o], (own_rows, cap), 0).reshape(
            2, own_rows // 2, cap
        )

    second = {h: second_step(h) for h in (0, 1, 2)}

    for copy in hot_copies:
        copy.wait_recv()
    hot_z[z] = part_of(hot_mid, my_quad, piece)[...] + hot_near[0] + hot_near[1] + hot_near[2]
    hot_copies = [same(hot_z.at[z], (along(k), rep)) for k in range(1, depth)]

    for copy in cold_copies:
        copy.wait_recv()
    arrived = incoming[...].reshape(n * cap, width)
    cold[1 - core] = matmul(own_hot[1 - core], arrived)
    cold_copy = send(cold.at[1 - core], cold_got, sibling)
    cold[core] = matmul(own_hot[core], arrived)

    second[3] = second_step(3)

    cold_copy.wait_recv()
    cold_half[...] = cold[core] + cold_got[...]
    cold_copy = send(cold_half, cold_last, over_y)

    third = {h: third_step(h) for h in (2, 0, 1)}

    for copy in hot_copies:
        copy.wait_recv()
    final = hot_z[0]
    for k in range(1, depth):
        final += hot_z[k]
    ours = core * 4 + my_quad
    part_of(hot_all, ours, piece)[...] = final
    hot_copies = [same(part_of(hot_all, ours, piece), device) for _, device in quads]

    third[3] = third_step(3)

    cold_copy.wait_recv()
    cold_full[core] = cold_half[...] + cold_last[...]
    cold_copy = same(cold_full.at[core], sibling)

    for copy in hot_copies:
        copy.wait_recv()
    hot_copy = same(part_of(hot_all, core, 4 * piece), sibling)

    for h in (3, 2, 0, 1):
        last_step(h)
    cold_copy.wait_recv()
    cold_out[...] = cold_full[...].reshape(cold_out.shape)
    hot_copy.wait_recv()
    sums_out[...] = hot_all[...]
    for copy in started:
        copy.wait_send()


def step(hot_ids, owner, offset, labels, out_weight, blocks, weight, table, cache, pending, n, cap):
    hot_feats, samples = hot_ids.shape
    lookups = owner.shape[1]
    features, columns = weight.shape
    own_rows, width = table.shape
    hot_rows = cache.shape[0]
    depth = n // 2
    rows = features // (4 * n)
    chunk = columns // 4
    sum_rows = blocks.shape[0] * BLOCK + columns // width
    piece = -(-sum_rows // 64) * 8
    f32 = lambda *shape: pltpu.VMEM(shape, jnp.float32)
    b16 = lambda *shape: pltpu.VMEM(shape, jnp.bfloat16)
    i32 = lambda *shape: pltpu.VMEM(shape, jnp.int32)
    copies = 6 * n + 8 * depth + 32
    vmem = pl.BlockSpec(memory_space=pltpu.VMEM)
    hbm = pl.BlockSpec(memory_space=pltpu.HBM)
    out = lambda *shape: jax.ShapeDtypeStruct(shape, jnp.float32)
    return pl.pallas_call(
        functools.partial(step_kernel, n, piece),
        out_shape=(
            out(rows, columns), out(8 * piece, width), out(own_rows, width), out(hot_rows, width)
        ),
        in_specs=[hbm] * 10,
        out_specs=(vmem,) * 4,
        scratch_shapes=[
            i32(hot_feats, samples), i32(1, lookups), i32(1, lookups), i32(1, samples),
            f32(1, columns), pltpu.SMEM(blocks.shape, jnp.int32),
            b16(features, columns), f32(own_rows // 4, width),
            f32(4, own_rows // 4, width), f32(hot_rows, width),
            f32(hot_rows, width), b16(n, 4, own_rows // 4, width), i32(n, 1, cap), i32(n, 1, cap),
            b16(n, lookups, own_rows), b16(n * cap, lookups), b16(hot_rows, hot_feats * samples),
            b16(2, own_rows // 2, n * cap),
            f32(samples, columns), f32(samples, columns), b16(samples, columns),
            b16(4 * depth, 2, rows, samples), b16(4 * depth, rows, samples),
            b16(4, samples, chunk), b16(4, samples, chunk),
            b16(n, cap, width), b16(n, cap, width),
            f32(4, depth, 2, 2, rows, chunk), b16(4, depth, 2, rows, chunk),
            b16(4, depth, 2, rows, chunk),
            f32(4, depth, 2, rows, chunk), f32(4, depth, rows, chunk), f32(4, depth, rows, chunk),
            f32(4, depth - 1, rows, chunk), b16(depth - 1, 2, 2, rows, chunk),
            b16(depth - 1, 2, 2, rows, chunk), f32(2, 2, rows, chunk), f32(2, rows, chunk),
            f32(2, rows, chunk), f32(rows, chunk),
            f32(2, own_rows // 2, width), f32(own_rows // 2, width), f32(own_rows // 2, width),
            f32(own_rows // 2, width), f32(2, own_rows // 2, width),
            f32(8 * piece, width), f32(4 * piece, width), f32(4 * piece, width),
            f32(3, piece, width), f32(depth, piece, width), f32(8 * piece, width),
            pltpu.SemaphoreType.DMA((11,)),
            pltpu.SemaphoreType.DMA((copies,)),
            pltpu.SemaphoreType.DMA((copies,)),
        ],
        compiler_params=pltpu.CompilerParams(
            collective_id=0, has_side_effects=True, vmem_limit_bytes=VMEM_LIMIT
        ),
    )(
        *[
            pltpu.with_memory_space_constraint(value, pltpu.HBM)
            for value in (
                hot_ids, owner, offset, labels, out_weight, blocks,
                weight, table.reshape(4, own_rows // 4, width), cache, pending,
            )
        ]
    )


def update_kernel(
    blocks_in, clock_in, top, sums, cold, carried, table, accum, cache, hot_accum,
    table_out, accum_out, cache_out, hot_accum_out, pending_out, top_out, head_out,
    blocks, clock, table_next, accum_next, cache_next, hot_accum_next, pending_next, sems,
):
    scalars = [
        pltpu.make_async_copy(blocks_in, blocks, sems.at[0]),
        pltpu.make_async_copy(clock_in, clock, sems.at[1]),
    ]
    for copy in scalars:
        copy.start()
    writes = []

    def write(src, dst):
        writes.append(pltpu.make_async_copy(src, dst, sems.at[2 + len(writes)]))
        writes[-1].start()

    picks = blocks.shape[0]
    write(top, top_out)
    write(sums.at[picks * BLOCK : picks * BLOCK + head_out.shape[0]], head_out)
    table_next[...], accum_next[...] = adagrad(table[...], accum[...], cold[...])
    write(table_next, table_out)
    write(accum_next, accum_out)
    pending_next[...] = carried[...]
    cache_next[...] = cache[...]
    hot_accum_next[...] = hot_accum[...]
    for copy in scalars:
        copy.wait()
    rows = [pl.ds(pl.multiple_of(blocks[k] * BLOCK, BLOCK), BLOCK) for k in range(picks)]
    for k in range(picks):
        pending_next[rows[k], :] = jnp.zeros((BLOCK, cache.shape[1]), jnp.float32)
    write(pending_next, pending_out)
    for k in range(picks):
        divisor = 1.0 + clock[blocks[k]].astype(jnp.float32)
        flush = sums[k * BLOCK : (k + 1) * BLOCK, :] / divisor
        cache_next[rows[k], :], hot_accum_next[rows[k], :] = adagrad(
            cache[rows[k], :], hot_accum[rows[k], :], flush
        )
    write(cache_next, cache_out)
    write(hot_accum_next, hot_accum_out)
    for copy in writes:
        copy.wait()


def update(blocks, clock, top, sums, cold, carried, table, accum, cache, hot_accum):
    head_rows = top.shape[1] // cache.shape[1]
    hbm = pl.BlockSpec(memory_space=pltpu.HBM)
    vmem = pl.BlockSpec(memory_space=pltpu.VMEM)
    like = lambda a: jax.ShapeDtypeStruct(a.shape, a.dtype)
    scratch = lambda a: pltpu.VMEM(a.shape, a.dtype)
    return pl.pallas_call(
        update_kernel,
        out_shape=(
            like(table), like(accum), like(cache), like(hot_accum), like(carried), like(top),
            jax.ShapeDtypeStruct((head_rows, cache.shape[1]), jnp.float32),
        ),
        in_specs=[hbm] * 2 + [vmem] * 8,
        out_specs=(hbm,) * 7,
        scratch_shapes=[
            pltpu.SMEM(blocks.shape, jnp.int32), pltpu.SMEM(clock.shape, jnp.int32),
            scratch(table), scratch(accum), scratch(cache), scratch(hot_accum), scratch(carried),
            pltpu.SemaphoreType.DMA((9,)),
        ],
        compiler_params=pltpu.CompilerParams(vmem_limit_bytes=VMEM_LIMIT // 2),
    )(
        pltpu.with_memory_space_constraint(blocks, pltpu.HBM),
        pltpu.with_memory_space_constraint(clock, pltpu.HBM),
        top, sums, cold, carried, table, accum, cache, hot_accum,
    )


def suits(n, rep_n, top_weight, hot_ids, cold_offset, hot_cache, cold_table):
    features, columns = top_weight.shape
    samples, lookups, width = hot_ids.shape[0], cold_offset.shape[0], hot_cache.shape[1]
    return (
        rep_n == 4
        and n % 2 == 0
        and n in (4, 8, 16)
        and features % (16 * 4 * n) == 0
        and columns % 1024 == 0
        and samples % 128 == 0
        and lookups == 2 * samples
        and width == 128
        and (2 * lookups // n) % 128 == 0
        and hot_cache.shape[0] % 128 == 0
        and cold_table.shape[0] % 256 == 0
    )


def direct(
    n, hot_ids, cold_owner, cold_offset, labels, top_weight, out_weight, cold_table, cold_accum,
    hot_cache, hot_accum, pending, refresh_blocks, block_clock,
):
    cap = 2 * cold_offset.shape[0] // n
    top, sums, cold, carried = step(
        hot_ids.T, cold_owner.reshape(1, -1), cold_offset.reshape(1, -1), labels.reshape(1, -1),
        out_weight.reshape(1, -1), refresh_blocks, top_weight, cold_table, hot_cache, pending, n, cap,
    )
    results = update(
        refresh_blocks, block_clock, top, sums, cold, carried, cold_table, cold_accum, hot_cache,
        hot_accum,
    )
    return results[:6] + (results[6].reshape(-1),)


def local(
    hot_ids,
    cold_owner,
    cold_offset,
    labels,
    top_weight,
    out_weight,
    cold_table,
    cold_accum,
    hot_cache,
    hot_accum,
    pending,
    refresh_blocks,
    block_clock,
):
    n, rep_n = lax.axis_size("dp"), lax.axis_size("rep")
    if suits(n, rep_n, top_weight, hot_ids, cold_offset, hot_cache, cold_table):
        return direct(
            n, hot_ids, cold_owner, cold_offset, labels, top_weight, out_weight, cold_table,
            cold_accum, hot_cache, hot_accum, pending, refresh_blocks, block_clock,
        )
    width = hot_cache.shape[1]
    samples = hot_ids.shape[0]
    hot_feats = hot_ids.shape[1]
    lookups = cold_offset.shape[0]
    cold_feats = lookups // samples
    owners_count = lax.axis_size("dp")
    capacity = max(2, 2 * lookups // owners_count)
    owners = cold_owner[:, 0]
    matches = (owners[:, None] == jnp.arange(owners_count, dtype=jnp.int32)[None, :]).astype(
        jnp.int32
    )
    before = jnp.arange(lookups)[:, None] > jnp.arange(lookups)[None, :]
    earlier = jnp.dot(
        before.astype(jnp.bfloat16),
        matches.astype(jnp.bfloat16),
        preferred_element_type=jnp.float32,
    ).astype(jnp.int32)
    positions = jnp.sum(earlier * matches, axis=1)
    targets = owners * capacity + positions
    places = jnp.arange(owners_count * capacity, dtype=jnp.int32)
    placed = targets[:, None] == places[None, :]
    requests = jnp.sum(jnp.where(placed, cold_offset[:, None], 0), axis=0)
    placed = placed.astype(jnp.bfloat16)
    requests = requests.reshape(owners_count, capacity)
    asked = lax.all_to_all(requests, "dp", split_axis=0, concat_axis=0, tiled=True)
    found = cold_table[asked].astype(jnp.bfloat16)
    returned = lax.all_to_all(found, "dp", split_axis=0, concat_axis=0, tiled=True)
    cold_rows = jnp.dot(
        placed,
        returned.reshape(owners_count * capacity, width),
        preferred_element_type=jnp.float32,
    ).astype(jnp.bfloat16)
    cold_rows = cold_rows.reshape(samples, cold_feats, width)
    hot_rows = hot_cache[hot_ids].astype(jnp.bfloat16)
    inputs = jnp.concatenate([hot_rows, cold_rows], axis=1).reshape(
        samples, (hot_feats + cold_feats) * width
    )
    preact = jnp.dot(inputs, top_weight, preferred_element_type=jnp.float32)
    hidden = jax.nn.silu(preact).astype(jnp.bfloat16)
    hidden_wide = hidden.astype(jnp.float32)
    logits = jnp.dot(hidden_wide, out_weight, precision=lax.Precision.HIGHEST)
    errors = jax.nn.sigmoid(logits) - labels.astype(jnp.float32)
    gates = jax.nn.sigmoid(preact)
    slope = gates * (1.0 + preact * (1.0 - gates))
    dhidden = (errors[:, None] * out_weight[None, :] * slope).astype(jnp.bfloat16)
    head_term = jnp.dot(errors, hidden_wide, precision=lax.Precision.HIGHEST)
    top_part = lax.dot_general(
        inputs, dhidden, (((0,), (0,)), ((), ())), preferred_element_type=jnp.float32
    )
    dinputs = lax.dot_general(
        dhidden, top_weight, (((1,), (1,)), ((), ())), preferred_element_type=jnp.float32
    ).astype(jnp.bfloat16)
    dinputs = dinputs.reshape(samples, hot_feats + cold_feats, width)
    cold_dx = dinputs[:, hot_feats:].reshape(lookups, width)
    outgoing = lax.dot_general(
        placed, cold_dx, (((0,), (0,)), ((), ())), preferred_element_type=jnp.float32
    ).astype(jnp.bfloat16)
    outgoing = outgoing.reshape(owners_count, capacity, width)
    own_rows = cold_table.shape[0]
    quarter = own_rows // lax.axis_size("rep")
    hot_count = hot_cache.shape[0]
    blocks_count = hot_count // BLOCK
    hot_dx = dinputs[:, :hot_feats].reshape(samples * hot_feats, width)
    hot_named = (
        jnp.arange(hot_count, dtype=jnp.int32)[:, None] == hot_ids.reshape(-1)[None, :]
    ).astype(jnp.bfloat16)
    hot_grad = jnp.dot(hot_named, hot_dx, preferred_element_type=jnp.float32)
    carried = (pending + hot_grad).reshape(blocks_count, BLOCK, width)
    picked = carried[refresh_blocks]
    divisors = 1.0 + block_clock.astype(jnp.float32)
    named = refresh_blocks[:, None] == jnp.arange(blocks_count, dtype=jnp.int32)[None, :]
    refreshed = jnp.any(named, axis=0)[:, None, None]
    cache_blocks = hot_cache.reshape(blocks_count, BLOCK, width)
    accum_blocks = hot_accum.reshape(blocks_count, BLOCK, width)
    incoming = lax.all_to_all(outgoing, "dp", split_axis=0, concat_axis=0, tiled=True)
    cold_grad = (
        jnp.zeros((own_rows, width), jnp.float32)
        .at[asked.reshape(-1)]
        .add(incoming.reshape(-1, width).astype(jnp.float32))
    )
    cold_share = lax.psum_scatter(cold_grad, "rep", scatter_dimension=0, tiled=True)
    offset_rows = lax.axis_index("rep") * quarter
    table_share = lax.dynamic_slice_in_dim(cold_table, offset_rows, quarter, 0)
    accum_share = lax.dynamic_slice_in_dim(cold_accum, offset_rows, quarter, 0)
    table_updated, accum_updated = adagrad(table_share, accum_share, cold_share)
    cold_table_new, cold_accum_new = (
        lax.all_gather(table_updated, "rep", axis=0, tiled=True),
        lax.all_gather(accum_updated, "rep", axis=0, tiled=True),
    )
    top_grad = lax.psum_scatter(top_part, ("dp", "rep"), scatter_dimension=0, tiled=True)
    picked_sum, out_grad = lax.psum((picked, head_term), ("dp", "rep"))
    block_sums = jnp.zeros((), jnp.float32)
    for k in range(refresh_blocks.shape[0]):
        block_sums = jnp.where(named[k][:, None, None], picked_sum[k][None], block_sums)
    flush = block_sums / divisors[:, None, None]
    cache_next, accum_next = adagrad(cache_blocks, accum_blocks, flush)
    hot_cache_new = jnp.where(refreshed, cache_next, cache_blocks).reshape(hot_count, width)
    hot_accum_new = jnp.where(refreshed, accum_next, accum_blocks).reshape(hot_count, width)
    pending_new = jnp.where(refreshed, 0.0, carried).reshape(hot_count, width)
    return (
        cold_table_new,
        cold_accum_new,
        hot_cache_new,
        hot_accum_new,
        pending_new,
        top_grad,
        out_grad,
    )


def solution(mesh):
    in_specs = (
        P(("dp", "rep"), None),
        P(("dp", "rep"), None),
        P(("dp", "rep")),
        P(("dp", "rep")),
        P(),
        P(),
        P("dp", None),
        P("dp", None),
        P(),
        P(),
        P(("dp", "rep"), None),
        P(),
        P(),
    )
    out_specs = (
        P("dp", None),
        P("dp", None),
        P(),
        P(),
        P(("dp", "rep"), None),
        P(("dp", "rep"), None),
        P(),
    )
    return jax.shard_map(local, mesh=mesh, in_specs=in_specs, out_specs=out_specs, check_vma=False)
```
